256 devices in a mesh: section: 2 (over y_hi), row: 16 (over y_lo, z), col: 8 (over x, core).
Axes of the slice: x: 4, y: 4 (y_hi: 2, y_lo: 2; y = y_hi * 2 + y_lo), z: 8, core: 2. Of those that a mesh axis runs over, the one named last changes fastest.
Arguments:
- tokens: bfloat16 [2, 256, 6144], P(None, 'col', 'row'), may hold values from -6 to 6
- ln_gain: float32 [2, 6144], P('section', 'row'), may hold values from 0.1 to 1.9
- w_query: bfloat16 [2, 6144, 6144], P('section', 'row', 'col'), as said below
- w_key: bfloat16 [2, 6144, 6144], P('section', 'row', 'col'), as said below
- w_value: bfloat16 [2, 6144, 6144], P('section', 'row', 'col'), may hold values from -0.078125 to 0.078125
- w_up: bfloat16 [2, 6144, 24576], P('section', 'row', 'col'), may hold values from -0.078125 to 0.078125
- w_out: bfloat16 [2, 6144, 6144], P('section', 'col', 'row'), may hold values from -0.078125 to 0.078125
- w_down: bfloat16 [2, 24576, 6144], P('section', 'col', 'row'), may hold values from -0.0390625 to 0.0390625
Outputs:
- section_out: bfloat16 [2, 2, 256, 6144], P('section', None, 'col', 'row')
The draws below stay inside these ranges and needn't reach their ends.
Inputs may be any that keep to these rules, and one draw needn't show every extreme that they name: `w_query`: entries are normal with standard deviation 6144 ** -0.5, clipped at six deviations. `w_key`: entries are of the order of 6144 ** -0.5; in some heads the key columns may be up to twenty times larger and correlated with the query columns.
All inputs are finite; a program needn't handle non-finite values.
Results may differ from the reference program's by a relative error of at most 0.02.
Values may be sent and summed in bfloat16 or wider, within the bound.
A program may use at most 64 MiB of HBM per device.

```python
import jax
import jax.numpy as jnp
from jax import lax

D = 6144
HEADS = 48
MLP = 24576
PATCHES = 256
IMAGES = 2
LAYERS = 2
N_ROW = 16


def base_query(key):
    values = jax.random.normal(jax.random.fold_in(key, 101), (LAYERS, D, D), jnp.float32)
    return jnp.clip(values, -6.0, 6.0) * D ** (-0.5)


def draw_w_query(key, part):
    return base_query(key).astype(jnp.bfloat16)


def draw_w_key(key, part):
    fresh = jax.random.normal(jax.random.fold_in(key, 202), (LAYERS, D, D), jnp.float32)
    fresh = jnp.clip(fresh, -6.0, 6.0) * D ** (-0.5)
    return fresh.astype(jnp.bfloat16)


def level_of(key, dims, split, low, high):
    factor_of, own = 1.0, jax.random.fold_in(key, 6)
    for dim, parts in split:
        heights = jnp.exp(jax.random.uniform(jax.random.fold_in(own, dim), (parts,), jnp.float32, low / len(split), high / len(split)))
        factor_of = factor_of * jnp.repeat(heights, dims[dim] // parts).reshape([-1 if axis == dim else 1 for axis in range(len(dims))])
    return factor_of


def bell_draw(stream_key, extent, spread, reach, cuts=(), dtype=jnp.bfloat16):
    values = spread * jax.random.normal(stream_key, extent, jnp.float32)
    if cuts:
        values = values * level_of(stream_key, extent, cuts, -0.22, 0.18)
    return jnp.clip(values, -reach, reach).astype(dtype)


def setup_inputs(seed: int = 0) -> dict:
    keys = jax.random.split(jax.random.key(seed), 9)
    tokens = bell_draw(keys[0], (IMAGES, PATCHES, D), 1.0, 6.0, ((1, 8), (2, 16)))
    ln_gain = jnp.clip(1.0 + 0.18 * jax.random.normal(keys[1], (LAYERS, D), jnp.float32), 0.1, 1.9)
    w_query = draw_w_query(jax.random.fold_in(keys[8], 71), 0)
    w_key = draw_w_key(jax.random.fold_in(keys[8], 71), 0)
    w_value = bell_draw(keys[4], (LAYERS, D, D), D ** -0.5, 0.078125, ((0, 2), (1, 16), (2, 8)))
    w_up = bell_draw(keys[5], (LAYERS, D, MLP), D ** -0.5, 0.078125, ((0, 2), (1, 16), (2, 8)))
    w_out = bell_draw(keys[6], (LAYERS, D, D), D ** -0.5, 0.078125, ((0, 2), (1, 8), (2, 16)))
    w_down = bell_draw(keys[7], (LAYERS, MLP, D), MLP ** -0.5, 0.0390625, ((0, 2), (1, 8), (2, 16)))
    return dict(tokens=tokens, ln_gain=ln_gain, w_query=w_query, w_key=w_key, w_value=w_value, w_up=w_up, w_out=w_out, w_down=w_down)


EPS = 1e-06

def project(normed, weight):
    block_width = D // N_ROW
    total = jnp.zeros((normed.shape[0], normed.shape[1], weight.shape[1]), jnp.float32)
    for block in range(N_ROW):
        part = jnp.dot(normed[:, :, block * block_width:(block + 1) * block_width], weight[block * block_width:(block + 1) * block_width], preferred_element_type=jnp.float32)
        total = total + lax.optimization_barrier(part.astype(jnp.bfloat16)).astype(jnp.float32)
    return total

def layer(x, gain, wq, wk, wv, wup, wout, wdown):
    xf = x.astype(jnp.float32)
    mean = lax.optimization_barrier(jnp.mean(xf, axis=-1, keepdims=True))
    var = jnp.maximum(lax.optimization_barrier(jnp.mean(xf * xf, axis=-1, keepdims=True)) - mean * mean, 0.0)
    normed = ((xf - mean) * lax.rsqrt(var + EPS) * gain.astype(jnp.float32)).astype(jnp.bfloat16)
    query = project(normed, wq).astype(jnp.bfloat16)
    keyed = project(normed, wk).astype(jnp.bfloat16)
    valued = project(normed, wv).astype(jnp.bfloat16)
    act = jax.nn.gelu(project(normed, wup), approximate=False).astype(jnp.bfloat16)
    head_dim = D // HEADS
    shape = (x.shape[0], x.shape[1], HEADS, head_dim)
    qh = query.reshape(shape).astype(jnp.float32)
    kh = keyed.reshape(shape).astype(jnp.float32)
    vh = valued.reshape(shape).astype(jnp.float32)
    scores = jnp.einsum('bqhd,bkhd->bhqk', qh, kh) / jnp.sqrt(jnp.float32(head_dim))
    scores = scores - lax.optimization_barrier(jnp.max(scores, axis=-1, keepdims=True))
    weights = jnp.exp(scores)
    probs = (weights / lax.optimization_barrier(jnp.sum(weights, axis=-1, keepdims=True))).astype(jnp.bfloat16)
    attn = jnp.einsum('bhqk,bkhd->bqhd', probs.astype(jnp.float32), vh)
    attn = attn.reshape(x.shape).astype(jnp.bfloat16)
    mixed = jnp.dot(attn, wout, preferred_element_type=jnp.float32) + jnp.dot(act, wdown, preferred_element_type=jnp.float32)
    return (xf + mixed).astype(jnp.bfloat16)

def reference(tokens, ln_gain, w_query, w_key, w_value, w_up, w_out, w_down):
    current = tokens
    outputs = []
    for level in range(LAYERS):
        current = layer(current, ln_gain[level], w_query[level], w_key[level], w_value[level], w_up[level], w_out[level], w_down[level])
        outputs.append(current)
    return jnp.stack(outputs)
```

```python
import functools
import math

import jax
import jax.numpy as jnp
from jax import lax
from jax.experimental import pallas as pl
from jax.experimental.pallas import tpu as pltpu
from jax.sharding import PartitionSpec as P

D = 6144
HEAD = 128
EPS = 1e-06
NZ = 8
MESH = pl.DeviceIdType.MESH
BF16 = jnp.bfloat16
F32 = jnp.float32


def wide(block):
    return lax.rem(block, 4) == 3


def by_width(block, narrow_size, wide_size, action):
    is_wide = wide(block)

    @pl.when(is_wide)
    def _():
        action(wide_size)

    @pl.when(jnp.logical_not(is_wide))
    def _():
        action(narrow_size)


def layer_kernel(
    n_col, patches, feats,
    x_ref, gain_ref, wq_ref, wk_ref, wv_ref, wup_ref, wout_ref, wdn_ref,
    y_ref,
    w_in, w_mix, gathered, own, stat,
    zs_p, zs_m, zr_p, zr_m, ys_p, ys_m, yr_p, yr_m, pair_s, pair_r, last_s, last_r,
    full, acts, acc, mix_s, mix_r,
    w_sem, ssem, rsem,
):
    row = lax.axis_index("row")
    col = lax.axis_index("col")
    n_row = 2 * NZ
    yb = lax.div(row, NZ)
    z = lax.rem(row, NZ)
    other = 1 - yb

    def around(step):
        return lax.rem(z + step + NZ, NZ)

    up_z = {"row": yb * NZ + around(1)}
    down_z = {"row": yb * NZ + around(-1)}
    pair = {"row": other * NZ + z}

    narrow_in, wide_in = 5 * HEAD, 6 * HEAD
    narrow_mix, wide_mix = 3 * HEAD, 6 * HEAD
    half = n_col // 2 * patches
    quarter = half // 2

    weight_waits = []
    for block in range(NZ):
        if block % 4 == 3:
            start = 6 * 2 * HEAD + (block // 4) * wide_in
            copies_in = [(wup_ref.at[:, start:start + wide_in], 0, wide_in)]
            copies_out = [(wdn_ref.at[start:start + wide_mix], 0, wide_mix)]
        else:
            head = block - block // 4
            cols = slice(head * HEAD, (head + 1) * HEAD)
            start = head * 2 * HEAD
            copies_in = [
                (wq_ref.at[:, cols], 0, HEAD),
                (wk_ref.at[:, cols], HEAD, HEAD),
                (wv_ref.at[:, cols], 2 * HEAD, HEAD),
                (wup_ref.at[:, start:start + 2 * HEAD], 3 * HEAD, 2 * HEAD),
            ]
            copies_out = [
                (wout_ref.at[cols], 0, HEAD),
                (wdn_ref.at[start:start + 2 * HEAD], HEAD, 2 * HEAD),
            ]
        for source, at, size in copies_in:
            copy = pltpu.make_async_copy(source, w_in.at[block, :, at:at + size], w_sem.at[len(weight_waits)])
            copy.start()
            weight_waits.append((copy, 0))
        for source, at, size in copies_out:
            copy = pltpu.make_async_copy(source, w_mix.at[block, at:at + size], w_sem.at[len(weight_waits)])
            copy.start()
            weight_waits.append((copy, 1))

    barrier = pltpu.get_barrier_semaphore()
    for step in range(1, n_row):
        pl.semaphore_signal(barrier, inc=1, device_id={"row": lax.rem(row + step, n_row)}, device_id_type=MESH)
    for step in range(1, n_col):
        pl.semaphore_signal(barrier, inc=1, device_id={"col": lax.rem(col + step, n_col)}, device_id_type=MESH)

    sems = iter(range(1000))
    sent = []

    def remote(source, target, sem, device):
        return pltpu.make_async_remote_copy(
            src_ref=source, dst_ref=target, send_sem=ssem.at[sem], recv_sem=rsem.at[sem],
            device_id=device, device_id_type=MESH,
        )

    xf = x_ref[...].astype(F32).reshape(2 * patches, feats)
    sums = jnp.sum(xf, axis=-1, keepdims=True)
    squares = jnp.sum(xf * xf, axis=-1, keepdims=True)
    columns = jnp.concatenate(
        [jnp.broadcast_to(sums, (2 * patches, 128)), jnp.broadcast_to(squares, (2 * patches, 128))], axis=0
    )
    if 4 * patches < 128:
        columns = jnp.concatenate([columns] * (128 // (4 * patches)), axis=0)
    stat[row] = columns.T[0:8]
    pl.semaphore_wait(barrier, n_row - 1 + n_col - 1)
    stat_copies = []
    for step in range(1, n_row):
        copy = remote(stat.at[row], stat.at[row], next(sems), {"row": lax.rem(row + step, n_row)})
        copy.start()
        stat_copies.append(copy)
    for copy in stat_copies:
        copy.wait()
    mean = jnp.sum(stat[...], axis=0) * (1.0 / D)
    lane = lax.broadcasted_iota(jnp.int32, (8, 128), 1)
    shifted = pltpu.roll(mean, 2 * patches, axis=1)
    var = jnp.maximum(mean - shifted * shifted, 0.0)
    both = jnp.where(lane < 2 * patches, mean, lax.rsqrt(var + EPS))
    back = jnp.broadcast_to(both[0:1], (128, 128)).T
    normed = (xf - back[0:2 * patches, 0:1]) * back[2 * patches:4 * patches, 0:1] * gain_ref[...]
    gathered[:, col] = normed.astype(BF16).reshape(2, patches, feats)
    col_copies = []
    for step in range(1, n_col):
        copy = remote(gathered.at[:, col], gathered.at[:, col], next(sems), {"col": lax.rem(col + step, n_col)})
        copy.start()
        col_copies.append(copy)
    for copy, kind in weight_waits:
        if kind == 0:
            copy.wait()
    for copy in col_copies:
        copy.wait()

    first_up, first_down = next(sems), next(sems)
    early_up, early_down = next(sems), next(sems)
    pair_base = next(sems)
    for _ in range(NZ - 1):
        next(sems)

    def send_in(source, target, sem, device, block):
        by_width(block, narrow_in, wide_in,
                 lambda w: remote(source.at[:, 0:w], target.at[:, 0:w], sem, device).start())

    def recv_in(target, sem, device, block):
        by_width(block, narrow_in, wide_in,
                 lambda w: remote(target.at[:, 0:w], target.at[:, 0:w], sem, device).wait_recv())

    def sent_in(source, sem, device, block):
        by_width(block, narrow_in, wide_in,
                 lambda w: remote(source.at[:, 0:w], source.at[:, 0:w], sem, device).wait_send())


    def order(i):
        away = 4 - lax.div(i + 1, 2)
        return around(jnp.where(lax.rem(i, 2) == 1, away, -away))

    def product(i, carry):
        block = order(i)
        own[block] = jnp.dot(gathered[...].reshape(2 * n_col * patches, feats), w_in[block],
                             preferred_element_type=F32).reshape(2, 2, half, wide_in)
        pair_s[i] = own[block, other, 0].astype(BF16)

        @pl.when(i == 0)
        def _():
            zs_p[0, 0] = own[block, 0, 1].astype(BF16)
            send_in(zs_p.at[0, 0], zr_p.at[0, 0], first_up, up_z, block)
            zs_m[0, 1] = own[block, 1, 1].astype(BF16)
            send_in(zs_m.at[0, 1], zr_m.at[0, 1], first_down, down_z, block)

        @pl.when(i == 1)
        def _():
            zs_p[1, 1] = own[block, 1, 1].astype(BF16)
            send_in(zs_p.at[1, 1], zr_p.at[1, 1], early_up, up_z, block)

        @pl.when(i == 2)
        def _():
            zs_m[1, 0] = own[block, 0, 1].astype(BF16)
            send_in(zs_m.at[1, 0], zr_m.at[1, 0], early_down, down_z, block)

        send_in(pair_s.at[i], pair_r.at[i], pair_base + i, pair, block)
        return carry

    lax.fori_loop(0, NZ, product, 0)
    for i in range(NZ):
        sent.append(lambda i=i: sent_in(pair_s.at[i], pair_base + i, pair, order(jnp.int32(i))))

    def up_block(stage):
        return around(4 - stage)

    def down_block(stage):
        return around(stage - 4)

    up_sem = {(1, 0, 0): first_up, (1, 1, 1): early_up}
    down_sem = {(1, 0, 1): first_down, (1, 1, 0): early_down}
    for key in [(1, 0, 0), (1, 1, 1)]:
        sent.append(lambda key=key: sent_in(zs_p.at[key[1], key[2]], up_sem[key], up_z, up_block(key[1])))
    for key in [(1, 0, 1), (1, 1, 0)]:
        sent.append(lambda key=key: sent_in(zs_m.at[key[1], key[2]], down_sem[key], down_z, down_block(key[1])))

    def mine(which, h, block):
        if which == 1:
            return own[block, h, 1]
        rows = slice(h * quarter, (h + 1) * quarter)
        return own[block, yb, 0, rows]

    def hop(which, stage, h, upward, extra=None):
        send_buf = (zs_p if upward else zs_m) if which == 1 else (ys_p if upward else ys_m)
        recv_buf = (zr_p if upward else zr_m) if which == 1 else (yr_p if upward else yr_m)
        table = up_sem if upward else down_sem
        device = up_z if upward else down_z
        source_device = device
        block = up_block(stage) if upward else down_block(stage)
        value = mine(which, h, block) if extra is None else extra
        first_half = 0 if upward else 1
        has_arrival = stage >= 2 or (stage == 1 and h == first_half)
        if has_arrival:
            recv_in(recv_buf.at[stage - 1, h], table[(which, stage - 1, h)], source_device, block)
            value = value + recv_buf[stage - 1, h].astype(F32)
        send_buf[stage, h] = value.astype(BF16)
        sem = next(sems)
        table[(which, stage, h)] = sem
        send_in(send_buf.at[stage, h], recv_buf.at[stage, h], sem, device, block)
        sent.append(lambda: sent_in(send_buf.at[stage, h], sem, device, block))

    hop(1, 1, 0, True)
    hop(1, 1, 1, False)

    def pair_sum(i):
        block = order(jnp.int32(i))
        recv_in(pair_r.at[i], pair_base + i, pair, block)
        own[block, yb, 0] = own[block, yb, 0] + pair_r[i].astype(F32)

    for stage in (2, 3):
        hop(1, stage, 1, True)
        hop(1, stage, 0, False)
        if stage == 2:
            pair_sum(0)
            hop(0, 0, 0, True)
            hop(0, 0, 1, False)
        hop(1, stage, 0, True)
        hop(1, stage, 1, False)
        if stage == 2:
            pair_sum(1)
            hop(0, 1, 1, True)
            pair_sum(2)
            hop(0, 1, 0, False)
    hop(0, 1, 0, True)
    hop(0, 1, 1, False)
    pair_sum(3)
    hop(0, 2, 1, True)
    pair_sum(4)
    hop(0, 2, 0, False)
    for h in (1, 0):
        recv_in(zr_p.at[3, h], up_sem[(1, 3, h)], up_z, z)
        recv_in(zr_m.at[3, h], down_sem[(1, 3, h)], down_z, z)
    last_s[...] = (own[z, other, 1] + zr_p[3, other].astype(F32) + zr_m[3, other].astype(F32)).astype(BF16)
    last_sem = next(sems)
    send_in(last_s, last_r, last_sem, pair, z)
    sent.append(lambda: sent_in(last_s, last_sem, pair, z))
    hop(0, 2, 0, True)
    hop(0, 2, 1, False)
    pair_sum(5)
    hop(0, 3, 1, True)
    pair_sum(6)
    hop(0, 3, 0, False)
    hop(0, 3, 0, True)
    hop(0, 3, 1, False)
    full[half:2 * half] = own[z, yb, 1] + zr_p[3, yb].astype(F32) + zr_m[3, yb].astype(F32)
    recv_in(last_r, last_sem, pair, z)
    full[half:2 * half] = full[half:2 * half] + last_r[...].astype(F32)
    pair_sum(7)
    for h in (1, 0):
        recv_in(yr_p.at[3, h], up_sem[(0, 3, h)], up_z, z)
        recv_in(yr_m.at[3, h], down_sem[(0, 3, h)], down_z, z)
    for h in (0, 1):
        full[h * quarter:(h + 1) * quarter] = (
            own[z, yb, 0, h * quarter:(h + 1) * quarter] + yr_p[3, h].astype(F32) + yr_m[3, h].astype(F32)
        )

    def gelu(value):
        return (0.5 * value * (1.0 + lax.erf(value * math.sqrt(0.5)))).astype(BF16)

    def hidden(size):
        acts[yb, z, :, 0:size] = gelu(full[:, 0:size])

    def attention(size):
        acts[yb, z, :, HEAD:size] = gelu(full[:, 3 * HEAD:5 * HEAD])
        query = full[:, 0:HEAD].astype(BF16)
        keyed = full[:, HEAD:2 * HEAD].astype(BF16)
        valued = full[:, 2 * HEAD:3 * HEAD].astype(BF16)
        scores = lax.dot_general(query, keyed, (((1,), (1,)), ((), ())), preferred_element_type=F32)
        scores = scores * (1.0 / math.sqrt(HEAD))
        expo = jnp.exp(scores - jnp.max(scores, axis=-1, keepdims=True))
        probs = (expo / jnp.sum(expo, axis=-1, keepdims=True)).astype(BF16)
        acts[yb, z, :, 0:HEAD] = jnp.dot(probs, valued, preferred_element_type=F32).astype(BF16)

    is_wide = wide(z)
    pl.when(is_wide)(lambda: hidden(wide_mix))
    pl.when(jnp.logical_not(is_wide))(lambda: attention(narrow_mix))

    def view(image, block, lo, hi, w):
        return acts.at[image, block, lo:hi, 0:w]

    def send_act(image, block, lo, hi, sem, device):
        by_width(block, narrow_mix, wide_mix, lambda w: remote(
            view(image, block, lo, hi, w), view(image, block, lo, hi, w), sem, device).start())
        sent.append(lambda: by_width(block, narrow_mix, wide_mix, lambda w: remote(
            view(image, block, lo, hi, w), view(image, block, lo, hi, w), sem, device).wait_send()))

    def recv_act(image, block, lo, hi, sem, device):
        by_width(block, narrow_mix, wide_mix, lambda w: remote(
            view(image, block, lo, hi, w), view(image, block, lo, hi, w), sem, device).wait_recv())

    images = [yb, other, yb]
    spans = [(0, half), (0, half), (half, 2 * half)]
    gather_sem = {}

    def pass_on(stage, stream, upward):
        lo, hi = spans[stream]
        if stage == 3:
            mid = lo + quarter
            lo, hi = (lo, mid) if upward else (mid, hi)
        block = around(-stage) if upward else around(stage)
        sem = next(sems)
        gather_sem[(stage, stream, upward)] = sem
        send_act(images[stream], block, lo, hi, sem, up_z if upward else down_z)

    def arrived(stage, stream, upward):
        lo, hi = spans[stream]
        if stage == 3:
            mid = lo + quarter
            lo, hi = (lo, mid) if upward else (mid, hi)
        block = around(-1 - stage) if upward else around(1 + stage)
        recv_act(images[stream], block, lo, hi, gather_sem[(stage, stream, upward)], up_z if upward else down_z)
        return block, lo, hi

    pair_first = next(sems)
    send_act(yb, z, 0, half, pair_first, pair)
    for stream in (0, 2):
        pass_on(0, stream, True)
        pass_on(0, stream, False)
    pair_waits = []
    own_sem = next(sems)
    send_act(yb, z, half, 2 * half, own_sem, pair)
    pair_waits.append((z, half, 2 * half, own_sem))
    recv_act(other, z, 0, half, pair_first, pair)
    pass_on(0, 1, True)
    pass_on(0, 1, False)

    for copy, kind in weight_waits:
        if kind == 1:
            copy.wait()

    def add_product(image, block, lo, hi):
        def add(w):
            acc[image, lo:hi] = acc[image, lo:hi] + jnp.dot(
                acts[image, block, lo:hi, 0:w], w_mix[block, 0:w], preferred_element_type=F32)
        by_width(block, narrow_mix, wide_mix, add)

    def add_block(block):
        add_product(0, block, 0, 2 * half)
        add_product(1, block, 0, 2 * half)

    acc[...] = jnp.zeros_like(acc)
    for stage in range(4):
        for stream in (0, 2, 1):
            for upward in (True, False):
                block, lo, hi = arrived(stage, stream, upward)
                if stage < 3:
                    pass_on(stage + 1, stream, upward)
                if stream == 2:
                    sem = next(sems)
                    send_act(yb, block, lo, hi, sem, pair)
                    pair_waits.append((block, lo, hi, sem))
    for block, lo, hi, sem in pair_waits:
        recv_act(other, block, lo, hi, sem, pair)

    def block_products(i, carry):
        add_block(i)
        return carry

    lax.fori_loop(0, NZ, block_products, 0)

    mix_s[...] = acc[...].astype(BF16).reshape(2, n_col, patches, feats)
    mix_copies = []
    for step in range(1, n_col):
        target = lax.rem(col + step, n_col)
        copy = remote(mix_s.at[:, target], mix_r.at[step - 1], next(sems), {"col": target})
        copy.start()
        mix_copies.append(copy)
    total = x_ref[...].astype(F32) + mix_s[:, col].astype(F32)
    for step, copy in enumerate(mix_copies):
        copy.wait()
        total = total + mix_r[step].astype(F32)
    y_ref[...] = total.astype(BF16)
    for wait in sent:
        wait()


def layer(x, weights):
    gain, wq, wk, wv, wup, wout, wdown = weights
    n_col = lax.axis_size("col")
    images, patches, feats = x.shape
    half = n_col // 2 * patches
    wide_in = 6 * HEAD
    vmem = pl.BlockSpec(memory_space=pltpu.VMEM)
    anywhere = pl.BlockSpec(memory_space=pl.ANY)
    z_buf = pltpu.VMEM((4, 2, half, wide_in), BF16)
    y_buf = pltpu.VMEM((4, 2, half // 2, wide_in), BF16)
    pair_buf = pltpu.VMEM((NZ, half, wide_in), BF16)
    scratch = [
        pltpu.VMEM((NZ, feats, wide_in), BF16),
        pltpu.VMEM((NZ, wide_in, feats), BF16),
        pltpu.VMEM((2, n_col, patches, feats), BF16),
        pltpu.VMEM((NZ, 2, 2, half, wide_in), F32),
        pltpu.VMEM((2 * NZ, 8, 128), F32),
        z_buf, z_buf, z_buf, z_buf, y_buf, y_buf, y_buf, y_buf, pair_buf, pair_buf,
        pltpu.VMEM((half, wide_in), BF16), pltpu.VMEM((half, wide_in), BF16),
        pltpu.VMEM((2 * half, wide_in), F32),
        pltpu.VMEM((2, NZ, 2 * half, wide_in), BF16),
        pltpu.VMEM((2, 2 * half, feats), F32),
        pltpu.VMEM((2, n_col, patches, feats), BF16),
        pltpu.VMEM((n_col - 1, 2, patches, feats), BF16),
        pltpu.SemaphoreType.DMA((40,)),
        pltpu.SemaphoreType.DMA((128,)),
        pltpu.SemaphoreType.DMA((128,)),
    ]
    return pl.pallas_call(
        functools.partial(layer_kernel, n_col, patches, feats),
        out_shape=jax.ShapeDtypeStruct(x.shape, BF16),
        in_specs=[vmem, vmem] + [anywhere] * 6,
        out_specs=vmem,
        scratch_shapes=scratch,
        compiler_params=pltpu.CompilerParams(
            collective_id=0, has_side_effects=True, vmem_limit_bytes=60 * 1024 * 1024
        ),
    )(x, gain[None], wq, wk, wv, wup, wout, wdown)


def local(tokens, ln_gain, w_query, w_key, w_value, w_up, w_out, w_down):
    weights = (ln_gain[0], w_query[0], w_key[0], w_value[0], w_up[0], w_out[0], w_down[0])
    section = lax.axis_index("section")
    sections = lax.axis_size("section")
    result = jnp.zeros_like(tokens)
    current = tokens
    for tick in range(sections):
        output = layer(current, weights)
        result = jnp.where(section == tick, output, result)
        if tick + 1 < sections:
            current = lax.ppermute(output, "section", [(s, s + 1) for s in range(sections - 1)])
    return result[None]


def solution(mesh):
    return jax.shard_map(
        local,
        mesh=mesh,
        in_specs=(
            P(None, "col", "row"),
            P("section", "row"),
            P("section", "row", "col"),
            P("section", "row", "col"),
            P("section", "row", "col"),
            P("section", "row", "col"),
            P("section", "col", "row"),
            P("section", "col", "row"),
        ),
        out_specs=P("section", None, "col", "row"),
        check_vma=False,
    )
```

```python
import functools
import math

import jax
import jax.numpy as jnp
from jax import lax
from jax.experimental import pallas as pl
from jax.experimental.pallas import tpu as pltpu
from jax.sharding import PartitionSpec as P

D = 6144
HEAD = 128
EPS = 1e-06
NZ = 8
MESH = pl.DeviceIdType.MESH
BF16 = jnp.bfloat16
F32 = jnp.float32


def wide(block):
    return lax.rem(block, 4) == 3


def by_width(block, narrow_size, wide_size, action):
    is_wide = wide(block)

    @pl.when(is_wide)
    def _():
        action(wide_size)

    @pl.when(jnp.logical_not(is_wide))
    def _():
        action(narrow_size)


def layers_kernel(
    n_col, patches, feats,
    x_ref, gain_ref, wq_ref, wk_ref, wv_ref, wup_ref, wout_ref, wdn_ref,
    y_ref,
    w_in, w_mix, gathered, own, stat,
    zs_p, zs_m, zr_p, zr_m, ys_p, ys_m, yr_p, yr_m, pair_s, pair_r, last_s, last_r,
    full, acts, acc, mix_s, mix_r,
    w1_in, w1_mix, gain1, xb1, gathered1, own1, stat1, zs1_p, zs1_m, zr1_p, zr1_m,
    acts1, acc1, mix1_s, mix1_r, ys1, yr1,
    w_sem, ssem, rsem,
):
    section = lax.axis_index("section")
    row = lax.axis_index("row")
    col = lax.axis_index("col")
    n_row = 2 * NZ
    yb = lax.div(row, NZ)
    z = lax.rem(row, NZ)
    other = 1 - yb

    def around(step):
        return lax.rem(z + step + NZ, NZ)

    up_z = {"row": yb * NZ + around(1)}
    down_z = {"row": yb * NZ + around(-1)}
    pair = {"row": other * NZ + z}
    outer = {"section": 1 - section, "row": other * NZ + z}
    diagonal = {"section": 1 - section, "row": row}
    in_first = section == 0
    in_second = section == 1

    narrow_in, wide_in = 5 * HEAD, 6 * HEAD
    narrow_mix, wide_mix = 3 * HEAD, 6 * HEAD
    half = n_col // 2 * patches
    quarter = half // 2

    barrier = pltpu.get_barrier_semaphore()
    for step in range(1, n_row):
        pl.semaphore_signal(barrier, inc=1, device_id={"row": lax.rem(row + step, n_row)}, device_id_type=MESH)
    for step in range(1, n_col):
        pl.semaphore_signal(barrier, inc=1, device_id={"col": lax.rem(col + step, n_col)}, device_id_type=MESH)
    for device in (outer, diagonal):
        pl.semaphore_signal(barrier, inc=1, device_id=device, device_id_type=MESH)

    sems = iter(range(1000))

    def remote(source, target, sem, device):
        return pltpu.make_async_remote_copy(
            src_ref=source, dst_ref=target, send_sem=ssem.at[sem], recv_sem=rsem.at[sem],
            device_id=device, device_id_type=MESH,
        )

    def ready():
        pl.semaphore_wait(barrier, n_row - 1 + n_col - 1 + 2)

    def column_stats(sums, squares):
        columns = jnp.concatenate(
            [jnp.broadcast_to(sums, (2 * patches, 128)), jnp.broadcast_to(squares, (2 * patches, 128))], axis=0
        )
        return columns.T[0:8]

    def mean_and_scale(total):
        mean = total * (1.0 / D)
        lane = lax.broadcasted_iota(jnp.int32, (8, 128), 1)
        shifted = pltpu.roll(mean, 2 * patches, axis=1)
        var = jnp.maximum(mean - shifted * shifted, 0.0)
        both = jnp.where(lane < 2 * patches, mean, lax.rsqrt(var + EPS))
        back = jnp.broadcast_to(both[0:1], (128, 128)).T
        return back[0:2 * patches, 0:1], back[2 * patches:4 * patches, 0:1]

    def gelu(value):
        return (0.5 * value * (1.0 + lax.erf(value * math.sqrt(0.5)))).astype(BF16)

    def attend(query, keyed, valued):
        scores = lax.dot_general(query, keyed, (((1,), (1,)), ((), ())), preferred_element_type=F32)
        scores = scores * (1.0 / math.sqrt(HEAD))
        expo = jnp.exp(scores - jnp.max(scores, axis=-1, keepdims=True))
        probs = (expo / jnp.sum(expo, axis=-1, keepdims=True)).astype(BF16)
        return jnp.dot(probs, valued, preferred_element_type=F32).astype(BF16)

    group = feats
    block_sems = {name: [next(sems) for _ in range(n)] for name, n in
                  (("pair", 5), ("outer", 5), ("via", 5), ("forward", 5), ("gain", 3))}
    mlp_first = 2 * group
    mlp_rest = 3 * group

    def head_cols(member, j):
        return pl.ds(pl.multiple_of((member * 3 + j) * HEAD, HEAD), HEAD)

    def third(at, g):
        return w_in.at[at + g // 2, :, (g % 2) * group:(g % 2 + 1) * group]

    @pl.when(in_second)
    def ship():
        copies = []

        def fetch(source, target):
            copy = pltpu.make_async_copy(source, target, w_sem.at[len(copies)])
            copy.start()
            copies.append(copy)

        start = pl.multiple_of(mlp_first + yb * mlp_rest, group)
        fetch(wup_ref.at[:, pl.ds(start, 2 * group)], w_in.at[4])
        fetch(wup_ref.at[:, pl.ds(pl.multiple_of(start + 2 * group, group), group)], w_in.at[5, :, 0:group])
        fetch(wdn_ref.at[pl.ds(start, 2 * group)], w_mix.at[3])
        fetch(wdn_ref.at[pl.ds(pl.multiple_of(start + 2 * group, group), group)], w_mix.at[4, 0:group])
        n_via = len(copies)
        start = pl.multiple_of(mlp_first + other * mlp_rest, group)
        fetch(wup_ref.at[:, pl.ds(start, 2 * group)], w_in.at[2])
        fetch(wup_ref.at[:, pl.ds(pl.multiple_of(start + 2 * group, group), group)], w_in.at[3, :, 0:group])
        fetch(wdn_ref.at[pl.ds(start, 2 * group)], w_mix.at[1])
        fetch(wdn_ref.at[pl.ds(pl.multiple_of(start + 2 * group, group), group)], w_mix.at[2, 0:group])
        n_outer = len(copies)
        for member, mine in ((other, False), (yb, True)):
            for j in range(3):
                for k, w_ref in enumerate((wq_ref, wk_ref, wv_ref)):
                    span = slice(k * HEAD, (k + 1) * HEAD)
                    at = (j % 2) * group + k * HEAD
                    target = w1_in.at[j, yb, :, span] if mine else w_in.at[j // 2, :, at:at + HEAD]
                    fetch(w_ref.at[:, head_cols(member, j)], target)
            rows = pl.ds(pl.multiple_of(member * group, group), group)
            fetch(wup_ref.at[:, rows], w1_in.at[3, yb] if mine else w_in.at[1, :, group:2 * group])
            fetch(wout_ref.at[rows], w1_mix.at[yb, 0:group] if mine else w_mix.at[0, 0:group])
            fetch(wdn_ref.at[rows], w1_mix.at[yb, group:2 * group] if mine else w_mix.at[0, group:2 * group])
            if not mine:
                n_pair = len(copies)
        gain1[yb] = jnp.broadcast_to(gain_ref[...], (8, feats))
        ready()
        out = []

        def send(source, target, sem, device):
            copy = remote(source, target, sem, device)
            copy.start()
            out.append(copy)

        for copy in copies[:n_via]:
            copy.wait()
        for g in range(3):
            send(third(4, g), third(6, g), block_sems["via"][g], pair)
        send(w_mix.at[3], w_mix.at[5], block_sems["via"][3], pair)
        send(w_mix.at[4, 0:group], w_mix.at[6, 0:group], block_sems["via"][4], pair)
        for copy in copies[n_via:n_outer]:
            copy.wait()
        for g in range(3):
            send(third(2, g), w1_in.at[g, yb], block_sems["outer"][g], outer)
        send(w_mix.at[1], w1_mix.at[yb, 0:2 * group], block_sems["outer"][3], outer)
        send(w_mix.at[2, 0:group], w1_mix.at[yb, 2 * group:3 * group], block_sems["outer"][4], outer)
        for copy in copies[n_outer:n_pair]:
            copy.wait()
        for g in range(4):
            send(third(0, g), w1_in.at[g, yb], block_sems["pair"][g], pair)
        send(w_mix.at[0], w1_mix.at[yb, 0:2 * group], block_sems["pair"][4], pair)
        for device, sem in zip((pair, outer, diagonal), block_sems["gain"]):
            send(gain1.at[yb], gain1.at[yb], sem, device)
        for g in range(3):
            remote(third(6, g), third(6, g), block_sems["via"][g], pair).wait_recv()
            send(third(6, g), w1_in.at[g, other], block_sems["forward"][g], outer)
        remote(w_mix.at[5], w_mix.at[5], block_sems["via"][3], pair).wait_recv()
        send(w_mix.at[5], w1_mix.at[other, 0:2 * group], block_sems["forward"][3], outer)
        remote(w_mix.at[6, 0:group], w_mix.at[6, 0:group], block_sems["via"][4], pair).wait_recv()
        send(w_mix.at[6, 0:group], w1_mix.at[other, 2 * group:3 * group], block_sems["forward"][4], outer)
        for copy in copies[n_pair:]:
            copy.wait()
        for g in range(4):
            remote(w1_in.at[g, other], w1_in.at[g, other], block_sems["pair"][g], pair).wait_recv()
        remote(w1_mix.at[other, 0:2 * group], w1_mix.at[other, 0:2 * group], block_sems["pair"][4], pair).wait_recv()
        remote(gain1.at[other], gain1.at[other], block_sems["gain"][0], pair).wait_recv()
        for copy in out:
            copy.wait_send()

    def first_layer():
        sent = []
        weight_waits = []
        for block in range(NZ):
            if block % 4 == 3:
                start = 6 * 2 * HEAD + (block // 4) * wide_in
                copies_in = [(wup_ref.at[:, start:start + wide_in], 0, wide_in)]
                copies_out = [(wdn_ref.at[start:start + wide_mix], 0, wide_mix)]
            else:
                head = block - block // 4
                cols = slice(head * HEAD, (head + 1) * HEAD)
                start = head * 2 * HEAD
                copies_in = [
                    (wq_ref.at[:, cols], 0, HEAD),
                    (wk_ref.at[:, cols], HEAD, HEAD),
                    (wv_ref.at[:, cols], 2 * HEAD, HEAD),
                    (wup_ref.at[:, start:start + 2 * HEAD], 3 * HEAD, 2 * HEAD),
                ]
                copies_out = [
                    (wout_ref.at[cols], 0, HEAD),
                    (wdn_ref.at[start:start + 2 * HEAD], HEAD, 2 * HEAD),
                ]
            for source, at, size in copies_in:
                copy = pltpu.make_async_copy(source, w_in.at[block, :, at:at + size], w_sem.at[len(weight_waits)])
                copy.start()
                weight_waits.append((copy, 0))
            for source, at, size in copies_out:
                copy = pltpu.make_async_copy(source, w_mix.at[block, at:at + size], w_sem.at[len(weight_waits)])
                copy.start()
                weight_waits.append((copy, 1))

        xf = x_ref[...].astype(F32).reshape(2 * patches, feats)
        sums = jnp.sum(xf, axis=-1, keepdims=True)
        squares = jnp.sum(xf * xf, axis=-1, keepdims=True)
        stat[row] = column_stats(sums, squares)
        ready()
        stat_copies = []
        for step in range(1, n_row):
            copy = remote(stat.at[row], stat.at[row], next(sems), {"row": lax.rem(row + step, n_row)})
            copy.start()
            stat_copies.append(copy)
        for copy in stat_copies:
            copy.wait()
        mean, scale = mean_and_scale(jnp.sum(stat[...], axis=0))
        normed = (xf - mean) * scale * gain_ref[...]
        gathered[:, col] = normed.astype(BF16).reshape(2, patches, feats)
        col_copies = []
        for step in range(1, n_col):
            copy = remote(gathered.at[:, col], gathered.at[:, col], next(sems), {"col": lax.rem(col + step, n_col)})
            copy.start()
            col_copies.append(copy)
        for copy, kind in weight_waits:
            if kind == 0:
                copy.wait()
        for copy in col_copies:
            copy.wait()

        first_up, first_down = next(sems), next(sems)
        early_up, early_down = next(sems), next(sems)
        pair_base = next(sems)
        for _ in range(NZ - 1):
            next(sems)

        def send_in(source, target, sem, device, block):
            by_width(block, narrow_in, wide_in,
                     lambda w: remote(source.at[:, 0:w], target.at[:, 0:w], sem, device).start())

        def recv_in(target, sem, device, block):
            by_width(block, narrow_in, wide_in,
                     lambda w: remote(target.at[:, 0:w], target.at[:, 0:w], sem, device).wait_recv())

        def sent_in(source, sem, device, block):
            by_width(block, narrow_in, wide_in,
                     lambda w: remote(source.at[:, 0:w], source.at[:, 0:w], sem, device).wait_send())


        def order(i):
            away = 4 - lax.div(i + 1, 2)
            return around(jnp.where(lax.rem(i, 2) == 1, away, -away))

        def product(i, carry):
            block = order(i)
            own[block] = jnp.dot(gathered[...].reshape(2 * n_col * patches, feats), w_in[block],
                                 preferred_element_type=F32).reshape(2, 2, half, wide_in)
            pair_s[i] = own[block, other, 0].astype(BF16)

            @pl.when(i == 0)
            def _():
                zs_p[0, 0] = own[block, 0, 1].astype(BF16)
                send_in(zs_p.at[0, 0], zr_p.at[0, 0], first_up, up_z, block)
                zs_m[0, 1] = own[block, 1, 1].astype(BF16)
                send_in(zs_m.at[0, 1], zr_m.at[0, 1], first_down, down_z, block)

            @pl.when(i == 1)
            def _():
                zs_p[1, 1] = own[block, 1, 1].astype(BF16)
                send_in(zs_p.at[1, 1], zr_p.at[1, 1], early_up, up_z, block)

            @pl.when(i == 2)
            def _():
                zs_m[1, 0] = own[block, 0, 1].astype(BF16)
                send_in(zs_m.at[1, 0], zr_m.at[1, 0], early_down, down_z, block)

            send_in(pair_s.at[i], pair_r.at[i], pair_base + i, pair, block)
            return carry

        lax.fori_loop(0, NZ, product, 0)
        for i in range(NZ):
            sent.append(lambda i=i: sent_in(pair_s.at[i], pair_base + i, pair, order(jnp.int32(i))))

        def up_block(stage):
            return around(4 - stage)

        def down_block(stage):
            return around(stage - 4)

        up_sem = {(1, 0, 0): first_up, (1, 1, 1): early_up}
        down_sem = {(1, 0, 1): first_down, (1, 1, 0): early_down}
        for key in [(1, 0, 0), (1, 1, 1)]:
            sent.append(lambda key=key: sent_in(zs_p.at[key[1], key[2]], up_sem[key], up_z, up_block(key[1])))
        for key in [(1, 0, 1), (1, 1, 0)]:
            sent.append(lambda key=key: sent_in(zs_m.at[key[1], key[2]], down_sem[key], down_z, down_block(key[1])))

        def mine(which, h, block):
            if which == 1:
                return own[block, h, 1]
            rows = slice(h * quarter, (h + 1) * quarter)
            return own[block, yb, 0, rows]

        def hop(which, stage, h, upward, extra=None):
            send_buf = (zs_p if upward else zs_m) if which == 1 else (ys_p if upward else ys_m)
            recv_buf = (zr_p if upward else zr_m) if which == 1 else (yr_p if upward else yr_m)
            table = up_sem if upward else down_sem
            device = up_z if upward else down_z
            source_device = device
            block = up_block(stage) if upward else down_block(stage)
            value = mine(which, h, block) if extra is None else extra
            first_half = 0 if upward else 1
            has_arrival = stage >= 2 or (stage == 1 and h == first_half)
            if has_arrival:
                recv_in(recv_buf.at[stage - 1, h], table[(which, stage - 1, h)], source_device, block)
                value = value + recv_buf[stage - 1, h].astype(F32)
            send_buf[stage, h] = value.astype(BF16)
            sem = next(sems)
            table[(which, stage, h)] = sem
            send_in(send_buf.at[stage, h], recv_buf.at[stage, h], sem, device, block)
            sent.append(lambda: sent_in(send_buf.at[stage, h], sem, device, block))

        hop(1, 1, 0, True)
        hop(1, 1, 1, False)

        def pair_sum(i):
            block = order(jnp.int32(i))
            recv_in(pair_r.at[i], pair_base + i, pair, block)
            own[block, yb, 0] = own[block, yb, 0] + pair_r[i].astype(F32)

        for stage in (2, 3):
            hop(1, stage, 1, True)
            hop(1, stage, 0, False)
            if stage == 2:
                pair_sum(0)
                hop(0, 0, 0, True)
                hop(0, 0, 1, False)
            hop(1, stage, 0, True)
            hop(1, stage, 1, False)
            if stage == 2:
                pair_sum(1)
                hop(0, 1, 1, True)
                pair_sum(2)
                hop(0, 1, 0, False)
        hop(0, 1, 0, True)
        hop(0, 1, 1, False)
        pair_sum(3)
        hop(0, 2, 1, True)
        pair_sum(4)
        hop(0, 2, 0, False)
        for h in (1, 0):
            recv_in(zr_p.at[3, h], up_sem[(1, 3, h)], up_z, z)
            recv_in(zr_m.at[3, h], down_sem[(1, 3, h)], down_z, z)
        last_s[...] = (own[z, other, 1] + zr_p[3, other].astype(F32) + zr_m[3, other].astype(F32)).astype(BF16)
        last_sem = next(sems)
        send_in(last_s, last_r, last_sem, pair, z)
        sent.append(lambda: sent_in(last_s, last_sem, pair, z))
        hop(0, 2, 0, True)
        hop(0, 2, 1, False)
        pair_sum(5)
        hop(0, 3, 1, True)
        pair_sum(6)
        hop(0, 3, 0, False)
        hop(0, 3, 0, True)
        hop(0, 3, 1, False)
        full[half:2 * half] = own[z, yb, 1] + zr_p[3, yb].astype(F32) + zr_m[3, yb].astype(F32)
        recv_in(last_r, last_sem, pair, z)
        full[half:2 * half] = full[half:2 * half] + last_r[...].astype(F32)
        pair_sum(7)
        for h in (1, 0):
            recv_in(yr_p.at[3, h], up_sem[(0, 3, h)], up_z, z)
            recv_in(yr_m.at[3, h], down_sem[(0, 3, h)], down_z, z)
        for h in (0, 1):
            full[h * quarter:(h + 1) * quarter] = (
                own[z, yb, 0, h * quarter:(h + 1) * quarter] + yr_p[3, h].astype(F32) + yr_m[3, h].astype(F32)
            )

        def hidden(size):
            acts[yb, z, :, 0:size] = gelu(full[:, 0:size])

        def attention(size):
            acts[yb, z, :, HEAD:size] = gelu(full[:, 3 * HEAD:5 * HEAD])
            acts[yb, z, :, 0:HEAD] = attend(
                full[:, 0:HEAD].astype(BF16), full[:, HEAD:2 * HEAD].astype(BF16), full[:, 2 * HEAD:3 * HEAD].astype(BF16)
            )

        is_wide = wide(z)
        pl.when(is_wide)(lambda: hidden(wide_mix))
        pl.when(jnp.logical_not(is_wide))(lambda: attention(narrow_mix))

        def view(image, block, lo, hi, w):
            return acts.at[image, block, lo:hi, 0:w]

        def send_act(image, block, lo, hi, sem, device):
            by_width(block, narrow_mix, wide_mix, lambda w: remote(
                view(image, block, lo, hi, w), view(image, block, lo, hi, w), sem, device).start())
            sent.append(lambda: by_width(block, narrow_mix, wide_mix, lambda w: remote(
                view(image, block, lo, hi, w), view(image, block, lo, hi, w), sem, device).wait_send()))

        def recv_act(image, block, lo, hi, sem, device):
            by_width(block, narrow_mix, wide_mix, lambda w: remote(
                view(image, block, lo, hi, w), view(image, block, lo, hi, w), sem, device).wait_recv())

        images = [yb, other, yb]
        spans = [(0, half), (0, half), (half, 2 * half)]
        gather_sem = {}

        def pass_on(stage, stream, upward):
            lo, hi = spans[stream]
            if stage == 3:
                mid = lo + quarter
                lo, hi = (lo, mid) if upward else (mid, hi)
            block = around(-stage) if upward else around(stage)
            sem = next(sems)
            gather_sem[(stage, stream, upward)] = sem
            send_act(images[stream], block, lo, hi, sem, up_z if upward else down_z)

        def arrived(stage, stream, upward):
            lo, hi = spans[stream]
            if stage == 3:
                mid = lo + quarter
                lo, hi = (lo, mid) if upward else (mid, hi)
            block = around(-1 - stage) if upward else around(1 + stage)
            recv_act(images[stream], block, lo, hi, gather_sem[(stage, stream, upward)], up_z if upward else down_z)
            return block, lo, hi

        pair_first = next(sems)
        send_act(yb, z, 0, half, pair_first, pair)
        for stream in (0, 2):
            pass_on(0, stream, True)
            pass_on(0, stream, False)
        pair_waits = []
        own_sem = next(sems)
        send_act(yb, z, half, 2 * half, own_sem, pair)
        pair_waits.append((z, half, 2 * half, own_sem))
        recv_act(other, z, 0, half, pair_first, pair)
        pass_on(0, 1, True)
        pass_on(0, 1, False)

        for copy, kind in weight_waits:
            if kind == 1:
                copy.wait()

        def add_product(image, block, lo, hi):
            def add(w):
                acc[image, lo:hi] = acc[image, lo:hi] + jnp.dot(
                    acts[image, block, lo:hi, 0:w], w_mix[block, 0:w], preferred_element_type=F32)
            by_width(block, narrow_mix, wide_mix, add)

        def add_block(block):
            add_product(0, block, 0, 2 * half)
            add_product(1, block, 0, 2 * half)

        acc[...] = jnp.zeros_like(acc)
        for stage in range(4):
            for stream in (0, 2, 1):
                for upward in (True, False):
                    block, lo, hi = arrived(stage, stream, upward)
                    if stage < 3:
                        pass_on(stage + 1, stream, upward)
                    if stream == 2:
                        sem = next(sems)
                        send_act(yb, block, lo, hi, sem, pair)
                        pair_waits.append((block, lo, hi, sem))
        for block, lo, hi, sem in pair_waits:
            recv_act(other, block, lo, hi, sem, pair)

        def block_products(i, carry):
            add_block(i)
            return carry

        lax.fori_loop(0, NZ, block_products, 0)

        mix_s[...] = acc[...].astype(BF16).reshape(2, n_col, patches, feats)
        mix_copies = []
        for step in range(1, n_col):
            target = lax.rem(col + step, n_col)
            copy = remote(mix_s.at[:, target], mix_r.at[step - 1], next(sems), {"col": target})
            copy.start()
            mix_copies.append(copy)
        total = x_ref[...].astype(F32) + mix_s[:, col].astype(F32)
        for step, copy in enumerate(mix_copies):
            copy.wait()
            total = total + mix_r[step].astype(F32)
        y_ref[...] = total.astype(BF16)
        xb1[yb] = total.astype(BF16)
        for device, sem in ((pair, spread[0]), (outer, spread[1]), (diagonal, spread[2])):
            copy = remote(xb1.at[yb], xb1.at[yb], sem, device)
            copy.start()
            sent.append(copy.wait_send)
        for wait in sent:
            wait()
        for g in range(3):
            remote(w1_in.at[g, other], w1_in.at[g, other], block_sems["outer"][g], outer).wait_recv()
            remote(w1_in.at[g, yb], w1_in.at[g, yb], block_sems["forward"][g], outer).wait_recv()
        for half_k, name in ((other, "outer"), (yb, "forward")):
            for k, (lo, hi) in ((3, (0, 2 * group)), (4, (2 * group, 3 * group))):
                part = w1_mix.at[half_k, lo:hi]
                remote(part, part, block_sems[name][k], outer).wait_recv()
        remote(gain1.at[other], gain1.at[other], block_sems["gain"][1], outer).wait_recv()
        remote(gain1.at[yb], gain1.at[yb], block_sems["gain"][2], diagonal).wait_recv()
        remote(xb1.at[other], xb1.at[other], spread[0], pair).wait_recv()

    spread = [next(sems) for _ in range(3)]
    pl.when(in_first)(first_layer)

    @pl.when(in_second)
    def _():
        remote(xb1.at[other], xb1.at[other], spread[1], outer).wait_recv()
        remote(xb1.at[yb], xb1.at[yb], spread[2], diagonal).wait_recv()

    sent = []
    n_tok = 2 * n_col * patches
    both = xb1[...].astype(F32).reshape(2, 2 * patches, feats)
    sums = jnp.sum(jnp.sum(both, axis=-1, keepdims=True), axis=0)
    squares = jnp.sum(jnp.sum(both * both, axis=-1, keepdims=True), axis=0)
    stat1[z] = column_stats(sums, squares)
    copies = []
    for step in range(1, NZ):
        copy = remote(stat1.at[z], stat1.at[z], next(sems), {"row": yb * NZ + around(step)})
        copy.start()
        copies.append(copy)
    for copy in copies:
        copy.wait()
    mean, scale = mean_and_scale(jnp.sum(stat1[...], axis=0))
    for k in range(2):
        normed = (both[k] - mean) * scale * gain1[k, 0:1]
        gathered1[k, :, col] = normed.astype(BF16).reshape(2, patches, feats)
    copies = []
    for step in range(1, n_col):
        copy = remote(gathered1.at[:, :, col], gathered1.at[:, :, col], next(sems), {"col": lax.rem(col + step, n_col)})
        copy.start()
        copies.append(copy)
    for copy in copies:
        copy.wait()

    half_rows = 4 * patches
    short_rows = 3 * patches

    def partial_product(g):
        return (
            jnp.dot(gathered1[0].reshape(n_tok, feats), w1_in[g, 0], preferred_element_type=F32)
            + jnp.dot(gathered1[1].reshape(n_tok, feats), w1_in[g, 1], preferred_element_type=F32)
        )

    @pl.when(in_first)
    def _():
        for g in range(3):
            value = partial_product(g).reshape(NZ, 2, patches, group)
            own1[:, :, g * patches:(g + 1) * patches] = value

    @pl.when(in_second)
    def _():
        for g in range(4):
            value = partial_product(g).reshape(2, 2, half_rows, group)
            own1[g] = value[0]
            own1[4 + g] = value[1]

    def by_section(action):
        pl.when(in_first)(lambda: action(short_rows))
        pl.when(in_second)(lambda: action(half_rows))

    up1, down1 = {}, {}

    def hop1(stage, h, upward):
        send_buf, recv_buf = (zs1_p, zr1_p) if upward else (zs1_m, zr1_m)
        table = up1 if upward else down1
        device = up_z if upward else down_z
        block = around(4 - stage) if upward else around(stage - 4)
        value = own1[block, h]
        if stage >= 2 or (stage == 1 and h == (0 if upward else 1)):
            sem = table[(stage - 1, h)]
            by_section(lambda n: remote(
                recv_buf.at[stage - 1, h, 0:n], recv_buf.at[stage - 1, h, 0:n], sem, device).wait_recv())
            value = value + recv_buf[stage - 1, h].astype(F32)
        send_buf[stage, h] = value.astype(BF16)
        sem_out = next(sems)
        table[(stage, h)] = sem_out
        by_section(lambda n: remote(
            send_buf.at[stage, h, 0:n], recv_buf.at[stage, h, 0:n], sem_out, device).start())
        sent.append(lambda: by_section(lambda n: remote(
            send_buf.at[stage, h, 0:n], recv_buf.at[stage, h, 0:n], sem_out, device).wait_send()))

    hop1(0, 0, True)
    hop1(0, 1, False)
    for stage in (1, 2, 3):
        hop1(stage, 1, True)
        hop1(stage, 0, False)
        hop1(stage, 0, True)
        hop1(stage, 1, False)
    for h in (1, 0):
        by_section(lambda n: remote(zr1_p.at[3, h, 0:n], zr1_p.at[3, h, 0:n], up1[(3, h)], up_z).wait_recv())
        by_section(lambda n: remote(zr1_m.at[3, h, 0:n], zr1_m.at[3, h, 0:n], down1[(3, h)], down_z).wait_recv())

    def summed(h):
        return own1[z, h] + zr1_p[3, h].astype(F32) + zr1_m[3, h].astype(F32)

    has_head = jnp.logical_and(in_second, jnp.logical_not(wide(z)))

    @pl.when(has_head)
    def _():
        value = jnp.concatenate([summed(0), summed(1)], axis=0).astype(BF16)
        result = attend(value[:, 0:HEAD], value[:, HEAD:2 * HEAD], value[:, 2 * HEAD:3 * HEAD])
        acts1[z, :, :, 0:HEAD] = result.reshape(2, half_rows, HEAD)

    @pl.when(jnp.logical_not(has_head))
    def _():
        for h in range(2):
            acts1[z, h] = gelu(summed(h))

    def by_kind(block, action):
        pl.when(in_first)(lambda: action(short_rows, group))
        is_wide = wide(block)
        pl.when(jnp.logical_and(in_second, is_wide))(lambda: action(half_rows, group))
        pl.when(jnp.logical_and(in_second, jnp.logical_not(is_wide)))(lambda: action(half_rows, HEAD))

    gather1 = {}

    def pass_on1(stage, h, upward):
        block = around(-stage) if upward else around(stage)
        sem = next(sems)
        gather1[(stage, h, upward)] = sem
        device = up_z if upward else down_z

        def copy(n, w):
            part = acts1.at[block, h, 0:n, 0:w]
            return remote(part, part, sem, device)

        by_kind(block, lambda n, w: copy(n, w).start())
        sent.append(lambda: by_kind(block, lambda n, w: copy(n, w).wait_send()))

    def arrived1(stage, h, upward):
        block = around(-1 - stage) if upward else around(1 + stage)
        device = up_z if upward else down_z
        by_kind(block, lambda n, w: remote(
            acts1.at[block, h, 0:n, 0:w], acts1.at[block, h, 0:n, 0:w], gather1[(stage, h, upward)], device).wait_recv())

    for h in range(2):
        for upward in (True, False):
            pass_on1(0, h, upward)
    for stage in range(4):
        for h in range(2):
            for upward in (True, False):
                if stage == 3 and h != (0 if upward else 1):
                    continue
                arrived1(stage, h, upward)
                if stage < 2 or (stage == 2 and h == (0 if upward else 1)):
                    pass_on1(stage + 1, h, upward)

    @pl.when(in_first)
    def _():
        for k in range(2):
            total = None
            for g in range(3):
                hidden = acts1[:, :, g * patches:(g + 1) * patches].reshape(n_tok, group)
                term = jnp.dot(hidden, w1_mix[k, g * group:(g + 1) * group], preferred_element_type=F32)
                total = term if total is None else total + term
            acc1[k] = total

    @pl.when(in_second)
    def _():
        for image in range(2):
            first = image * 4
            value = jnp.concatenate(
                [acts1[first + j, :, :, 0:HEAD].reshape(2 * half_rows, HEAD) for j in range(3)]
                + [acts1[first + 3].reshape(2 * half_rows, group)], axis=1)
            for k in range(2):
                acc1[k, image * 2 * half_rows:(image + 1) * 2 * half_rows] = jnp.dot(
                    value, w1_mix[k, 0:2 * group], preferred_element_type=F32)

    for k in range(2):
        mix1_s[k] = acc1[k].astype(BF16).reshape(2, n_col, patches, feats)
    copies = []
    for step in range(1, n_col):
        target = lax.rem(col + step, n_col)
        copy = remote(mix1_s.at[:, :, target], mix1_r.at[step - 1], next(sems), {"col": target})
        copy.start()
        copies.append(copy)
    total = mix1_s[:, :, col].astype(F32)
    for step, copy in enumerate(copies):
        copy.wait()
        total = total + mix1_r[step].astype(F32)
    ys1[...] = total.astype(BF16)
    to_pair, to_outer, to_diagonal = next(sems), next(sems), next(sems)

    @pl.when(in_first)
    def _():
        copies = [remote(ys1.at[other], yr1.at[1], to_outer, outer), remote(ys1.at[yb], yr1.at[2], to_diagonal, diagonal)]
        for copy in copies:
            copy.start()
        for copy in copies:
            copy.wait_send()

    @pl.when(in_second)
    def _():
        copy = remote(ys1.at[other], yr1.at[0], to_pair, pair)
        copy.start()
        copy.wait()
        remote(yr1.at[1], yr1.at[1], to_outer, outer).wait_recv()
        remote(yr1.at[2], yr1.at[2], to_diagonal, diagonal).wait_recv()
        result = xb1[yb].astype(F32) + ys1[yb].astype(F32)
        for k in range(3):
            result = result + yr1[k].astype(F32)
        y_ref[...] = result.astype(BF16)

    assert next(sems) < 208
    for wait in sent:
        wait()


def layers(x, weights):
    gain, wq, wk, wv, wup, wout, wdown = weights
    n_col = lax.axis_size("col")
    images, patches, feats = x.shape
    half = n_col // 2 * patches
    wide_in = 6 * HEAD
    vmem = pl.BlockSpec(memory_space=pltpu.VMEM)
    anywhere = pl.BlockSpec(memory_space=pl.ANY)
    z_buf = pltpu.VMEM((4, 2, half, wide_in), BF16)
    y_buf = pltpu.VMEM((4, 2, half // 2, wide_in), BF16)
    z1_buf = pltpu.VMEM((4, 2, 4 * patches, feats), BF16)
    pair_buf = pltpu.VMEM((NZ, half, wide_in), BF16)
    scratch = [
        pltpu.VMEM((NZ, feats, wide_in), BF16),
        pltpu.VMEM((NZ, wide_in, feats), BF16),
        pltpu.VMEM((2, n_col, patches, feats), BF16),
        pltpu.VMEM((NZ, 2, 2, half, wide_in), F32),
        pltpu.VMEM((2 * NZ, 8, 128), F32),
        z_buf, z_buf, z_buf, z_buf, y_buf, y_buf, y_buf, y_buf, pair_buf, pair_buf,
        pltpu.VMEM((half, wide_in), BF16), pltpu.VMEM((half, wide_in), BF16),
        pltpu.VMEM((2 * half, wide_in), F32),
        pltpu.VMEM((2, NZ, 2 * half, wide_in), BF16),
        pltpu.VMEM((2, 2 * half, feats), F32),
        pltpu.VMEM((2, n_col, patches, feats), BF16),
        pltpu.VMEM((n_col - 1, 2, patches, feats), BF16),
        pltpu.VMEM((4, 2, feats, feats), BF16),
        pltpu.VMEM((2, 3 * feats, feats), BF16),
        pltpu.VMEM((2, 8, feats), F32),
        pltpu.VMEM((2, 2, patches, feats), BF16),
        pltpu.VMEM((2, 2, n_col, patches, feats), BF16),
        pltpu.VMEM((NZ, 2, 4 * patches, feats), F32),
        pltpu.VMEM((NZ, 8, 128), F32),
        z1_buf, z1_buf, z1_buf, z1_buf,
        pltpu.VMEM((NZ, 2, 4 * patches, feats), BF16),
        pltpu.VMEM((2, 2 * n_col * patches, feats), F32),
        pltpu.VMEM((2, 2, n_col, patches, feats), BF16),
        pltpu.VMEM((n_col - 1, 2, 2, patches, feats), BF16),
        pltpu.VMEM((2, 2, patches, feats), BF16),
        pltpu.VMEM((3, 2, patches, feats), BF16),
        pltpu.SemaphoreType.DMA((40,)),
        pltpu.SemaphoreType.DMA((208,)),
        pltpu.SemaphoreType.DMA((208,)),
    ]
    return pl.pallas_call(
        functools.partial(layers_kernel, n_col, patches, feats),
        out_shape=jax.ShapeDtypeStruct(x.shape, BF16),
        in_specs=[vmem, vmem] + [anywhere] * 6,
        out_specs=vmem,
        scratch_shapes=scratch,
        compiler_params=pltpu.CompilerParams(
            collective_id=0, has_side_effects=True, vmem_limit_bytes=67043328
        ),
    )(x, gain[None], wq, wk, wv, wup, wout, wdown)


def local(tokens, ln_gain, w_query, w_key, w_value, w_up, w_out, w_down):
    weights = (ln_gain[0], w_query[0], w_key[0], w_value[0], w_up[0], w_out[0], w_down[0])
    return layers(tokens, weights)[None]


def solution(mesh):
    return jax.shard_map(
        local,
        mesh=mesh,
        in_specs=(
            P(None, "col", "row"),
            P("section", "row"),
            P("section", "row", "col"),
            P("section", "row", "col"),
            P("section", "row", "col"),
            P("section", "row", "col"),
            P("section", "col", "row"),
            P("section", "col", "row"),
        ),
        out_specs=P("section", None, "col", "row"),
        check_vma=False,
    )
```

```python
import functools
import math

import jax
import jax.numpy as jnp
from jax import lax
from jax.experimental import pallas as pl
from jax.experimental.pallas import tpu as pltpu
from jax.sharding import PartitionSpec as P

D = 6144
HEAD = 128
EPS = 1e-06
NZ = 8
MESH = pl.DeviceIdType.MESH
BF16 = jnp.bfloat16
F32 = jnp.float32


def wide(block):
    return lax.rem(block, 4) == 3


def by_width(block, narrow_size, wide_size, action):
    is_wide = wide(block)

    @pl.when(is_wide)
    def _():
        action(wide_size)

    @pl.when(jnp.logical_not(is_wide))
    def _():
        action(narrow_size)


def layers_kernel(
    n_col, patches, feats,
    x_ref, gain_ref, wq_ref, wk_ref, wv_ref, wup_ref, wout_ref, wdn_ref,
    y_ref,
    w_in, w_mix, gathered, own, stat,
    zs_p, zs_m, zr_p, zr_m, ys_p, ys_m, yr_p, yr_m, pair_s, pair_r, last_s, last_r,
    full, acts, acc, mix_s,
    stat_col, mix_d, mix_t,
    w1_in, w1_mix, gain1, xb1, gathered1, own1, stat1, zs1_p, zs1_m, zr1_p, zr1_m,
    acts1, acc1, mix1_s, mix_r, ys1, yr1,
    w_sem, ssem, rsem,
):
    section = lax.axis_index("section")
    row = lax.axis_index("row")
    col = lax.axis_index("col")
    n_row = 2 * NZ
    yb = lax.div(row, NZ)
    z = lax.rem(row, NZ)
    other = 1 - yb

    def around(step):
        return lax.rem(z + step + NZ, NZ)

    up_z = {"row": yb * NZ + around(1)}
    down_z = {"row": yb * NZ + around(-1)}
    pair = {"row": other * NZ + z}
    outer = {"section": 1 - section, "row": other * NZ + z}
    diagonal = {"section": 1 - section, "row": row}
    n_x = n_col // 2
    core = lax.rem(col, 2)
    chip_x = lax.div(col, 2)
    sibling = {"col": 2 * chip_x + 1 - core}

    def along_x(step):
        return lax.rem(chip_x + step, n_x)

    def same_core(step):
        return {"col": 2 * along_x(step) + core}
    in_first = section == 0
    in_second = section == 1

    narrow_in, wide_in = 5 * HEAD, 6 * HEAD
    narrow_mix, wide_mix = 3 * HEAD, 6 * HEAD
    half = n_col // 2 * patches
    quarter = half // 2

    barrier = pltpu.get_barrier_semaphore()
    for step in range(1, n_row):
        pl.semaphore_signal(barrier, inc=1, device_id={"row": lax.rem(row + step, n_row)}, device_id_type=MESH)
    for step in range(1, n_col):
        pl.semaphore_signal(barrier, inc=1, device_id={"col": lax.rem(col + step, n_col)}, device_id_type=MESH)
    for device in (outer, diagonal):
        pl.semaphore_signal(barrier, inc=1, device_id=device, device_id_type=MESH)

    sems = iter(range(1000))

    def remote(source, target, sem, device):
        return pltpu.make_async_remote_copy(
            src_ref=source, dst_ref=target, send_sem=ssem.at[sem], recv_sem=rsem.at[sem],
            device_id=device, device_id_type=MESH,
        )

    def ready():
        pl.semaphore_wait(barrier, n_row - 1 + n_col - 1 + 2)

    def column_stats(sums, squares):
        columns = jnp.concatenate(
            [jnp.broadcast_to(sums, (2 * patches, 128)), jnp.broadcast_to(squares, (2 * patches, 128))], axis=0
        )
        return columns.T[0:8]

    def lane_stats(total):
        mean = total * (1.0 / D)
        lane = lax.broadcasted_iota(jnp.int32, (8, 128), 1)
        shifted = pltpu.roll(mean, 2 * patches, axis=1)
        var = jnp.maximum(mean - shifted * shifted, 0.0)
        return jnp.where(lane < 2 * patches, mean, lax.rsqrt(var + EPS))

    def to_columns(table):
        rows = table[:, 0, :]
        return jnp.concatenate([rows] * (128 // n_col), axis=0).T

    def normalise(block, columns, c, gain):
        value = block.astype(F32).reshape(2 * patches, feats)
        mean, scale = columns[0:2 * patches, c:c + 1], columns[2 * patches:4 * patches, c:c + 1]
        return ((value - mean) * scale * gain).astype(BF16).reshape(2, patches, feats)

    def col_gather(view):
        arrive = []
        for step in (1, 3, 2):
            copy = remote(view(col), view(col), next(sems), same_core(step))
            copy.start()
            arrive.append((copy, step))
        first = remote(view(col), view(col), next(sems), sibling)
        first.start()

        def finish():
            handed = [first]
            for copy, step in arrive:
                copy.wait()
                block = view(2 * along_x(n_x - step) + core)
                onward = remote(block, block, next(sems), sibling)
                onward.start()
                handed.append(onward)
            for copy in handed:
                copy.wait()

        return finish

    def gelu(value):
        return (0.5 * value * (1.0 + lax.erf(value * math.sqrt(0.5)))).astype(BF16)

    def attend(query, keyed, valued):
        scores = lax.dot_general(query, keyed, (((1,), (1,)), ((), ())), preferred_element_type=F32)
        scores = scores * (1.0 / math.sqrt(HEAD))
        expo = jnp.exp(scores - jnp.max(scores, axis=-1, keepdims=True))
        probs = (expo / jnp.sum(expo, axis=-1, keepdims=True)).astype(BF16)
        return jnp.dot(probs, valued, preferred_element_type=F32).astype(BF16)

    def col_sum(parts, from_sibling, sums, arrived_sums, at, read):
        swap = remote(at(parts, slice(None), 1 - core), at(from_sibling), next(sems), sibling)
        swap.start()
        swap.wait()
        out = []
        for step in (2, 1, 3):
            target = along_x(step)
            value = read(parts, target, core).astype(F32) + read(from_sibling, target).astype(F32)
            put(sums, at, target, value.astype(BF16))
            copy = remote(at(sums, target), at(arrived_sums.at[step - 1]), next(sems), same_core(step))
            copy.start()
            out.append((copy, step))
        value = read(parts, chip_x, core).astype(F32) + read(from_sibling, chip_x).astype(F32)
        for copy, step in out:
            copy.wait()
            value = value + read(arrived_sums.at[step - 1]).astype(F32)
        return value

    def put(ref, at, target, value):
        at(ref, target)[...] = value

    group = feats
    block_sems = {name: [next(sems) for _ in range(n)] for name, n in
                  (("pair", 5), ("outer", 5), ("via", 5), ("forward", 5), ("gain", 3))}
    mlp_first = 2 * group
    mlp_rest = 3 * group

    def head_cols(member, j):
        return pl.ds(pl.multiple_of((member * 3 + j) * HEAD, HEAD), HEAD)

    def third(at, g):
        return w_in.at[at + g // 2, :, (g % 2) * group:(g % 2 + 1) * group]

    @pl.when(in_second)
    def ship():
        copies = []

        def fetch(source, target):
            copy = pltpu.make_async_copy(source, target, w_sem.at[len(copies)])
            copy.start()
            copies.append(copy)

        start = pl.multiple_of(mlp_first + yb * mlp_rest, group)
        fetch(wup_ref.at[:, pl.ds(start, 2 * group)], w_in.at[4])
        fetch(wup_ref.at[:, pl.ds(pl.multiple_of(start + 2 * group, group), group)], w_in.at[5, :, 0:group])
        fetch(wdn_ref.at[pl.ds(start, 2 * group)], w_mix.at[3])
        fetch(wdn_ref.at[pl.ds(pl.multiple_of(start + 2 * group, group), group)], w_mix.at[4, 0:group])
        n_via = len(copies)
        start = pl.multiple_of(mlp_first + other * mlp_rest, group)
        fetch(wup_ref.at[:, pl.ds(start, 2 * group)], w_in.at[2])
        fetch(wup_ref.at[:, pl.ds(pl.multiple_of(start + 2 * group, group), group)], w_in.at[3, :, 0:group])
        fetch(wdn_ref.at[pl.ds(start, 2 * group)], w_mix.at[1])
        fetch(wdn_ref.at[pl.ds(pl.multiple_of(start + 2 * group, group), group)], w_mix.at[2, 0:group])
        n_outer = len(copies)
        for member, mine in ((other, False), (yb, True)):
            for j in range(3):
                for k, w_ref in enumerate((wq_ref, wk_ref, wv_ref)):
                    span = slice(k * HEAD, (k + 1) * HEAD)
                    at = (j % 2) * group + k * HEAD
                    target = w1_in.at[j, yb, :, span] if mine else w_in.at[j // 2, :, at:at + HEAD]
                    fetch(w_ref.at[:, head_cols(member, j)], target)
            rows = pl.ds(pl.multiple_of(member * group, group), group)
            fetch(wup_ref.at[:, rows], w1_in.at[3, yb] if mine else w_in.at[1, :, group:2 * group])
            fetch(wout_ref.at[rows], w1_mix.at[yb, 0:group] if mine else w_mix.at[0, 0:group])
            fetch(wdn_ref.at[rows], w1_mix.at[yb, group:2 * group] if mine else w_mix.at[0, group:2 * group])
            if not mine:
                n_pair = len(copies)
        gain1[yb] = jnp.broadcast_to(gain_ref[...], (8, feats))
        ready()
        out = []

        def send(source, target, sem, device):
            copy = remote(source, target, sem, device)
            copy.start()
            out.append(copy)

        for copy in copies[:n_via]:
            copy.wait()
        for g in range(3):
            send(third(4, g), third(6, g), block_sems["via"][g], pair)
        send(w_mix.at[3], w_mix.at[5], block_sems["via"][3], pair)
        send(w_mix.at[4, 0:group], w_mix.at[6, 0:group], block_sems["via"][4], pair)
        for copy in copies[n_via:n_outer]:
            copy.wait()
        for g in range(3):
            send(third(2, g), w1_in.at[g, yb], block_sems["outer"][g], outer)
        send(w_mix.at[1], w1_mix.at[yb, 0:2 * group], block_sems["outer"][3], outer)
        send(w_mix.at[2, 0:group], w1_mix.at[yb, 2 * group:3 * group], block_sems["outer"][4], outer)
        for copy in copies[n_outer:n_pair]:
            copy.wait()
        for g in range(4):
            send(third(0, g), w1_in.at[g, yb], block_sems["pair"][g], pair)
        send(w_mix.at[0], w1_mix.at[yb, 0:2 * group], block_sems["pair"][4], pair)
        for device, sem in zip((pair, outer, diagonal), block_sems["gain"]):
            send(gain1.at[yb], gain1.at[yb], sem, device)
        for g in range(3):
            remote(third(6, g), third(6, g), block_sems["via"][g], pair).wait_recv()
            send(third(6, g), w1_in.at[g, other], block_sems["forward"][g], outer)
        remote(w_mix.at[5], w_mix.at[5], block_sems["via"][3], pair).wait_recv()
        send(w_mix.at[5], w1_mix.at[other, 0:2 * group], block_sems["forward"][3], outer)
        remote(w_mix.at[6, 0:group], w_mix.at[6, 0:group], block_sems["via"][4], pair).wait_recv()
        send(w_mix.at[6, 0:group], w1_mix.at[other, 2 * group:3 * group], block_sems["forward"][4], outer)
        for copy in copies[n_pair:]:
            copy.wait()
        for g in range(4):
            remote(w1_in.at[g, other], w1_in.at[g, other], block_sems["pair"][g], pair).wait_recv()
        remote(w1_mix.at[other, 0:2 * group], w1_mix.at[other, 0:2 * group], block_sems["pair"][4], pair).wait_recv()
        remote(gain1.at[other], gain1.at[other], block_sems["gain"][0], pair).wait_recv()
        for copy in out:
            copy.wait_send()

    def first_layer():
        sent = []
        weight_waits = []
        for block in range(NZ):
            if block % 4 == 3:
                start = 6 * 2 * HEAD + (block // 4) * wide_in
                copies_in = [(wup_ref.at[:, start:start + wide_in], 0, wide_in)]
                copies_out = [(wdn_ref.at[start:start + wide_mix], 0, wide_mix)]
            else:
                head = block - block // 4
                cols = slice(head * HEAD, (head + 1) * HEAD)
                start = head * 2 * HEAD
                copies_in = [
                    (wq_ref.at[:, cols], 0, HEAD),
                    (wk_ref.at[:, cols], HEAD, HEAD),
                    (wv_ref.at[:, cols], 2 * HEAD, HEAD),
                    (wup_ref.at[:, start:start + 2 * HEAD], 3 * HEAD, 2 * HEAD),
                ]
                copies_out = [
                    (wout_ref.at[cols], 0, HEAD),
                    (wdn_ref.at[start:start + 2 * HEAD], HEAD, 2 * HEAD),
                ]
            for source, at, size in copies_in:
                copy = pltpu.make_async_copy(source, w_in.at[block, :, at:at + size], w_sem.at[len(weight_waits)])
                copy.start()
                weight_waits.append((copy, 0))
            for source, at, size in copies_out:
                copy = pltpu.make_async_copy(source, w_mix.at[block, at:at + size], w_sem.at[len(weight_waits)])
                copy.start()
                weight_waits.append((copy, 1))

        xf = x_ref[...].astype(F32).reshape(2 * patches, feats)
        sums = jnp.sum(xf, axis=-1, keepdims=True)
        squares = jnp.sum(xf * xf, axis=-1, keepdims=True)
        stat[row] = column_stats(sums, squares)
        ready()
        gathered[:, col] = x_ref[...]
        stat_copies = []
        for step in range(1, n_row):
            copy = remote(stat.at[row], stat.at[row], next(sems), {"row": lax.rem(row + step, n_row)})
            copy.start()
            stat_copies.append(copy)
        finish_x = col_gather(lambda c: gathered.at[:, c])
        for copy in stat_copies:
            copy.wait()
        stat_col[0, col] = lane_stats(jnp.sum(stat[...], axis=0))
        finish_stats = col_gather(lambda c: stat_col.at[0, c])
        for copy, kind in weight_waits:
            if kind == 0:
                copy.wait()
        finish_x()
        finish_stats()
        columns = to_columns(stat_col[0])
        for c in range(n_col):
            gathered[:, c] = normalise(gathered[:, c], columns, c, gain_ref[...])

        first_up, first_down = next(sems), next(sems)
        early_up, early_down = next(sems), next(sems)
        pair_base = next(sems)
        for _ in range(NZ - 1):
            next(sems)

        def send_in(source, target, sem, device, block):
            by_width(block, narrow_in, wide_in,
                     lambda w: remote(source.at[:, 0:w], target.at[:, 0:w], sem, device).start())

        def recv_in(target, sem, device, block):
            by_width(block, narrow_in, wide_in,
                     lambda w: remote(target.at[:, 0:w], target.at[:, 0:w], sem, device).wait_recv())

        def sent_in(source, sem, device, block):
            by_width(block, narrow_in, wide_in,
                     lambda w: remote(source.at[:, 0:w], source.at[:, 0:w], sem, device).wait_send())


        def order(i):
            away = 4 - lax.div(i + 1, 2)
            return around(jnp.where(lax.rem(i, 2) == 1, away, -away))

        def product(i, carry):
            block = order(i)
            own[block] = jnp.dot(gathered[...].reshape(2 * n_col * patches, feats), w_in[block],
                                 preferred_element_type=F32).reshape(2, 2, half, wide_in)
            pair_s[i] = own[block, other, 0].astype(BF16)

            @pl.when(i == 0)
            def _():
                zs_p[0, 0] = own[block, 0, 1].astype(BF16)
                send_in(zs_p.at[0, 0], zr_p.at[0, 0], first_up, up_z, block)
                zs_m[0, 1] = own[block, 1, 1].astype(BF16)
                send_in(zs_m.at[0, 1], zr_m.at[0, 1], first_down, down_z, block)

            @pl.when(i == 1)
            def _():
                zs_p[1, 1] = own[block, 1, 1].astype(BF16)
                send_in(zs_p.at[1, 1], zr_p.at[1, 1], early_up, up_z, block)

            @pl.when(i == 2)
            def _():
                zs_m[1, 0] = own[block, 0, 1].astype(BF16)
                send_in(zs_m.at[1, 0], zr_m.at[1, 0], early_down, down_z, block)

            send_in(pair_s.at[i], pair_r.at[i], pair_base + i, pair, block)
            return carry

        lax.fori_loop(0, NZ, product, 0)
        for i in range(NZ):
            sent.append(lambda i=i: sent_in(pair_s.at[i], pair_base + i, pair, order(jnp.int32(i))))

        def up_block(stage):
            return around(4 - stage)

        def down_block(stage):
            return around(stage - 4)

        up_sem = {(1, 0, 0): first_up, (1, 1, 1): early_up}
        down_sem = {(1, 0, 1): first_down, (1, 1, 0): early_down}
        for key in [(1, 0, 0), (1, 1, 1)]:
            sent.append(lambda key=key: sent_in(zs_p.at[key[1], key[2]], up_sem[key], up_z, up_block(key[1])))
        for key in [(1, 0, 1), (1, 1, 0)]:
            sent.append(lambda key=key: sent_in(zs_m.at[key[1], key[2]], down_sem[key], down_z, down_block(key[1])))

        def mine(which, h, block):
            if which == 1:
                return own[block, h, 1]
            rows = slice(h * quarter, (h + 1) * quarter)
            return own[block, yb, 0, rows]

        def hop(which, stage, h, upward, extra=None):
            send_buf = (zs_p if upward else zs_m) if which == 1 else (ys_p if upward else ys_m)
            recv_buf = (zr_p if upward else zr_m) if which == 1 else (yr_p if upward else yr_m)
            table = up_sem if upward else down_sem
            device = up_z if upward else down_z
            source_device = device
            block = up_block(stage) if upward else down_block(stage)
            value = mine(which, h, block) if extra is None else extra
            first_half = 0 if upward else 1
            has_arrival = stage >= 2 or (stage == 1 and h == first_half)
            if has_arrival:
                recv_in(recv_buf.at[stage - 1, h], table[(which, stage - 1, h)], source_device, block)
                value = value + recv_buf[stage - 1, h].astype(F32)
            send_buf[stage, h] = value.astype(BF16)
            sem = next(sems)
            table[(which, stage, h)] = sem
            send_in(send_buf.at[stage, h], recv_buf.at[stage, h], sem, device, block)
            sent.append(lambda: sent_in(send_buf.at[stage, h], sem, device, block))

        hop(1, 1, 0, True)
        hop(1, 1, 1, False)

        def pair_sum(i):
            block = order(jnp.int32(i))
            recv_in(pair_r.at[i], pair_base + i, pair, block)
            own[block, yb, 0] = own[block, yb, 0] + pair_r[i].astype(F32)

        for stage in (2, 3):
            hop(1, stage, 1, True)
            hop(1, stage, 0, False)
            if stage == 2:
                pair_sum(0)
                hop(0, 0, 0, True)
                hop(0, 0, 1, False)
            hop(1, stage, 0, True)
            hop(1, stage, 1, False)
            if stage == 2:
                pair_sum(1)
                hop(0, 1, 1, True)
                pair_sum(2)
                hop(0, 1, 0, False)
        hop(0, 1, 0, True)
        hop(0, 1, 1, False)
        pair_sum(3)
        hop(0, 2, 1, True)
        pair_sum(4)
        hop(0, 2, 0, False)
        for h in (1, 0):
            recv_in(zr_p.at[3, h], up_sem[(1, 3, h)], up_z, z)
            recv_in(zr_m.at[3, h], down_sem[(1, 3, h)], down_z, z)
        last_s[...] = (own[z, other, 1] + zr_p[3, other].astype(F32) + zr_m[3, other].astype(F32)).astype(BF16)
        last_sem = next(sems)
        send_in(last_s, last_r, last_sem, pair, z)
        sent.append(lambda: sent_in(last_s, last_sem, pair, z))
        hop(0, 2, 0, True)
        hop(0, 2, 1, False)
        pair_sum(5)
        hop(0, 3, 1, True)
        pair_sum(6)
        hop(0, 3, 0, False)
        hop(0, 3, 0, True)
        hop(0, 3, 1, False)
        full[half:2 * half] = own[z, yb, 1] + zr_p[3, yb].astype(F32) + zr_m[3, yb].astype(F32)
        recv_in(last_r, last_sem, pair, z)
        full[half:2 * half] = full[half:2 * half] + last_r[...].astype(F32)
        pair_sum(7)
        for h in (1, 0):
            recv_in(yr_p.at[3, h], up_sem[(0, 3, h)], up_z, z)
            recv_in(yr_m.at[3, h], down_sem[(0, 3, h)], down_z, z)
        for h in (0, 1):
            full[h * quarter:(h + 1) * quarter] = (
                own[z, yb, 0, h * quarter:(h + 1) * quarter] + yr_p[3, h].astype(F32) + yr_m[3, h].astype(F32)
            )

        def hidden(size):
            acts[yb, z, :, 0:size] = gelu(full[:, 0:size])

        def attention(size):
            acts[yb, z, :, HEAD:size] = gelu(full[:, 3 * HEAD:5 * HEAD])
            acts[yb, z, :, 0:HEAD] = attend(
                full[:, 0:HEAD].astype(BF16), full[:, HEAD:2 * HEAD].astype(BF16), full[:, 2 * HEAD:3 * HEAD].astype(BF16)
            )

        is_wide = wide(z)
        pl.when(is_wide)(lambda: hidden(wide_mix))
        pl.when(jnp.logical_not(is_wide))(lambda: attention(narrow_mix))

        def view(image, block, lo, hi, w):
            return acts.at[image, block, lo:hi, 0:w]

        def send_act(image, block, lo, hi, sem, device):
            by_width(block, narrow_mix, wide_mix, lambda w: remote(
                view(image, block, lo, hi, w), view(image, block, lo, hi, w), sem, device).start())
            sent.append(lambda: by_width(block, narrow_mix, wide_mix, lambda w: remote(
                view(image, block, lo, hi, w), view(image, block, lo, hi, w), sem, device).wait_send()))

        def recv_act(image, block, lo, hi, sem, device):
            by_width(block, narrow_mix, wide_mix, lambda w: remote(
                view(image, block, lo, hi, w), view(image, block, lo, hi, w), sem, device).wait_recv())

        images = [yb, other, yb]
        spans = [(0, half), (0, half), (half, 2 * half)]
        gather_sem = {}

        def pass_on(stage, stream, upward):
            lo, hi = spans[stream]
            if stage == 3:
                mid = lo + quarter
                lo, hi = (lo, mid) if upward else (mid, hi)
            block = around(-stage) if upward else around(stage)
            sem = next(sems)
            gather_sem[(stage, stream, upward)] = sem
            send_act(images[stream], block, lo, hi, sem, up_z if upward else down_z)

        def arrived(stage, stream, upward):
            lo, hi = spans[stream]
            if stage == 3:
                mid = lo + quarter
                lo, hi = (lo, mid) if upward else (mid, hi)
            block = around(-1 - stage) if upward else around(1 + stage)
            recv_act(images[stream], block, lo, hi, gather_sem[(stage, stream, upward)], up_z if upward else down_z)
            return block, lo, hi

        pair_first = next(sems)
        send_act(yb, z, 0, half, pair_first, pair)
        for stream in (0, 2):
            pass_on(0, stream, True)
            pass_on(0, stream, False)
        own_sem = next(sems)
        send_act(yb, z, half, 2 * half, own_sem, pair)
        recv_act(other, z, 0, half, pair_first, pair)
        pass_on(0, 1, True)
        pass_on(0, 1, False)

        for copy, kind in weight_waits:
            if kind == 1:
                copy.wait()

        def add_product(image, block, lo, hi):
            def add(w):
                acc[image, lo:hi] = acc[image, lo:hi] + jnp.dot(
                    acts[image, block, lo:hi, 0:w], w_mix[block, 0:w], preferred_element_type=F32)
            by_width(block, narrow_mix, wide_mix, add)

        acc[...] = jnp.zeros_like(acc)
        pair_done = {}

        def products_of(stage):
            for block in sorted_blocks(stage):
                add_product(yb, block, 0, 2 * half)
                add_product(other, block, 0, half)

        def sorted_blocks(stage):
            return [around(1 + stage)] if stage == 3 else [around(1 + stage), around(-1 - stage)]

        def pair_products(waits, blocks):
            for wait in waits:
                recv_act(other, *wait, pair)
            for block in blocks:
                add_product(other, block, half, 2 * half)

        for stage in range(4):
            coming = []
            for stream in (2, 0, 1):
                for upward in (True, False):
                    block, lo, hi = arrived(stage, stream, upward)
                    if stage < 3:
                        pass_on(stage + 1, stream, upward)
                    if stream == 2:
                        sem = next(sems)
                        send_act(yb, block, lo, hi, sem, pair)
                        coming.append((block, lo, hi, sem))
            pair_done[stage] = coming
            if stage == 0:
                add_product(yb, z, 0, 2 * half)
                add_product(other, z, 0, half)
                pair_products([(z, half, 2 * half, own_sem)], [z])
            else:
                pair_products(pair_done[stage - 1], sorted_blocks(stage - 1))
            products_of(stage)
        pair_products(pair_done[3], sorted_blocks(3))
        mix_s[...] = acc[...].astype(BF16).reshape(2, n_x, 2, patches, feats)
        total = x_ref[...].astype(F32) + col_sum(
            mix_s, mix_d.at[0], mix_t.at[0], mix_r.at[:, 0], lambda ref, *at: ref.at[(slice(None), *at)],
            lambda ref, *at: ref[(slice(None), *at)])
        y_ref[...] = total.astype(BF16)
        xb1[yb] = total.astype(BF16)
        for device, sem in ((pair, spread[0]), (outer, spread[1]), (diagonal, spread[2])):
            copy = remote(xb1.at[yb], xb1.at[yb], sem, device)
            copy.start()
            sent.append(copy.wait_send)
        for wait in sent:
            wait()
        for g in range(3):
            remote(w1_in.at[g, other], w1_in.at[g, other], block_sems["outer"][g], outer).wait_recv()
            remote(w1_in.at[g, yb], w1_in.at[g, yb], block_sems["forward"][g], outer).wait_recv()
        for half_k, name in ((other, "outer"), (yb, "forward")):
            for k, (lo, hi) in ((3, (0, 2 * group)), (4, (2 * group, 3 * group))):
                part = w1_mix.at[half_k, lo:hi]
                remote(part, part, block_sems[name][k], outer).wait_recv()
        remote(gain1.at[other], gain1.at[other], block_sems["gain"][1], outer).wait_recv()
        remote(gain1.at[yb], gain1.at[yb], block_sems["gain"][2], diagonal).wait_recv()
        remote(xb1.at[other], xb1.at[other], spread[0], pair).wait_recv()

    spread = [next(sems) for _ in range(3)]
    pl.when(in_first)(first_layer)

    @pl.when(in_second)
    def _():
        remote(xb1.at[other], xb1.at[other], spread[1], outer).wait_recv()
        remote(xb1.at[yb], xb1.at[yb], spread[2], diagonal).wait_recv()

    sent = []
    n_tok = 2 * n_col * patches
    both = xb1[...].astype(F32).reshape(2, 2 * patches, feats)
    sums = jnp.sum(jnp.sum(both, axis=-1, keepdims=True), axis=0)
    squares = jnp.sum(jnp.sum(both * both, axis=-1, keepdims=True), axis=0)
    stat1[z] = column_stats(sums, squares)
    copies = []
    for step in range(1, NZ):
        copy = remote(stat1.at[z], stat1.at[z], next(sems), {"row": yb * NZ + around(step)})
        copy.start()
        copies.append(copy)
    for k in range(2):
        gathered1[k, :, col] = xb1[k]
    finish_x1 = col_gather(lambda c: gathered1.at[:, :, c])
    for copy in copies:
        copy.wait()
    stat_col[1, col] = lane_stats(jnp.sum(stat1[...], axis=0))
    finish_stats1 = col_gather(lambda c: stat_col.at[1, c])
    finish_x1()
    finish_stats1()
    columns1 = to_columns(stat_col[1])
    for c in range(n_col):
        for k in range(2):
            gathered1[k, :, c] = normalise(gathered1[k, :, c], columns1, c, gain1[k, 0:1])

    half_rows = 4 * patches
    short_rows = 3 * patches

    def partial_product(g):
        return (
            jnp.dot(gathered1[0].reshape(n_tok, feats), w1_in[g, 0], preferred_element_type=F32)
            + jnp.dot(gathered1[1].reshape(n_tok, feats), w1_in[g, 1], preferred_element_type=F32)
        )

    @pl.when(in_first)
    def _():
        for g in range(3):
            value = partial_product(g).reshape(NZ, 2, patches, group)
            own1[:, :, g * patches:(g + 1) * patches] = value

    @pl.when(in_second)
    def _():
        for g in range(4):
            value = partial_product(g).reshape(2, 2, half_rows, group)
            own1[g] = value[0]
            own1[4 + g] = value[1]

    def by_section(action):
        pl.when(in_first)(lambda: action(short_rows))
        pl.when(in_second)(lambda: action(half_rows))

    up1, down1 = {}, {}

    def hop1(stage, h, upward):
        send_buf, recv_buf = (zs1_p, zr1_p) if upward else (zs1_m, zr1_m)
        table = up1 if upward else down1
        device = up_z if upward else down_z
        block = around(4 - stage) if upward else around(stage - 4)
        value = own1[block, h]
        if stage >= 2 or (stage == 1 and h == (0 if upward else 1)):
            sem = table[(stage - 1, h)]
            by_section(lambda n: remote(
                recv_buf.at[stage - 1, h, 0:n], recv_buf.at[stage - 1, h, 0:n], sem, device).wait_recv())
            value = value + recv_buf[stage - 1, h].astype(F32)
        send_buf[stage, h] = value.astype(BF16)
        sem_out = next(sems)
        table[(stage, h)] = sem_out
        by_section(lambda n: remote(
            send_buf.at[stage, h, 0:n], recv_buf.at[stage, h, 0:n], sem_out, device).start())
        sent.append(lambda: by_section(lambda n: remote(
            send_buf.at[stage, h, 0:n], recv_buf.at[stage, h, 0:n], sem_out, device).wait_send()))

    hop1(0, 0, True)
    hop1(0, 1, False)
    for stage in (1, 2, 3):
        hop1(stage, 1, True)
        hop1(stage, 0, False)
        hop1(stage, 0, True)
        hop1(stage, 1, False)
    for h in (1, 0):
        by_section(lambda n: remote(zr1_p.at[3, h, 0:n], zr1_p.at[3, h, 0:n], up1[(3, h)], up_z).wait_recv())
        by_section(lambda n: remote(zr1_m.at[3, h, 0:n], zr1_m.at[3, h, 0:n], down1[(3, h)], down_z).wait_recv())

    def summed(h):
        return own1[z, h] + zr1_p[3, h].astype(F32) + zr1_m[3, h].astype(F32)

    has_head = jnp.logical_and(in_second, jnp.logical_not(wide(z)))

    @pl.when(has_head)
    def _():
        value = jnp.concatenate([summed(0), summed(1)], axis=0).astype(BF16)
        result = attend(value[:, 0:HEAD], value[:, HEAD:2 * HEAD], value[:, 2 * HEAD:3 * HEAD])
        acts1[z, :, :, 0:HEAD] = result.reshape(2, half_rows, HEAD)

    @pl.when(jnp.logical_not(has_head))
    def _():
        for h in range(2):
            acts1[z, h] = gelu(summed(h))

    def by_kind(block, action):
        pl.when(in_first)(lambda: action(short_rows, group))
        is_wide = wide(block)
        pl.when(jnp.logical_and(in_second, is_wide))(lambda: action(half_rows, group))
        pl.when(jnp.logical_and(in_second, jnp.logical_not(is_wide)))(lambda: action(half_rows, HEAD))

    gather1 = {}

    def pass_on1(stage, h, upward):
        block = around(-stage) if upward else around(stage)
        sem = next(sems)
        gather1[(stage, h, upward)] = sem
        device = up_z if upward else down_z

        def copy(n, w):
            part = acts1.at[block, h, 0:n, 0:w]
            return remote(part, part, sem, device)

        by_kind(block, lambda n, w: copy(n, w).start())
        sent.append(lambda: by_kind(block, lambda n, w: copy(n, w).wait_send()))

    def arrived1(stage, h, upward):
        block = around(-1 - stage) if upward else around(1 + stage)
        device = up_z if upward else down_z
        by_kind(block, lambda n, w: remote(
            acts1.at[block, h, 0:n, 0:w], acts1.at[block, h, 0:n, 0:w], gather1[(stage, h, upward)], device).wait_recv())

    for h in range(2):
        for upward in (True, False):
            pass_on1(0, h, upward)
    for stage in range(4):
        for h in range(2):
            for upward in (True, False):
                if stage == 3 and h != (0 if upward else 1):
                    continue
                arrived1(stage, h, upward)
                if stage < 2 or (stage == 2 and h == (0 if upward else 1)):
                    pass_on1(stage + 1, h, upward)

    @pl.when(in_first)
    def _():
        for k in range(2):
            total = None
            for g in range(3):
                hidden = acts1[:, :, g * patches:(g + 1) * patches].reshape(n_tok, group)
                term = jnp.dot(hidden, w1_mix[k, g * group:(g + 1) * group], preferred_element_type=F32)
                total = term if total is None else total + term
            acc1[k] = total

    @pl.when(in_second)
    def _():
        for image in range(2):
            first = image * 4
            value = jnp.concatenate(
                [acts1[first + j, :, :, 0:HEAD].reshape(2 * half_rows, HEAD) for j in range(3)]
                + [acts1[first + 3].reshape(2 * half_rows, group)], axis=1)
            for k in range(2):
                acc1[k, image * 2 * half_rows:(image + 1) * 2 * half_rows] = jnp.dot(
                    value, w1_mix[k, 0:2 * group], preferred_element_type=F32)

    for k in range(2):
        mix1_s[k] = acc1[k].astype(BF16).reshape(2, n_x, 2, patches, feats)
    both_dims = (slice(None), slice(None))
    total = col_sum(
        mix1_s, mix_d, mix_t, mix_r, lambda ref, *at: ref.at[(*both_dims, *at)],
        lambda ref, *at: ref[(*both_dims, *at)])
    ys1[...] = total.astype(BF16)
    to_pair, to_outer, to_diagonal = next(sems), next(sems), next(sems)

    @pl.when(in_first)
    def _():
        copies = [remote(ys1.at[other], yr1.at[1], to_outer, outer), remote(ys1.at[yb], yr1.at[2], to_diagonal, diagonal)]
        for copy in copies:
            copy.start()
        for copy in copies:
            copy.wait_send()

    @pl.when(in_second)
    def _():
        copy = remote(ys1.at[other], yr1.at[0], to_pair, pair)
        copy.start()
        copy.wait()
        remote(yr1.at[1], yr1.at[1], to_outer, outer).wait_recv()
        remote(yr1.at[2], yr1.at[2], to_diagonal, diagonal).wait_recv()
        result = xb1[yb].astype(F32) + ys1[yb].astype(F32)
        for k in range(3):
            result = result + yr1[k].astype(F32)
        y_ref[...] = result.astype(BF16)

    assert next(sems) < 208
    for wait in sent:
        wait()


def layers(x, weights):
    gain, wq, wk, wv, wup, wout, wdown = weights
    n_col = lax.axis_size("col")
    images, patches, feats = x.shape
    half = n_col // 2 * patches
    wide_in = 6 * HEAD
    vmem = pl.BlockSpec(memory_space=pltpu.VMEM)
    anywhere = pl.BlockSpec(memory_space=pl.ANY)
    z_buf = pltpu.VMEM((4, 2, half, wide_in), BF16)
    y_buf = pltpu.VMEM((4, 2, half // 2, wide_in), BF16)
    z1_buf = pltpu.VMEM((4, 2, 4 * patches, feats), BF16)
    pair_buf = pltpu.VMEM((NZ, half, wide_in), BF16)
    scratch = [
        pltpu.VMEM((NZ, feats, wide_in), BF16),
        pltpu.VMEM((NZ, wide_in, feats), BF16),
        pltpu.VMEM((2, n_col, patches, feats), BF16),
        pltpu.VMEM((NZ, 2, 2, half, wide_in), F32),
        pltpu.VMEM((2 * NZ, 8, 128), F32),
        z_buf, z_buf, z_buf, z_buf, y_buf, y_buf, y_buf, y_buf, pair_buf, pair_buf,
        pltpu.VMEM((half, wide_in), BF16), pltpu.VMEM((half, wide_in), BF16),
        pltpu.VMEM((2 * half, wide_in), F32),
        pltpu.VMEM((2, NZ, 2 * half, wide_in), BF16),
        pltpu.VMEM((2, 2 * half, feats), F32),
        pltpu.VMEM((2, n_col // 2, 2, patches, feats), BF16),
        pltpu.VMEM((2, n_col, 8, 128), F32),
        pltpu.VMEM((2, 2, n_col // 2, patches, feats), BF16),
        pltpu.VMEM((2, 2, n_col // 2, patches, feats), BF16),
        pltpu.VMEM((4, 2, feats, feats), BF16),
        pltpu.VMEM((2, 3 * feats, feats), BF16),
        pltpu.VMEM((2, 8, feats), F32),
        pltpu.VMEM((2, 2, patches, feats), BF16),
        pltpu.VMEM((2, 2, n_col, patches, feats), BF16),
        pltpu.VMEM((NZ, 2, 4 * patches, feats), F32),
        pltpu.VMEM((NZ, 8, 128), F32),
        z1_buf, z1_buf, z1_buf, z1_buf,
        pltpu.VMEM((NZ, 2, 4 * patches, feats), BF16),
        pltpu.VMEM((2, 2 * n_col * patches, feats), F32),
        pltpu.VMEM((2, 2, n_col // 2, 2, patches, feats), BF16),
        pltpu.VMEM((3, 2, 2, patches, feats), BF16),
        pltpu.VMEM((2, 2, patches, feats), BF16),
        pltpu.VMEM((3, 2, patches, feats), BF16),
        pltpu.SemaphoreType.DMA((40,)),
        pltpu.SemaphoreType.DMA((208,)),
        pltpu.SemaphoreType.DMA((208,)),
    ]
    return pl.pallas_call(
        functools.partial(layers_kernel, n_col, patches, feats),
        out_shape=jax.ShapeDtypeStruct(x.shape, BF16),
        in_specs=[vmem, vmem] + [anywhere] * 6,
        out_specs=vmem,
        scratch_shapes=scratch,
        compiler_params=pltpu.CompilerParams(
            collective_id=0, has_side_effects=True, vmem_limit_bytes=67043328
        ),
    )(x, gain[None], wq, wk, wv, wup, wout, wdown)


def local(tokens, ln_gain, w_query, w_key, w_value, w_up, w_out, w_down):
    weights = (ln_gain[0], w_query[0], w_key[0], w_value[0], w_up[0], w_out[0], w_down[0])
    return layers(tokens, weights)[None]


def solution(mesh):
    return jax.shard_map(
        local,
        mesh=mesh,
        in_specs=(
            P(None, "col", "row"),
            P("section", "row"),
            P("section", "row", "col"),
            P("section", "row", "col"),
            P("section", "row", "col"),
            P("section", "row", "col"),
            P("section", "col", "row"),
            P("section", "col", "row"),
        ),
        out_specs=P("section", None, "col", "row"),
        check_vma=False,
    )
```

```python
import functools
import math

import jax
import jax.numpy as jnp
from jax import lax
from jax.experimental import pallas as pl
from jax.experimental.pallas import tpu as pltpu
from jax.sharding import PartitionSpec as P

D = 6144
HEAD = 128
EPS = 1e-06
NZ = 8
MESH = pl.DeviceIdType.MESH
BF16 = jnp.bfloat16
F32 = jnp.float32


def wide(block):
    return lax.rem(block, 4) == 3


def either(condition, yes, no):
    def run(action):
        def branch():
            action()

        return branch

    lax.cond(condition, run(yes), run(no))


def by_width(block, narrow_size, wide_size, action):
    either(wide(block), lambda: action(wide_size), lambda: action(narrow_size))


def layers_kernel(
    n_col, patches, feats,
    x_ref, gain_ref, wq_ref, wk_ref, wv_ref, wup_ref, wout_ref, wdn_ref,
    y_ref,
    w_in, w_mix, w_main, w_g, w_gs, w_ms, gathered, gain0, own, own_g, stat,
    gs_p, gs_m, gr_p, gr_m, zs_p, zs_m, zr_p, zr_m, ys_p, ys_m, yr_p, yr_m, pair_s, pair_r, last_s, last_r,
    full, acts, acc,
    stat_col, xraw, terms, mix_d, mix_t, mix_e,
    w1_in, w1_mix, gain1, xb1, gathered1, own1, stat1, zs1_p, zs1_m, zr1_p, zr1_m,
    acts1, acc1, mix1_s, mix_r, ys1, yr1,
    w_sem, ssem, rsem,
):
    section = lax.axis_index("section")
    row = lax.axis_index("row")
    col = lax.axis_index("col")
    n_row = 2 * NZ
    yb = lax.div(row, NZ)
    z = lax.rem(row, NZ)
    other = 1 - yb

    def around(step):
        return lax.rem(z + step + NZ, NZ)

    up_z = {"row": yb * NZ + around(1)}
    down_z = {"row": yb * NZ + around(-1)}
    pair = {"row": other * NZ + z}
    outer = {"section": 1 - section, "row": other * NZ + z}
    diagonal = {"section": 1 - section, "row": row}
    n_x = n_col // 2
    core = lax.rem(col, 2)
    chip_x = lax.div(col, 2)
    sibling = {"col": 2 * chip_x + 1 - core}

    def along_x(step):
        return lax.rem(chip_x + step, n_x)

    def same_core(step):
        return {"col": 2 * along_x(step) + core}
    in_first = section == 0
    in_second = section == 1

    narrow_mix, wide_mix = 3 * HEAD, 6 * HEAD

    barrier = pltpu.get_barrier_semaphore()
    for step in range(1, n_row):
        pl.semaphore_signal(barrier, inc=1, device_id={"row": lax.rem(row + step, n_row)}, device_id_type=MESH)
    for step in range(1, n_col):
        pl.semaphore_signal(barrier, inc=1, device_id={"col": lax.rem(col + step, n_col)}, device_id_type=MESH)
    for device in (outer, diagonal):
        pl.semaphore_signal(barrier, inc=1, device_id=device, device_id_type=MESH)

    sems = iter(range(1000))

    def remote(source, target, sem, device):
        return pltpu.make_async_remote_copy(
            src_ref=source, dst_ref=target, send_sem=ssem.at[sem], recv_sem=rsem.at[sem],
            device_id=device, device_id_type=MESH,
        )

    def ready():
        pl.semaphore_wait(barrier, n_row - 1 + n_col - 1 + 2)

    def column_stats(sums, squares):
        columns = jnp.concatenate(
            [jnp.broadcast_to(sums, (2 * patches, 128)), jnp.broadcast_to(squares, (2 * patches, 128))], axis=0
        )
        return columns.T[0:8]

    def lane_stats(total):
        mean = total * (1.0 / D)
        lane = lax.broadcasted_iota(jnp.int32, (8, 128), 1)
        shifted = pltpu.roll(mean, 2 * patches, axis=1)
        var = jnp.maximum(mean - shifted * shifted, 0.0)
        return jnp.where(lane < 2 * patches, mean, lax.rsqrt(var + EPS))

    def to_columns(table):
        rows = table[:, 0, :]
        return jnp.concatenate([rows] * (128 // n_col), axis=0).T

    def normalise(block, columns, c, gain):
        value = block.astype(F32).reshape(2 * patches, feats)
        mean, scale = columns[0:2 * patches, c:c + 1], columns[2 * patches:4 * patches, c:c + 1]
        return ((value - mean) * scale * gain).astype(BF16).reshape(2, patches, feats)

    def col_gather(view):
        arrive = []
        for step in (1, 3, 2):
            copy = remote(view(col), view(col), next(sems), same_core(step))
            copy.start()
            arrive.append((copy, step))
        first = remote(view(col), view(col), next(sems), sibling)
        first.start()

        def finish():
            handed = [first]
            for copy, step in arrive:
                copy.wait()
                block = view(2 * along_x(n_x - step) + core)
                onward = remote(block, block, next(sems), sibling)
                onward.start()
                handed.append(onward)
            for copy in handed:
                copy.wait()

        return finish

    def gelu(value):
        return (0.5 * value * (1.0 + lax.erf(value * math.sqrt(0.5)))).astype(BF16)

    def attend(query, keyed, valued):
        scores = lax.dot_general(query, keyed, (((1,), (1,)), ((), ())), preferred_element_type=F32)
        scores = scores * (1.0 / math.sqrt(HEAD))
        expo = jnp.exp(scores - jnp.max(scores, axis=-1, keepdims=True))
        probs = (expo / jnp.sum(expo, axis=-1, keepdims=True)).astype(BF16)
        return jnp.dot(probs, valued, preferred_element_type=F32).astype(BF16)

    def col_peers():
        for dx in (2, 1, 3, 0):
            for dc in range(2):
                if dx or dc:
                    target_core = lax.rem(core + dc, 2)
                    yield 2 * dx + dc - 1, along_x(dx), target_core, {"col": 2 * along_x(dx) + target_core}

    def col_direct(view):
        copies = []
        for _, _, _, device in col_peers():
            copy = remote(view(col), view(col), next(sems), device)
            copy.start()
            copies.append(copy)
        return copies

    def col_sum():
        copies = []
        for slot, target_x, target_core, device in col_peers():
            copy = remote(mix1_s.at[:, :, target_x, target_core], mix_r.at[slot], next(sems), device)
            copy.start()
            copies.append((copy, slot))
        value = mix1_s[:, :, chip_x, core].astype(F32)
        for copy, slot in copies:
            copy.wait()
            value = value + mix_r[slot].astype(F32)
        return value

    def col_sum_by_core():
        swap = remote(mix1_s.at[:, :, :, 1 - core], mix_d, next(sems), sibling)
        swap.start()
        swap.wait()
        copies = []
        for step in (2, 1, 3):
            target = along_x(step)
            mix_t[:, :, target] = (
                mix1_s[:, :, target, core].astype(F32) + mix_d[:, :, target].astype(F32)).astype(BF16)
            copy = remote(mix_t.at[:, :, target], mix_e.at[step - 1], next(sems), same_core(step))
            copy.start()
            copies.append((copy, step - 1))
        value = mix1_s[:, :, chip_x, core].astype(F32) + mix_d[:, :, chip_x].astype(F32)
        for copy, slot in copies:
            copy.wait()
            value = value + mix_e[slot].astype(F32)
        return value

    group = feats
    block_sems = {name: [next(sems) for _ in range(n)] for name, n in
                  (("pair", 5), ("outer", 5), ("via", 5), ("forward", 5), ("gain", 3))}
    mlp_first = 2 * group
    mlp_rest = 3 * group

    def head_cols(member, j):
        return pl.ds(pl.multiple_of((member * 3 + j) * HEAD, HEAD), HEAD)

    def third(at, g):
        return w_in.at[at + g // 2, :, (g % 2) * group:(g % 2 + 1) * group]

    @pl.when(in_second)
    def ship():
        copies = []

        def fetch(source, target):
            copy = pltpu.make_async_copy(source, target, w_sem.at[len(copies)])
            copy.start()
            copies.append(copy)

        start = pl.multiple_of(mlp_first + yb * mlp_rest, group)
        fetch(wup_ref.at[:, pl.ds(start, 2 * group)], w_in.at[4])
        fetch(wup_ref.at[:, pl.ds(pl.multiple_of(start + 2 * group, group), group)], w_in.at[5, :, 0:group])
        fetch(wdn_ref.at[pl.ds(start, 2 * group)], w_mix.at[3])
        fetch(wdn_ref.at[pl.ds(pl.multiple_of(start + 2 * group, group), group)], w_mix.at[4, 0:group])
        n_via = len(copies)
        start = pl.multiple_of(mlp_first + other * mlp_rest, group)
        fetch(wup_ref.at[:, pl.ds(start, 2 * group)], w_in.at[2])
        fetch(wup_ref.at[:, pl.ds(pl.multiple_of(start + 2 * group, group), group)], w_in.at[3, :, 0:group])
        fetch(wdn_ref.at[pl.ds(start, 2 * group)], w_mix.at[1])
        fetch(wdn_ref.at[pl.ds(pl.multiple_of(start + 2 * group, group), group)], w_mix.at[2, 0:group])
        n_outer = len(copies)
        for member, mine in ((other, False), (yb, True)):
            for j in range(3):
                for k, w_ref in enumerate((wq_ref, wk_ref, wv_ref)):
                    span = slice(k * HEAD, (k + 1) * HEAD)
                    at = (j % 2) * group + k * HEAD
                    target = w1_in.at[j, yb, :, span] if mine else w_in.at[j // 2, :, at:at + HEAD]
                    fetch(w_ref.at[:, head_cols(member, j)], target)
            rows = pl.ds(pl.multiple_of(member * group, group), group)
            fetch(wup_ref.at[:, rows], w1_in.at[3, yb] if mine else w_in.at[1, :, group:2 * group])
            fetch(wout_ref.at[rows], w1_mix.at[yb, 0:group] if mine else w_mix.at[0, 0:group])
            fetch(wdn_ref.at[rows], w1_mix.at[yb, group:2 * group] if mine else w_mix.at[0, group:2 * group])
            if not mine:
                n_pair = len(copies)
        gain1[yb] = jnp.broadcast_to(gain_ref[...], (8, feats))
        ready()
        out = []

        def send(source, target, sem, device):
            copy = remote(source, target, sem, device)
            copy.start()
            out.append(copy)

        for copy in copies[:n_via]:
            copy.wait()
        for g in range(3):
            send(third(4, g), third(6, g), block_sems["via"][g], pair)
        send(w_mix.at[3], w_mix.at[5], block_sems["via"][3], pair)
        send(w_mix.at[4, 0:group], w_mix.at[6, 0:group], block_sems["via"][4], pair)
        for copy in copies[n_via:n_outer]:
            copy.wait()
        for g in range(3):
            send(third(2, g), w1_in.at[g, yb], block_sems["outer"][g], outer)
        send(w_mix.at[1], w1_mix.at[yb, 0:2 * group], block_sems["outer"][3], outer)
        send(w_mix.at[2, 0:group], w1_mix.at[yb, 2 * group:3 * group], block_sems["outer"][4], outer)
        for copy in copies[n_outer:n_pair]:
            copy.wait()
        for g in range(4):
            send(third(0, g), w1_in.at[g, yb], block_sems["pair"][g], pair)
        send(w_mix.at[0], w1_mix.at[yb, 0:2 * group], block_sems["pair"][4], pair)
        for device, sem in zip((pair, outer, diagonal), block_sems["gain"]):
            send(gain1.at[yb], gain1.at[yb], sem, device)
        for g in range(3):
            remote(third(6, g), third(6, g), block_sems["via"][g], pair).wait_recv()
            send(third(6, g), w1_in.at[g, other], block_sems["forward"][g], outer)
        remote(w_mix.at[5], w_mix.at[5], block_sems["via"][3], pair).wait_recv()
        send(w_mix.at[5], w1_mix.at[other, 0:2 * group], block_sems["forward"][3], outer)
        remote(w_mix.at[6, 0:group], w_mix.at[6, 0:group], block_sems["via"][4], pair).wait_recv()
        send(w_mix.at[6, 0:group], w1_mix.at[other, 2 * group:3 * group], block_sems["forward"][4], outer)
        for copy in copies[n_pair:]:
            copy.wait()
        for g in range(4):
            remote(w1_in.at[g, other], w1_in.at[g, other], block_sems["pair"][g], pair).wait_recv()
        remote(w1_mix.at[other, 0:2 * group], w1_mix.at[other, 0:2 * group], block_sems["pair"][4], pair).wait_recv()
        remote(gain1.at[other], gain1.at[other], block_sems["gain"][0], pair).wait_recv()
        for copy in out:
            copy.wait_send()

    def pieces_of_ring(copy, after=None):
        ring_sem = {}

        def onward(stage, piece, upward):
            block = around(-stage) if upward else around(stage)
            sem = next(sems)
            ring_sem[(stage, piece, upward)] = sem
            copy(block, piece, sem, up_z if upward else down_z, "start")
            sent.append(lambda: copy(block, piece, sem, up_z if upward else down_z, "wait_send"))

        def last(piece, upward):
            return (piece < 2) == upward

        for piece in (2, 3, 0, 1):
            onward(0, piece, True)
            onward(0, (piece + 2) % 4, False)
        if after is not None:
            after(-1)
        for stage in range(4):
            for piece in (2, 3, 0, 1):
                for upward in (True, False):
                    p = piece if upward else (piece + 2) % 4
                    if stage == 3 and not last(p, upward):
                        continue
                    block = around(-1 - stage) if upward else around(1 + stage)
                    copy(block, p, ring_sem[(stage, p, upward)], up_z if upward else down_z, "wait_recv")
                    if stage < 2 or (stage == 2 and last(p, upward)):
                        onward(stage + 1, p, upward)
            if after is not None:
                after(stage)

    sent = []
    main_n, main_w, part_g = 3 * HEAD, 4 * HEAD, 2 * HEAD
    image_rows = n_col * patches
    late = image_rows // 2
    early = image_rows - late
    y_rows = early // 2

    def member_hidden(member, g):
        if g == 3:
            start = 6 * part_g + member * 3 * part_g
            return start, start + main_w
        start = (member * 3 + g) * part_g
        return start, start

    def first_layer():
        waits = {"stage": [], "own": [], "mix": [], "mix_stage": []}
        count = iter(range(1000))

        def fetch(source, target, kind):
            copy = pltpu.make_async_copy(source, target, w_sem.at[next(count)])
            copy.start()
            waits[kind].append(copy)

        def columns_at(start, size):
            return pl.ds(pl.multiple_of(start, HEAD), size)

        for g in range(4):
            fetch(wup_ref.at[:, columns_at(member_hidden(other, g)[1], part_g)], w_gs.at[g], "stage")
        for g in range(4):
            fetch(wup_ref.at[:, columns_at(member_hidden(yb, g)[1], part_g)], w_g.at[g, yb], "own")
        for block in range(NZ):
            member, g = block // 4, block % 4
            if g == 3:
                start = member_hidden(member, g)[0]
                fetch(wup_ref.at[:, start:start + main_w], w_main.at[block], "own")
            else:
                cols = slice((member * 3 + g) * HEAD, (member * 3 + g + 1) * HEAD)
                for k, w_ref in enumerate((wq_ref, wk_ref, wv_ref)):
                    fetch(w_ref.at[:, cols], w_main.at[block, :, k * HEAD:(k + 1) * HEAD], "own")
        for member, kind in ((other, "mix_stage"), (yb, "mix")):
            for g in range(4):
                target = w_ms.at[g] if kind == "mix_stage" else w_mix.at[yb * 4 + g]
                rows = columns_at(member_hidden(member, g)[0], wide_mix if g == 3 else part_g)
                if g == 3:
                    fetch(wdn_ref.at[rows], target, kind)
                else:
                    fetch(wout_ref.at[columns_at((member * 3 + g) * HEAD, HEAD)], target.at[0:HEAD], kind)
                    fetch(wdn_ref.at[rows], target.at[HEAD:narrow_mix], kind)

        xf = x_ref[...].astype(F32).reshape(2 * patches, feats)
        sums = jnp.sum(xf, axis=-1, keepdims=True)
        squares = jnp.sum(xf * xf, axis=-1, keepdims=True)
        stat[row] = column_stats(sums, squares)
        xraw[yb] = x_ref[...]
        gathered[yb, :, col] = x_ref[...]
        gain0[yb] = jnp.broadcast_to(gain_ref[...], (8, feats))
        ready()
        x_copy = remote(xraw.at[yb], xraw.at[yb], x_spread[0], pair)
        x_copy.start()
        stat_copies = []
        for step in range(1, n_row):
            copy = remote(stat.at[row], stat.at[row], next(sems), {"row": lax.rem(row + step, n_row)})
            copy.start()
            stat_copies.append(copy)
        finish_own = col_gather(lambda c: gathered.at[yb, :, c])
        gain_copy = remote(gain0.at[yb], gain0.at[yb], next(sems), pair)
        gain_copy.start()
        for device, sem in ((outer, x_spread[1]), (diagonal, x_spread[2])):
            copy = remote(xraw.at[yb], xraw.at[yb], sem, device)
            copy.start()
            sent.append(copy.wait_send)

        def group_at(i):
            return lax.rem(z + (0, 3, 1, 2)[i], 4)

        def traced_group_at(i):
            return lax.rem(z + jnp.where(i == 0, 0, jnp.where(i == 1, 3, i - 1)), 4)

        g_base = next(sems)
        for _ in range(3):
            next(sems)
        for copy in waits["stage"]:
            copy.wait()
        for i in range(4):
            g = group_at(i)
            copy = remote(w_gs.at[g], w_g.at[g, yb], g_base + i, pair)
            copy.start()
            sent.append(copy.wait_send)
        x_copy.wait()
        gathered[other, :, col] = xraw[other]
        finish_other = col_gather(lambda c: gathered.at[other, :, c])
        finish_own()
        for copy in stat_copies:
            copy.wait()
        stat_col[0, col] = lane_stats(jnp.sum(stat[...], axis=0))
        finish_stats = col_direct(lambda c: stat_col.at[0, c])
        for copy in waits["own"]:
            copy.wait()
        finish_other()
        for copy in finish_stats:
            copy.wait()
        gain_copy.wait()
        columns = to_columns(stat_col[0])
        for c in range(n_col):
            for k in range(2):
                gathered[k, :, c] = normalise(gathered[k, :, c], columns, c, gain0[k, 0:1])

        bufs = {
            "G": (gs_p, gs_m, gr_p, gr_m), "Z": (zs_p, zs_m, zr_p, zr_m), "Y": (ys_p, ys_m, yr_p, yr_m),
        }
        tables = {True: {}, False: {}}
        pair_base = next(sems)
        for _ in range(NZ - 1):
            next(sems)

        def by_part(kind, block, action):
            if kind == "G":
                action(part_g)
            else:
                by_width(block, main_n, main_w, action)

        def move(kind, source, target, sem, device, block, what):
            by_part(kind, block, lambda w: getattr(remote(source.at[:, 0:w], target.at[:, 0:w], sem, device), what)())

        def ring_block(stage, upward):
            return around(4 - stage) if upward else around(stage - 4)

        def term(kind, h, block):
            g, image = lax.rem(block, 4), lax.div(block, 4)
            if kind == "G":
                return own_g[g, image, h]
            if kind == "Z":
                return own[h * 4 + g, image, early:image_rows]
            return own[yb * 4 + g, image, h * y_rows:(h + 1) * y_rows]

        def reserve(kind, stage, h, upward):
            sem = next(sems)
            tables[upward][(kind, stage, h)] = sem
            send_buf = bufs[kind][0 if upward else 1].at[stage, h]
            device = up_z if upward else down_z
            block = ring_block(stage, upward)
            sent.append(lambda: move(kind, send_buf, send_buf, sem, device, block, "wait_send"))

        def hop(kind, stage, h, upward):
            send_buf = bufs[kind][0 if upward else 1]
            recv_buf = bufs[kind][2 if upward else 3]
            device = up_z if upward else down_z
            block = ring_block(stage, upward)
            value = term(kind, h, block)
            if stage >= 2 or (stage == 1 and h == (0 if upward else 1)):
                buf = recv_buf.at[stage - 1, h]
                move(kind, buf, buf, tables[upward][(kind, stage - 1, h)], device, block, "wait_recv")
                value = value + recv_buf[stage - 1, h].astype(F32)
            send_buf[stage, h] = value.astype(BF16)
            if (kind, stage, h) not in tables[upward]:
                reserve(kind, stage, h, upward)
            move(kind, send_buf.at[stage, h], recv_buf.at[stage, h], tables[upward][(kind, stage, h)], device, block, "start")

        for kind in ("G", "Z"):
            reserve(kind, 0, 0, True)
            reserve(kind, 0, 1, False)
            reserve(kind, 1, 1, True)
            reserve(kind, 1, 0, False)

        def order(i):
            away = 4 - lax.div(i + 1, 2)
            return around(jnp.where(lax.rem(i, 2) == 1, away, -away))

        def send_pair(i):
            block = order(i)
            pair_s[i] = own[other * 4 + lax.rem(block, 4), lax.div(block, 4), 0:early].astype(BF16)
            move("Y", pair_s.at[i], pair_r.at[i], pair_base + i, pair, block, "start")

        n_tok = 2 * image_rows

        def product(i, carry):
            g = traced_group_at(i)
            for member in range(2):
                own[member * 4 + g] = jnp.dot(
                    gathered[yb].reshape(n_tok, feats), w_main[member * 4 + g], preferred_element_type=F32
                ).reshape(2, image_rows, main_w)

            @pl.when(i == 0)
            def _():
                hop("Z", 0, 0, True)
                hop("Z", 0, 1, False)

            @pl.when(i == 1)
            def _():
                hop("Z", 1, 1, True)

            @pl.when(i == 2)
            def _():
                hop("Z", 1, 0, False)

            send_pair(i)
            return carry

        def product_g(i, carry):
            g = traced_group_at(i)
            remote(w_g.at[g, other], w_g.at[g, other], g_base + i, pair).wait_recv()
            own_g[g] = (
                jnp.dot(gathered[0].reshape(n_tok, feats), w_g[g, 0], preferred_element_type=F32)
                + jnp.dot(gathered[1].reshape(n_tok, feats), w_g[g, 1], preferred_element_type=F32)
            ).reshape(2, 2, image_rows // 2, part_g)

            @pl.when(i == 0)
            def _():
                hop("G", 0, 0, True)
                hop("G", 0, 1, False)

            @pl.when(i == 1)
            def _():
                hop("G", 1, 1, True)

            @pl.when(i == 2)
            def _():
                hop("G", 1, 0, False)

            return carry

        lax.fori_loop(0, 4, product, 0)

        def rest_of_pair(i, carry):
            send_pair(i)
            return carry

        lax.fori_loop(4, NZ, rest_of_pair, 0)
        for copy in waits["mix_stage"]:
            copy.wait()
        mix_sems = [next(sems) for _ in range(4)]

        def send_mix(g):
            n = wide_mix if g == 3 else narrow_mix
            copy = remote(w_ms.at[g, 0:n], w_mix.at[yb * 4 + g, 0:n], mix_sems[g], pair)
            copy.start()
            sent.append(copy.wait_send)

        for i in range(NZ):
            sent.append(lambda i=i: move(
                "Y", pair_s.at[i], pair_s.at[i], pair_base + i, pair, order(jnp.int32(i)), "wait_send"))

        def pair_sum(i):
            block = order(jnp.int32(i))
            move("Y", pair_r.at[i], pair_r.at[i], pair_base + i, pair, block, "wait_recv")
            at = own.at[yb * 4 + lax.rem(block, 4), lax.div(block, 4), 0:early]
            at[...] = at[...] + pair_r[i].astype(F32)

        def four(kind, stage, before=(None, None)):
            for sums, h, upward in ((before[0], 1, True), (before[1], 0, False), (None, 0, True), (None, 1, False)):
                if sums is not None:
                    pair_sum(sums)
                hop(kind, stage, h, upward)

        def all_in(kind):
            for h, upward in ((1, True), (0, False), (0, True), (1, False)):
                buf = bufs[kind][2 if upward else 3].at[3, h]
                move(kind, buf, buf, tables[upward][(kind, 3, h)], up_z if upward else down_z, z, "wait_recv")

        hop("Z", 1, 0, True)
        hop("Z", 1, 1, False)
        lax.fori_loop(0, 1, product_g, 0)
        four("Z", 2)
        lax.fori_loop(1, 3, product_g, 0)
        four("Z", 3)
        lax.fori_loop(3, 4, product_g, 0)
        hop("G", 1, 0, True)
        hop("G", 1, 1, False)
        pair_sum(0)
        hop("Y", 0, 0, True)
        hop("Y", 0, 1, False)
        four("G", 2)
        all_in("Z")
        last_s[...] = (term("Z", other, z) + zr_p[3, other].astype(F32) + zr_m[3, other].astype(F32)).astype(BF16)
        last_sem = next(sems)
        move("Z", last_s, last_r, last_sem, pair, z, "start")
        sent.append(lambda: move("Z", last_s, last_s, last_sem, pair, z, "wait_send"))
        for g in (3, 0, 1, 2):
            send_mix(g)
        four("Y", 1, (1, 2))
        four("G", 3)
        four("Y", 2, (3, 4))
        four("Y", 3, (5, 6))
        is_wide = wide(z)
        all_in("G")
        for h in range(2):
            hidden = gelu(term("G", h, z) + gr_p[3, h].astype(F32) + gr_m[3, h].astype(F32))

            @pl.when(is_wide)
            def _():
                acts[z, h, :, main_w:wide_mix] = hidden

            @pl.when(jnp.logical_not(is_wide))
            def _():
                acts[z, h, :, HEAD:narrow_mix] = hidden

        full[early:image_rows] = term("Z", yb, z) + zr_p[3, yb].astype(F32) + zr_m[3, yb].astype(F32)
        move("Z", last_r, last_r, last_sem, pair, z, "wait_recv")
        full[early:image_rows] = full[early:image_rows] + last_r[...].astype(F32)
        pair_sum(7)
        all_in("Y")
        for h in range(2):
            full[h * y_rows:(h + 1) * y_rows] = term("Y", h, z) + yr_p[3, h].astype(F32) + yr_m[3, h].astype(F32)

        @pl.when(is_wide)
        def _():
            acts[z, :, :, 0:main_w] = gelu(full[...]).reshape(2, image_rows // 2, main_w)

        @pl.when(jnp.logical_not(is_wide))
        def _():
            value = full[:, 0:main_n].astype(BF16)
            result = attend(value[:, 0:HEAD], value[:, HEAD:2 * HEAD], value[:, 2 * HEAD:3 * HEAD])
            acts[z, :, :, 0:HEAD] = result.reshape(2, image_rows // 2, HEAD)

        piece_rows = image_rows // 4

        def act_copy(block, piece, sem, device, what):
            rows = slice((piece % 2) * piece_rows, (piece % 2 + 1) * piece_rows)

            def action(w):
                part = acts.at[block, piece // 2, rows, 0:w]
                getattr(remote(part, part, sem, device), what)()

            by_width(block, narrow_mix, wide_mix, action)

        def add_product(k, block):
            g, image = lax.rem(block, 4), lax.div(block, 4)

            def add(w):
                acc[k, image] = acc[k, image] + jnp.dot(
                    acts[block, :, :, 0:w].reshape(image_rows, w), w_mix[k * 4 + g, 0:w], preferred_element_type=F32)

            by_width(block, narrow_mix, wide_mix, add)

        def add_known(k, block):
            g, image = block % 4, block // 4
            w = wide_mix if g == 3 else narrow_mix
            acc[k, image] = acc[k, image] + jnp.dot(
                acts[block, :, :, 0:w].reshape(image_rows, w), w_mix[k * 4 + g, 0:w], preferred_element_type=F32)

        acc[...] = jnp.zeros_like(acc)

        def after_stage(stage):
            if stage == -1:
                for copy in waits["mix"]:
                    copy.wait()
                add_product(yb, z)
            elif stage < 3:
                add_product(yb, around(-1 - stage))
                add_product(yb, around(1 + stage))
                if stage == 2:
                    for g in (3, 0, 1, 2):
                        n = wide_mix if g == 3 else narrow_mix
                        part = w_mix.at[other * 4 + g, 0:n]
                        remote(part, part, mix_sems[g], pair).wait_recv()
                        for block in (g, g + 4):
                            pl.when(around(4) != block)(lambda block=block: add_known(other, block))
            else:
                add_product(yb, around(4))
                add_product(other, around(4))

        pieces_of_ring(act_copy, after_stage)

        for k in range(2):
            mix1_s[k] = acc[k].astype(BF16).reshape(2, n_x, 2, patches, feats)
        total = col_sum_by_core()
        terms[yb] = total.astype(BF16)
        for device, sem in ((pair, spread[0]), (outer, spread[1]), (diagonal, spread[2])):
            copy = remote(terms.at[yb], terms.at[yb], sem, device)
            copy.start()
        for wait in sent:
            wait()
        sent.clear()
        for g in range(3):
            remote(w1_in.at[g, other], w1_in.at[g, other], block_sems["outer"][g], outer).wait_recv()
            remote(w1_in.at[g, yb], w1_in.at[g, yb], block_sems["forward"][g], outer).wait_recv()
        for half_k, name in ((other, "outer"), (yb, "forward")):
            for k, (lo, hi) in ((3, (0, 2 * group)), (4, (2 * group, 3 * group))):
                part = w1_mix.at[half_k, lo:hi]
                remote(part, part, block_sems[name][k], outer).wait_recv()
        remote(gain1.at[other], gain1.at[other], block_sems["gain"][1], outer).wait_recv()
        remote(gain1.at[yb], gain1.at[yb], block_sems["gain"][2], diagonal).wait_recv()
        remote(terms.at[other], terms.at[other], spread[0], pair).wait_recv()

    x_spread = [next(sems) for _ in range(3)]
    spread = [next(sems) for _ in range(3)]
    pl.when(in_first)(first_layer)

    @pl.when(in_second)
    def _():
        remote(terms.at[other], terms.at[other], spread[1], outer).wait_recv()
        remote(terms.at[yb], terms.at[yb], spread[2], diagonal).wait_recv()
        remote(xraw.at[other], xraw.at[other], x_spread[1], outer).wait_recv()
        remote(xraw.at[yb], xraw.at[yb], x_spread[2], diagonal).wait_recv()
    for k in range(2):
        xb1[k] = (xraw[k].astype(F32) + terms[0, k].astype(F32) + terms[1, k].astype(F32)).astype(BF16)

    @pl.when(in_first)
    def _():
        y_ref[...] = xb1[yb]

    n_tok = 2 * n_col * patches
    both = xb1[...].astype(F32).reshape(2, 2 * patches, feats)
    sums = jnp.sum(jnp.sum(both, axis=-1, keepdims=True), axis=0)
    squares = jnp.sum(jnp.sum(both * both, axis=-1, keepdims=True), axis=0)
    stat1[z] = column_stats(sums, squares)
    copies = []
    for step in range(1, NZ):
        copy = remote(stat1.at[z], stat1.at[z], next(sems), {"row": yb * NZ + around(step)})
        copy.start()
        copies.append(copy)
    finish_k = []
    for k in range(2):
        gathered1[k, :, col] = xb1[k]
        finish_k.append(col_gather(lambda c, k=k: gathered1.at[k, :, c]))
    for copy in copies:
        copy.wait()
    stat_col[1, col] = lane_stats(jnp.sum(stat1[...], axis=0))
    finish_stats1 = col_direct(lambda c: stat_col.at[1, c])
    for finish in finish_k:
        finish()
    for copy in finish_stats1:
        copy.wait()
    columns1 = to_columns(stat_col[1])
    for c in range(n_col):
        for k in range(2):
            gathered1[k, :, c] = normalise(gathered1[k, :, c], columns1, c, gain1[k, 0:1])

    half_rows = 4 * patches
    short_rows = 3 * patches

    def partial_product(g):
        return (
            jnp.dot(gathered1[0].reshape(n_tok, feats), w1_in[g, 0], preferred_element_type=F32)
            + jnp.dot(gathered1[1].reshape(n_tok, feats), w1_in[g, 1], preferred_element_type=F32)
        )

    @pl.when(in_first)
    def _():
        for g in range(3):
            value = partial_product(g).reshape(NZ, 2, patches, group)
            own1[:, :, g * patches:(g + 1) * patches] = value

    @pl.when(in_second)
    def _():
        for g in range(4):
            value = partial_product(g).reshape(2, 2, half_rows, group)
            own1[g] = value[0]
            own1[4 + g] = value[1]

    def by_section(action):
        either(in_first, lambda: action(short_rows), lambda: action(half_rows))

    up1, down1 = {}, {}

    def hop1(stage, h, upward):
        send_buf, recv_buf = (zs1_p, zr1_p) if upward else (zs1_m, zr1_m)
        table = up1 if upward else down1
        device = up_z if upward else down_z
        block = around(4 - stage) if upward else around(stage - 4)
        value = own1[block, h]
        if stage >= 2 or (stage == 1 and h == (0 if upward else 1)):
            sem = table[(stage - 1, h)]
            by_section(lambda n: remote(
                recv_buf.at[stage - 1, h, 0:n], recv_buf.at[stage - 1, h, 0:n], sem, device).wait_recv())
            value = value + recv_buf[stage - 1, h].astype(F32)
        send_buf[stage, h] = value.astype(BF16)
        sem_out = next(sems)
        table[(stage, h)] = sem_out
        by_section(lambda n: remote(
            send_buf.at[stage, h, 0:n], recv_buf.at[stage, h, 0:n], sem_out, device).start())
        sent.append(lambda: by_section(lambda n: remote(
            send_buf.at[stage, h, 0:n], recv_buf.at[stage, h, 0:n], sem_out, device).wait_send()))

    hop1(0, 0, True)
    hop1(0, 1, False)
    for stage in (1, 2, 3):
        hop1(stage, 1, True)
        hop1(stage, 0, False)
        hop1(stage, 0, True)
        hop1(stage, 1, False)
    for h in (1, 0):
        by_section(lambda n: remote(zr1_p.at[3, h, 0:n], zr1_p.at[3, h, 0:n], up1[(3, h)], up_z).wait_recv())
        by_section(lambda n: remote(zr1_m.at[3, h, 0:n], zr1_m.at[3, h, 0:n], down1[(3, h)], down_z).wait_recv())

    def summed(h):
        return own1[z, h] + zr1_p[3, h].astype(F32) + zr1_m[3, h].astype(F32)

    has_head = jnp.logical_and(in_second, jnp.logical_not(wide(z)))

    @pl.when(has_head)
    def _():
        value = jnp.concatenate([summed(0), summed(1)], axis=0).astype(BF16)
        result = attend(value[:, 0:HEAD], value[:, HEAD:2 * HEAD], value[:, 2 * HEAD:3 * HEAD])
        acts1[z, :, :, 0:HEAD] = result.reshape(2, half_rows, HEAD)

    @pl.when(jnp.logical_not(has_head))
    def _():
        for h in range(2):
            acts1[z, h] = gelu(summed(h))

    def by_kind(block, action):
        either(
            in_first,
            lambda: action(short_rows, group),
            lambda: by_width(block, HEAD, group, lambda w: action(half_rows, w)),
        )

    def act_copy1(block, piece, sem, device, what):
        def action(n, w):
            part = acts1.at[block, piece // 2, (piece % 2) * (n // 2):(piece % 2 + 1) * (n // 2), 0:w]
            getattr(remote(part, part, sem, device), what)()

        by_kind(block, action)

    pieces_of_ring(act_copy1)
    @pl.when(in_first)
    def _():
        for k in range(2):
            total = None
            for g in range(3):
                hidden = acts1[:, :, g * patches:(g + 1) * patches].reshape(n_tok, group)
                term = jnp.dot(hidden, w1_mix[k, g * group:(g + 1) * group], preferred_element_type=F32)
                total = term if total is None else total + term
            acc1[k] = total

    @pl.when(in_second)
    def _():
        for image in range(2):
            first = image * 4
            value = jnp.concatenate(
                [acts1[first + j, :, :, 0:HEAD].reshape(2 * half_rows, HEAD) for j in range(3)]
                + [acts1[first + 3].reshape(2 * half_rows, group)], axis=1)
            for k in range(2):
                acc1[k, image * 2 * half_rows:(image + 1) * 2 * half_rows] = jnp.dot(
                    value, w1_mix[k, 0:2 * group], preferred_element_type=F32)

    for k in range(2):
        mix1_s[k] = acc1[k].astype(BF16).reshape(2, n_x, 2, patches, feats)
    total = col_sum()
    ys1[...] = total.astype(BF16)
    to_pair, to_outer, to_diagonal = next(sems), next(sems), next(sems)

    @pl.when(in_first)
    def _():
        copies = [remote(ys1.at[other], yr1.at[1], to_outer, outer), remote(ys1.at[yb], yr1.at[2], to_diagonal, diagonal)]
        for copy in copies:
            copy.start()
        for copy in copies:
            copy.wait_send()

    @pl.when(in_second)
    def _():
        copy = remote(ys1.at[other], yr1.at[0], to_pair, pair)
        copy.start()
        copy.wait()
        remote(yr1.at[1], yr1.at[1], to_outer, outer).wait_recv()
        remote(yr1.at[2], yr1.at[2], to_diagonal, diagonal).wait_recv()
        result = xb1[yb].astype(F32) + ys1[yb].astype(F32)
        for k in range(3):
            result = result + yr1[k].astype(F32)
        y_ref[...] = result.astype(BF16)

    assert next(sems) < 288
    for wait in sent:
        wait()

    @pl.when(in_first)
    def _():
        for device, sem in ((pair, spread[0]), (outer, spread[1]), (diagonal, spread[2])):
            remote(terms.at[yb], terms.at[yb], sem, device).wait_send()


def layers(x, weights):
    gain, wq, wk, wv, wup, wout, wdown = weights
    n_col = lax.axis_size("col")
    images, patches, feats = x.shape
    wide_in = 6 * HEAD
    vmem = pl.BlockSpec(memory_space=pltpu.VMEM)
    anywhere = pl.BlockSpec(memory_space=pl.ANY)
    rows = n_col * patches
    late = rows // 2
    early = rows - late
    g_buf = pltpu.VMEM((4, 2, rows // 2, 2 * HEAD), BF16)
    z_buf = pltpu.VMEM((4, 2, late, 4 * HEAD), BF16)
    y_buf = pltpu.VMEM((4, 2, early // 2, 4 * HEAD), BF16)
    pair_buf = pltpu.VMEM((NZ, early, 4 * HEAD), BF16)
    z1_buf = pltpu.VMEM((4, 2, 4 * patches, feats), BF16)
    scratch = [
        pltpu.VMEM((NZ, feats, wide_in), BF16),
        pltpu.VMEM((NZ, wide_in, feats), BF16),
        pltpu.VMEM((NZ, feats, 4 * HEAD), BF16),
        pltpu.VMEM((4, 2, feats, 2 * HEAD), BF16),
        pltpu.VMEM((4, feats, 2 * HEAD), BF16),
        pltpu.VMEM((4, wide_in, feats), BF16),
        pltpu.VMEM((2, 2, n_col, patches, feats), BF16),
        pltpu.VMEM((2, 8, feats), F32),
        pltpu.VMEM((NZ, 2, rows, 4 * HEAD), F32),
        pltpu.VMEM((4, 2, 2, rows // 2, 2 * HEAD), F32),
        pltpu.VMEM((2 * NZ, 8, 128), F32),
        g_buf, g_buf, g_buf, g_buf, z_buf, z_buf, z_buf, z_buf, y_buf, y_buf, y_buf, y_buf, pair_buf, pair_buf,
        pltpu.VMEM((late, 4 * HEAD), BF16), pltpu.VMEM((late, 4 * HEAD), BF16),
        pltpu.VMEM((rows, 4 * HEAD), F32),
        pltpu.VMEM((NZ, 2, rows // 2, wide_in), BF16),
        pltpu.VMEM((2, 2, rows, feats), F32),
        pltpu.VMEM((2, n_col, 8, 128), F32),
        pltpu.VMEM((2, 2, patches, feats), BF16),
        pltpu.VMEM((2, 2, 2, patches, feats), BF16),
        pltpu.VMEM((2, 2, n_col // 2, patches, feats), BF16),
        pltpu.VMEM((2, 2, n_col // 2, patches, feats), BF16),
        pltpu.VMEM((n_col // 2 - 1, 2, 2, patches, feats), BF16),
        pltpu.VMEM((4, 2, feats, feats), BF16),
        pltpu.VMEM((2, 3 * feats, feats), BF16),
        pltpu.VMEM((2, 8, feats), F32),
        pltpu.VMEM((2, 2, patches, feats), BF16),
        pltpu.VMEM((2, 2, n_col, patches, feats), BF16),
        pltpu.VMEM((NZ, 2, 4 * patches, feats), F32),
        pltpu.VMEM((NZ, 8, 128), F32),
        z1_buf, z1_buf, z1_buf, z1_buf,
        pltpu.VMEM((NZ, 2, 4 * patches, feats), BF16),
        pltpu.VMEM((2, 2 * n_col * patches, feats), F32),
        pltpu.VMEM((2, 2, n_col // 2, 2, patches, feats), BF16),
        pltpu.VMEM((n_col - 1, 2, 2, patches, feats), BF16),
        pltpu.VMEM((2, 2, patches, feats), BF16),
        pltpu.VMEM((3, 2, patches, feats), BF16),
        pltpu.SemaphoreType.DMA((64,)),
        pltpu.SemaphoreType.DMA((288,)),
        pltpu.SemaphoreType.DMA((288,)),
    ]
    return pl.pallas_call(
        functools.partial(layers_kernel, n_col, patches, feats),
        out_shape=jax.ShapeDtypeStruct(x.shape, BF16),
        in_specs=[vmem, vmem] + [anywhere] * 6,
        out_specs=vmem,
        scratch_shapes=scratch,
        compiler_params=pltpu.CompilerParams(
            collective_id=0, has_side_effects=True, vmem_limit_bytes=67043328
        ),
    )(x, gain[None], wq, wk, wv, wup, wout, wdown)


def local(tokens, ln_gain, w_query, w_key, w_value, w_up, w_out, w_down):
    weights = (ln_gain[0], w_query[0], w_key[0], w_value[0], w_up[0], w_out[0], w_down[0])
    return layers(tokens, weights)[None]


def solution(mesh):
    return jax.shard_map(
        local,
        mesh=mesh,
        in_specs=(
            P(None, "col", "row"),
            P("section", "row"),
            P("section", "row", "col"),
            P("section", "row", "col"),
            P("section", "row", "col"),
            P("section", "row", "col"),
            P("section", "col", "row"),
            P("section", "col", "row"),
        ),
        out_specs=P("section", None, "col", "row"),
        check_vma=False,
    )
```

```python
import functools
import math

import jax
import jax.numpy as jnp
from jax import lax
from jax.experimental import pallas as pl
from jax.experimental.pallas import tpu as pltpu
from jax.sharding import PartitionSpec as P

D = 6144
HEAD = 128
EPS = 1e-06
NZ = 8
MESH = pl.DeviceIdType.MESH
BF16 = jnp.bfloat16
F32 = jnp.float32


def wide(block):
    return lax.rem(block, 4) == 3


def either(condition, yes, no):
    def run(action):
        def branch():
            action()

        return branch

    lax.cond(condition, run(yes), run(no))


def by_width(block, narrow_size, wide_size, action):
    either(wide(block), lambda: action(wide_size), lambda: action(narrow_size))


def layers_kernel(
    n_col, patches, feats,
    x_ref, gain_ref, wq_ref, wk_ref, wv_ref, wup_ref, wout_ref, wdn_ref,
    y_ref,
    w_in, w_mix, w_main, w_g, w_gs, w_ms, gathered, gain0, own, own_g, stat,
    gs_p, gs_m, gr_p, gr_m, zs_p, zs_m, zr_p, zr_m, ys_p, ys_m, yr_p, yr_m, pair_s, pair_r, last_s, last_r,
    full, acts, acc,
    stat_col, xraw, terms, mix_d, mix_t, mix_e,
    w1_in, w1_mix, gain1, xb1, gathered1, own1, stat1, zs1_p, zs1_m, zr1_p, zr1_m,
    acts1, acc1, mix1_s, mix_r, ys1, yr1,
    w_sem, ssem, rsem,
):
    section = lax.axis_index("section")
    row = lax.axis_index("row")
    col = lax.axis_index("col")
    n_row = 2 * NZ
    yb = lax.div(row, NZ)
    z = lax.rem(row, NZ)
    other = 1 - yb

    def around(step):
        return lax.rem(z + step + NZ, NZ)

    up_z = {"row": yb * NZ + around(1)}
    down_z = {"row": yb * NZ + around(-1)}
    pair = {"row": other * NZ + z}
    outer = {"section": 1 - section, "row": other * NZ + z}
    diagonal = {"section": 1 - section, "row": row}
    n_x = n_col // 2
    core = lax.rem(col, 2)
    chip_x = lax.div(col, 2)
    sibling = {"col": 2 * chip_x + 1 - core}

    def along_x(step):
        return lax.rem(chip_x + step, n_x)

    def same_core(step):
        return {"col": 2 * along_x(step) + core}
    in_first = section == 0
    in_second = section == 1

    narrow_mix, wide_mix = 3 * HEAD, 6 * HEAD

    barrier = pltpu.get_barrier_semaphore()
    for step in range(1, n_row):
        pl.semaphore_signal(barrier, inc=1, device_id={"row": lax.rem(row + step, n_row)}, device_id_type=MESH)
    for step in range(1, n_col):
        pl.semaphore_signal(barrier, inc=1, device_id={"col": lax.rem(col + step, n_col)}, device_id_type=MESH)
    for device in (outer, diagonal):
        pl.semaphore_signal(barrier, inc=1, device_id=device, device_id_type=MESH)

    sems = iter(range(1000))

    def remote(source, target, sem, device):
        return pltpu.make_async_remote_copy(
            src_ref=source, dst_ref=target, send_sem=ssem.at[sem], recv_sem=rsem.at[sem],
            device_id=device, device_id_type=MESH,
        )

    def ready():
        pl.semaphore_wait(barrier, n_row - 1 + n_col - 1 + 2)

    def column_stats(sums, squares):
        columns = jnp.concatenate(
            [jnp.broadcast_to(sums, (2 * patches, 128)), jnp.broadcast_to(squares, (2 * patches, 128))], axis=0
        )
        return columns.T[0:8]

    def lane_stats(total):
        mean = total * (1.0 / D)
        lane = lax.broadcasted_iota(jnp.int32, (8, 128), 1)
        shifted = pltpu.roll(mean, 2 * patches, axis=1)
        var = jnp.maximum(mean - shifted * shifted, 0.0)
        return jnp.where(lane < 2 * patches, mean, lax.rsqrt(var + EPS))

    def to_columns(table):
        rows = table[:, 0, :]
        return jnp.concatenate([rows] * (128 // n_col), axis=0).T

    def normalise(block, columns, c, gain):
        value = block.astype(F32).reshape(2 * patches, feats)
        mean, scale = columns[0:2 * patches, c:c + 1], columns[2 * patches:4 * patches, c:c + 1]
        return ((value - mean) * scale * gain).astype(BF16).reshape(2, patches, feats)

    def col_gather(view):
        arrive = []
        for step in (1, 3, 2):
            copy = remote(view(col), view(col), next(sems), same_core(step))
            copy.start()
            arrive.append((copy, step))
        first = remote(view(col), view(col), next(sems), sibling)
        first.start()

        def finish():
            handed = [first]
            for copy, step in arrive:
                copy.wait()
                block = view(2 * along_x(n_x - step) + core)
                onward = remote(block, block, next(sems), sibling)
                onward.start()
                handed.append(onward)
            for copy in handed:
                copy.wait()

        return finish

    def gelu(value):
        return (0.5 * value * (1.0 + lax.erf(value * math.sqrt(0.5)))).astype(BF16)

    def attend(query, keyed, valued):
        scores = lax.dot_general(query, keyed, (((1,), (1,)), ((), ())), preferred_element_type=F32)
        scores = scores * (1.0 / math.sqrt(HEAD))
        expo = jnp.exp(scores - jnp.max(scores, axis=-1, keepdims=True))
        probs = (expo / jnp.sum(expo, axis=-1, keepdims=True)).astype(BF16)
        return jnp.dot(probs, valued, preferred_element_type=F32).astype(BF16)

    def col_peers():
        for dx in (2, 1, 3, 0):
            for dc in range(2):
                if dx or dc:
                    target_core = lax.rem(core + dc, 2)
                    yield 2 * dx + dc - 1, along_x(dx), target_core, {"col": 2 * along_x(dx) + target_core}

    def col_direct(view):
        copies = []
        for _, _, _, device in col_peers():
            copy = remote(view(col), view(col), next(sems), device)
            copy.start()
            copies.append(copy)
        return copies

    def col_sum():
        copies = []
        for slot, target_x, target_core, device in col_peers():
            copy = remote(mix1_s.at[:, :, target_x, target_core], mix_r.at[slot], next(sems), device)
            copy.start()
            copies.append((copy, slot))
        value = mix1_s[:, :, chip_x, core].astype(F32)
        for copy, slot in copies:
            copy.wait()
            value = value + mix_r[slot].astype(F32)
        return value

    def col_sum_by_core():
        swaps = []
        for step in (2, 1, 3, 0):
            target = along_x(step)
            swap = remote(mix1_s.at[:, :, target, 1 - core], mix_d.at[:, :, target], next(sems), sibling)
            swap.start()
            swaps.append(swap)
        copies = []
        for step, swap in zip((2, 1, 3), swaps):
            target = along_x(step)
            swap.wait()
            mix_t[:, :, target] = (
                mix1_s[:, :, target, core].astype(F32) + mix_d[:, :, target].astype(F32)).astype(BF16)
            copy = remote(mix_t.at[:, :, target], mix_e.at[step - 1], next(sems), same_core(step))
            copy.start()
            copies.append((copy, step - 1))
        swaps[3].wait()
        value = mix1_s[:, :, chip_x, core].astype(F32) + mix_d[:, :, chip_x].astype(F32)
        for copy, slot in copies:
            copy.wait()
            value = value + mix_e[slot].astype(F32)
        return value

    group = feats
    block_sems = {name: [next(sems) for _ in range(n)] for name, n in
                  (("pair", 5), ("outer", 5), ("via", 5), ("forward", 5), ("gain", 3))}
    mlp_first = 2 * group
    mlp_rest = 3 * group

    def head_cols(member, j):
        return pl.ds(pl.multiple_of((member * 3 + j) * HEAD, HEAD), HEAD)

    def third(at, g):
        return w_in.at[at + g // 2, :, (g % 2) * group:(g % 2 + 1) * group]

    @pl.when(in_second)
    def ship():
        copies = []

        def fetch(source, target):
            copy = pltpu.make_async_copy(source, target, w_sem.at[len(copies)])
            copy.start()
            copies.append(copy)

        start = pl.multiple_of(mlp_first + yb * mlp_rest, group)
        fetch(wup_ref.at[:, pl.ds(start, 2 * group)], w_in.at[4])
        fetch(wup_ref.at[:, pl.ds(pl.multiple_of(start + 2 * group, group), group)], w_in.at[5, :, 0:group])
        fetch(wdn_ref.at[pl.ds(start, 2 * group)], w_mix.at[3])
        fetch(wdn_ref.at[pl.ds(pl.multiple_of(start + 2 * group, group), group)], w_mix.at[4, 0:group])
        n_via = len(copies)
        start = pl.multiple_of(mlp_first + other * mlp_rest, group)
        fetch(wup_ref.at[:, pl.ds(start, 2 * group)], w_in.at[2])
        fetch(wup_ref.at[:, pl.ds(pl.multiple_of(start + 2 * group, group), group)], w_in.at[3, :, 0:group])
        fetch(wdn_ref.at[pl.ds(start, 2 * group)], w_mix.at[1])
        fetch(wdn_ref.at[pl.ds(pl.multiple_of(start + 2 * group, group), group)], w_mix.at[2, 0:group])
        n_outer = len(copies)
        for member, mine in ((other, False), (yb, True)):
            for j in range(3):
                for k, w_ref in enumerate((wq_ref, wk_ref, wv_ref)):
                    span = slice(k * HEAD, (k + 1) * HEAD)
                    at = (j % 2) * group + k * HEAD
                    target = w1_in.at[j, yb, :, span] if mine else w_in.at[j // 2, :, at:at + HEAD]
                    fetch(w_ref.at[:, head_cols(member, j)], target)
            rows = pl.ds(pl.multiple_of(member * group, group), group)
            fetch(wup_ref.at[:, rows], w1_in.at[3, yb] if mine else w_in.at[1, :, group:2 * group])
            fetch(wout_ref.at[rows], w1_mix.at[yb, 0:group] if mine else w_mix.at[0, 0:group])
            fetch(wdn_ref.at[rows], w1_mix.at[yb, group:2 * group] if mine else w_mix.at[0, group:2 * group])
            if not mine:
                n_pair = len(copies)
        gain1[yb] = jnp.broadcast_to(gain_ref[...], (8, feats))
        ready()
        out = []

        def send(source, target, sem, device):
            copy = remote(source, target, sem, device)
            copy.start()
            out.append(copy)

        for copy in copies[:n_via]:
            copy.wait()
        for g in range(3):
            send(third(4, g), third(6, g), block_sems["via"][g], pair)
        send(w_mix.at[3], w_mix.at[5], block_sems["via"][3], pair)
        send(w_mix.at[4, 0:group], w_mix.at[6, 0:group], block_sems["via"][4], pair)
        for copy in copies[n_via:n_outer]:
            copy.wait()
        for g in range(3):
            send(third(2, g), w1_in.at[g, yb], block_sems["outer"][g], outer)
        send(w_mix.at[1], w1_mix.at[yb, 0:2 * group], block_sems["outer"][3], outer)
        send(w_mix.at[2, 0:group], w1_mix.at[yb, 2 * group:3 * group], block_sems["outer"][4], outer)
        for copy in copies[n_outer:n_pair]:
            copy.wait()
        for g in range(4):
            send(third(0, g), w1_in.at[g, yb], block_sems["pair"][g], pair)
        send(w_mix.at[0], w1_mix.at[yb, 0:2 * group], block_sems["pair"][4], pair)
        for device, sem in zip((pair, outer, diagonal), block_sems["gain"]):
            send(gain1.at[yb], gain1.at[yb], sem, device)
        for g in range(3):
            remote(third(6, g), third(6, g), block_sems["via"][g], pair).wait_recv()
            send(third(6, g), w1_in.at[g, other], block_sems["forward"][g], outer)
        remote(w_mix.at[5], w_mix.at[5], block_sems["via"][3], pair).wait_recv()
        send(w_mix.at[5], w1_mix.at[other, 0:2 * group], block_sems["forward"][3], outer)
        remote(w_mix.at[6, 0:group], w_mix.at[6, 0:group], block_sems["via"][4], pair).wait_recv()
        send(w_mix.at[6, 0:group], w1_mix.at[other, 2 * group:3 * group], block_sems["forward"][4], outer)
        for copy in copies[n_pair:]:
            copy.wait()
        for g in range(4):
            remote(w1_in.at[g, other], w1_in.at[g, other], block_sems["pair"][g], pair).wait_recv()
        remote(w1_mix.at[other, 0:2 * group], w1_mix.at[other, 0:2 * group], block_sems["pair"][4], pair).wait_recv()
        remote(gain1.at[other], gain1.at[other], block_sems["gain"][0], pair).wait_recv()
        for copy in out:
            copy.wait_send()

    def pieces_of_ring(copy, after=None):
        ring_sem = {}

        def onward(stage, piece, upward):
            block = around(-stage) if upward else around(stage)
            sem = next(sems)
            ring_sem[(stage, piece, upward)] = sem
            copy(block, piece, sem, up_z if upward else down_z, "start")
            sent.append(lambda: copy(block, piece, sem, up_z if upward else down_z, "wait_send"))

        def last(piece, upward):
            return (piece < 2) == upward

        for piece in (2, 3, 0, 1):
            onward(0, piece, True)
            onward(0, (piece + 2) % 4, False)
        if after is not None:
            after(-1)
        for stage in range(4):
            for piece in (2, 3, 0, 1):
                for upward in (True, False):
                    p = piece if upward else (piece + 2) % 4
                    if stage == 3 and not last(p, upward):
                        continue
                    block = around(-1 - stage) if upward else around(1 + stage)
                    copy(block, p, ring_sem[(stage, p, upward)], up_z if upward else down_z, "wait_recv")
                    if stage < 2 or (stage == 2 and last(p, upward)):
                        onward(stage + 1, p, upward)
            if after is not None:
                after(stage)

    sent = []
    main_n, main_w, part_g = 3 * HEAD, 4 * HEAD, 2 * HEAD
    image_rows = n_col * patches
    late = image_rows // 2
    early = image_rows - late
    y_rows = early // 2

    def member_hidden(member, g):
        if g == 3:
            start = 6 * part_g + member * 3 * part_g
            return start, start + main_w
        start = (member * 3 + g) * part_g
        return start, start

    def first_layer():
        waits = {"stage": [], "own": [], "mix": [], "mix_stage": []}
        count = iter(range(1000))

        def fetch(source, target, kind):
            copy = pltpu.make_async_copy(source, target, w_sem.at[next(count)])
            copy.start()
            waits[kind].append(copy)

        def columns_at(start, size):
            return pl.ds(pl.multiple_of(start, HEAD), size)

        for g in range(4):
            fetch(wup_ref.at[:, columns_at(member_hidden(other, g)[1], part_g)], w_gs.at[g], "stage")
        xf = x_ref[...].astype(F32).reshape(2 * patches, feats)
        sums = jnp.sum(xf, axis=-1, keepdims=True)
        squares = jnp.sum(xf * xf, axis=-1, keepdims=True)
        stat[row] = column_stats(sums, squares)
        xraw[yb] = x_ref[...]
        gathered[yb, :, col] = x_ref[...]
        gain0[yb] = jnp.broadcast_to(gain_ref[...], (8, feats))
        ready()
        x_copy = remote(xraw.at[yb], xraw.at[yb], x_spread[0], pair)
        x_copy.start()
        stat_copies = []
        for step in range(1, n_row):
            copy = remote(stat.at[row], stat.at[row], next(sems), {"row": lax.rem(row + step, n_row)})
            copy.start()
            stat_copies.append(copy)
        finish_own = col_gather(lambda c: gathered.at[yb, :, c])
        gain_copy = remote(gain0.at[yb], gain0.at[yb], next(sems), pair)
        gain_copy.start()
        for device, sem in ((outer, x_spread[1]), (diagonal, x_spread[2])):
            copy = remote(xraw.at[yb], xraw.at[yb], sem, device)
            copy.start()
            sent.append(copy.wait_send)

        def group_at(i):
            return lax.rem(z + (0, 3, 1, 2)[i], 4)

        def traced_group_at(i):
            return lax.rem(z + jnp.where(i == 0, 0, jnp.where(i == 1, 3, i - 1)), 4)

        g_base = next(sems)
        for _ in range(3):
            next(sems)
        for g in range(4):
            fetch(wup_ref.at[:, columns_at(member_hidden(yb, g)[1], part_g)], w_g.at[g, yb], "own")
        for block in range(NZ):
            member, g = block // 4, block % 4
            if g == 3:
                start = member_hidden(member, g)[0]
                fetch(wup_ref.at[:, start:start + main_w], w_main.at[block], "own")
            else:
                cols = slice((member * 3 + g) * HEAD, (member * 3 + g + 1) * HEAD)
                for k, w_ref in enumerate((wq_ref, wk_ref, wv_ref)):
                    fetch(w_ref.at[:, cols], w_main.at[block, :, k * HEAD:(k + 1) * HEAD], "own")
        for member, kind in ((other, "mix_stage"), (yb, "mix")):
            for g in range(4):
                target = w_ms.at[g] if kind == "mix_stage" else w_mix.at[yb * 4 + g]
                rows = columns_at(member_hidden(member, g)[0], wide_mix if g == 3 else part_g)
                if g == 3:
                    fetch(wdn_ref.at[rows], target, kind)
                else:
                    fetch(wout_ref.at[columns_at((member * 3 + g) * HEAD, HEAD)], target.at[0:HEAD], kind)
                    fetch(wdn_ref.at[rows], target.at[HEAD:narrow_mix], kind)
        for copy in waits["stage"]:
            copy.wait()
        for i in range(4):
            g = group_at(i)
            copy = remote(w_gs.at[g], w_g.at[g, yb], g_base + i, pair)
            copy.start()
            sent.append(copy.wait_send)
        x_copy.wait()
        gathered[other, :, col] = xraw[other]
        finish_other = col_gather(lambda c: gathered.at[other, :, c])
        finish_own()
        for copy in stat_copies:
            copy.wait()
        stat_col[0, col] = lane_stats(jnp.sum(stat[...], axis=0))
        finish_stats = col_direct(lambda c: stat_col.at[0, c])
        for copy in waits["own"]:
            copy.wait()
        finish_other()
        for copy in finish_stats:
            copy.wait()
        gain_copy.wait()
        columns = to_columns(stat_col[0])
        for c in range(n_col):
            for k in range(2):
                gathered[k, :, c] = normalise(gathered[k, :, c], columns, c, gain0[k, 0:1])

        bufs = {
            "G": (gs_p, gs_m, gr_p, gr_m), "Z": (zs_p, zs_m, zr_p, zr_m), "Y": (ys_p, ys_m, yr_p, yr_m),
        }
        tables = {True: {}, False: {}}
        pair_base = next(sems)
        for _ in range(NZ - 1):
            next(sems)

        def by_part(kind, block, action):
            if kind == "G":
                action(part_g)
            else:
                by_width(block, main_n, main_w, action)

        def move(kind, source, target, sem, device, block, what):
            by_part(kind, block, lambda w: getattr(remote(source.at[:, 0:w], target.at[:, 0:w], sem, device), what)())

        def ring_block(stage, upward):
            return around(4 - stage) if upward else around(stage - 4)

        def term(kind, h, block):
            g, image = lax.rem(block, 4), lax.div(block, 4)
            if kind == "G":
                return own_g[g, image, h]
            if kind == "Z":
                return own[h * 4 + g, image, early:image_rows]
            return own[yb * 4 + g, image, h * y_rows:(h + 1) * y_rows]

        def reserve(kind, stage, h, upward):
            sem = next(sems)
            tables[upward][(kind, stage, h)] = sem
            send_buf = bufs[kind][0 if upward else 1].at[stage, h]
            device = up_z if upward else down_z
            block = ring_block(stage, upward)
            sent.append(lambda: move(kind, send_buf, send_buf, sem, device, block, "wait_send"))

        def hop(kind, stage, h, upward):
            send_buf = bufs[kind][0 if upward else 1]
            recv_buf = bufs[kind][2 if upward else 3]
            device = up_z if upward else down_z
            block = ring_block(stage, upward)
            value = term(kind, h, block)
            if stage >= 2 or (stage == 1 and h == (0 if upward else 1)):
                buf = recv_buf.at[stage - 1, h]
                move(kind, buf, buf, tables[upward][(kind, stage - 1, h)], device, block, "wait_recv")
                value = value + recv_buf[stage - 1, h].astype(F32)
            send_buf[stage, h] = value.astype(BF16)
            if (kind, stage, h) not in tables[upward]:
                reserve(kind, stage, h, upward)
            move(kind, send_buf.at[stage, h], recv_buf.at[stage, h], tables[upward][(kind, stage, h)], device, block, "start")

        for kind in ("G", "Z"):
            reserve(kind, 0, 0, True)
            reserve(kind, 0, 1, False)
            reserve(kind, 1, 1, True)
            reserve(kind, 1, 0, False)

        def order(i):
            away = 4 - lax.div(i + 1, 2)
            return around(jnp.where(lax.rem(i, 2) == 1, away, -away))

        def send_pair(i):
            block = order(i)
            pair_s[i] = own[other * 4 + lax.rem(block, 4), lax.div(block, 4), 0:early].astype(BF16)
            move("Y", pair_s.at[i], pair_r.at[i], pair_base + i, pair, block, "start")

        n_tok = 2 * image_rows

        def product(i, carry):
            g = traced_group_at(i)
            for member in range(2):
                own[member * 4 + g] = jnp.dot(
                    gathered[yb].reshape(n_tok, feats), w_main[member * 4 + g], preferred_element_type=F32
                ).reshape(2, image_rows, main_w)

            @pl.when(i == 0)
            def _():
                hop("Z", 0, 0, True)
                hop("Z", 0, 1, False)

            @pl.when(i == 1)
            def _():
                hop("Z", 1, 1, True)

            @pl.when(i == 2)
            def _():
                hop("Z", 1, 0, False)

            send_pair(i)
            return carry

        def product_g(i, carry):
            g = traced_group_at(i)
            remote(w_g.at[g, other], w_g.at[g, other], g_base + i, pair).wait_recv()
            own_g[g] = (
                jnp.dot(gathered[0].reshape(n_tok, feats), w_g[g, 0], preferred_element_type=F32)
                + jnp.dot(gathered[1].reshape(n_tok, feats), w_g[g, 1], preferred_element_type=F32)
            ).reshape(2, 2, image_rows // 2, part_g)

            @pl.when(i == 0)
            def _():
                hop("G", 0, 0, True)
                hop("G", 0, 1, False)

            @pl.when(i == 1)
            def _():
                hop("G", 1, 1, True)

            @pl.when(i == 2)
            def _():
                hop("G", 1, 0, False)

            return carry

        lax.fori_loop(0, 4, product, 0)

        def rest_of_pair(i, carry):
            send_pair(i)
            return carry

        lax.fori_loop(4, NZ, rest_of_pair, 0)
        for copy in waits["mix_stage"]:
            copy.wait()
        mix_sems = [next(sems) for _ in range(4)]

        def send_mix(g):
            n = wide_mix if g == 3 else narrow_mix
            copy = remote(w_ms.at[g, 0:n], w_mix.at[yb * 4 + g, 0:n], mix_sems[g], pair)
            copy.start()
            sent.append(copy.wait_send)

        for i in range(NZ):
            sent.append(lambda i=i: move(
                "Y", pair_s.at[i], pair_s.at[i], pair_base + i, pair, order(jnp.int32(i)), "wait_send"))

        def pair_sum(i):
            block = order(jnp.int32(i))
            move("Y", pair_r.at[i], pair_r.at[i], pair_base + i, pair, block, "wait_recv")
            at = own.at[yb * 4 + lax.rem(block, 4), lax.div(block, 4), 0:early]
            at[...] = at[...] + pair_r[i].astype(F32)

        def four(kind, stage, before=(None, None)):
            for sums, h, upward in ((before[0], 1, True), (before[1], 0, False), (None, 0, True), (None, 1, False)):
                if sums is not None:
                    pair_sum(sums)
                hop(kind, stage, h, upward)

        def all_in(kind):
            for h, upward in ((1, True), (0, False), (0, True), (1, False)):
                buf = bufs[kind][2 if upward else 3].at[3, h]
                move(kind, buf, buf, tables[upward][(kind, 3, h)], up_z if upward else down_z, z, "wait_recv")

        hop("Z", 1, 0, True)
        hop("Z", 1, 1, False)
        lax.fori_loop(0, 1, product_g, 0)
        four("Z", 2)
        lax.fori_loop(1, 3, product_g, 0)
        four("Z", 3)
        lax.fori_loop(3, 4, product_g, 0)
        hop("G", 1, 0, True)
        hop("G", 1, 1, False)
        pair_sum(0)
        hop("Y", 0, 0, True)
        hop("Y", 0, 1, False)
        four("G", 2)
        all_in("Z")
        last_s[...] = (term("Z", other, z) + zr_p[3, other].astype(F32) + zr_m[3, other].astype(F32)).astype(BF16)
        last_sem = next(sems)
        move("Z", last_s, last_r, last_sem, pair, z, "start")
        sent.append(lambda: move("Z", last_s, last_s, last_sem, pair, z, "wait_send"))
        for g in (3, 0, 1, 2):
            send_mix(g)
        four("Y", 1, (1, 2))
        four("G", 3)
        four("Y", 2, (3, 4))
        four("Y", 3, (5, 6))
        is_wide = wide(z)
        all_in("G")
        for h in range(2):
            hidden = gelu(term("G", h, z) + gr_p[3, h].astype(F32) + gr_m[3, h].astype(F32))

            @pl.when(is_wide)
            def _():
                acts[z, h, :, main_w:wide_mix] = hidden

            @pl.when(jnp.logical_not(is_wide))
            def _():
                acts[z, h, :, HEAD:narrow_mix] = hidden

        full[early:image_rows] = term("Z", yb, z) + zr_p[3, yb].astype(F32) + zr_m[3, yb].astype(F32)
        move("Z", last_r, last_r, last_sem, pair, z, "wait_recv")
        full[early:image_rows] = full[early:image_rows] + last_r[...].astype(F32)
        pair_sum(7)
        all_in("Y")
        for h in range(2):
            full[h * y_rows:(h + 1) * y_rows] = term("Y", h, z) + yr_p[3, h].astype(F32) + yr_m[3, h].astype(F32)

        @pl.when(is_wide)
        def _():
            acts[z, :, :, 0:main_w] = gelu(full[...]).reshape(2, image_rows // 2, main_w)

        @pl.when(jnp.logical_not(is_wide))
        def _():
            value = full[:, 0:main_n].astype(BF16)
            result = attend(value[:, 0:HEAD], value[:, HEAD:2 * HEAD], value[:, 2 * HEAD:3 * HEAD])
            acts[z, :, :, 0:HEAD] = result.reshape(2, image_rows // 2, HEAD)

        piece_rows = image_rows // 4

        def act_copy(block, piece, sem, device, what):
            rows = slice((piece % 2) * piece_rows, (piece % 2 + 1) * piece_rows)

            def action(w):
                part = acts.at[block, piece // 2, rows, 0:w]
                getattr(remote(part, part, sem, device), what)()

            by_width(block, narrow_mix, wide_mix, action)

        def add_product(k, block):
            g, image = lax.rem(block, 4), lax.div(block, 4)

            def add(w):
                acc[k, image] = acc[k, image] + jnp.dot(
                    acts[block, :, :, 0:w].reshape(image_rows, w), w_mix[k * 4 + g, 0:w], preferred_element_type=F32)

            by_width(block, narrow_mix, wide_mix, add)

        def add_known(k, block):
            g, image = block % 4, block // 4
            w = wide_mix if g == 3 else narrow_mix
            acc[k, image] = acc[k, image] + jnp.dot(
                acts[block, :, :, 0:w].reshape(image_rows, w), w_mix[k * 4 + g, 0:w], preferred_element_type=F32)

        acc[...] = jnp.zeros_like(acc)

        def after_stage(stage):
            if stage == -1:
                for copy in waits["mix"]:
                    copy.wait()
                add_product(yb, z)
            elif stage < 3:
                add_product(yb, around(-1 - stage))
                add_product(yb, around(1 + stage))
                if stage == 2:
                    for g in (3, 0, 1, 2):
                        n = wide_mix if g == 3 else narrow_mix
                        part = w_mix.at[other * 4 + g, 0:n]
                        remote(part, part, mix_sems[g], pair).wait_recv()
                        for block in (g, g + 4):
                            pl.when(around(4) != block)(lambda block=block: add_known(other, block))
            else:
                add_product(yb, around(4))
                add_product(other, around(4))

        pieces_of_ring(act_copy, after_stage)

        for k in range(2):
            mix1_s[k] = acc[k].astype(BF16).reshape(2, n_x, 2, patches, feats)
        total = col_sum_by_core()
        terms[yb] = total.astype(BF16)
        for device, sem in ((pair, spread[0]), (outer, spread[1]), (diagonal, spread[2])):
            copy = remote(terms.at[yb], terms.at[yb], sem, device)
            copy.start()
        for wait in sent:
            wait()
        sent.clear()
        for g in range(3):
            remote(w1_in.at[g, other], w1_in.at[g, other], block_sems["outer"][g], outer).wait_recv()
            remote(w1_in.at[g, yb], w1_in.at[g, yb], block_sems["forward"][g], outer).wait_recv()
        for half_k, name in ((other, "outer"), (yb, "forward")):
            for k, (lo, hi) in ((3, (0, 2 * group)), (4, (2 * group, 3 * group))):
                part = w1_mix.at[half_k, lo:hi]
                remote(part, part, block_sems[name][k], outer).wait_recv()
        remote(gain1.at[other], gain1.at[other], block_sems["gain"][1], outer).wait_recv()
        remote(gain1.at[yb], gain1.at[yb], block_sems["gain"][2], diagonal).wait_recv()
        remote(terms.at[other], terms.at[other], spread[0], pair).wait_recv()

    x_spread = [next(sems) for _ in range(3)]
    spread = [next(sems) for _ in range(3)]
    pl.when(in_first)(first_layer)

    @pl.when(in_second)
    def _():
        remote(terms.at[other], terms.at[other], spread[1], outer).wait_recv()
        remote(terms.at[yb], terms.at[yb], spread[2], diagonal).wait_recv()
        remote(xraw.at[other], xraw.at[other], x_spread[1], outer).wait_recv()
        remote(xraw.at[yb], xraw.at[yb], x_spread[2], diagonal).wait_recv()
    for k in range(2):
        xb1[k] = (xraw[k].astype(F32) + terms[0, k].astype(F32) + terms[1, k].astype(F32)).astype(BF16)

    @pl.when(in_first)
    def _():
        y_ref[...] = xb1[yb]

    n_tok = 2 * n_col * patches
    both = xb1[...].astype(F32).reshape(2, 2 * patches, feats)
    sums = jnp.sum(jnp.sum(both, axis=-1, keepdims=True), axis=0)
    squares = jnp.sum(jnp.sum(both * both, axis=-1, keepdims=True), axis=0)
    stat1[z] = column_stats(sums, squares)
    copies = []
    for step in range(1, NZ):
        copy = remote(stat1.at[z], stat1.at[z], next(sems), {"row": yb * NZ + around(step)})
        copy.start()
        copies.append(copy)
    finish_k = []
    for k in range(2):
        gathered1[k, :, col] = xb1[k]
        finish_k.append(col_gather(lambda c, k=k: gathered1.at[k, :, c]))
    for copy in copies:
        copy.wait()
    stat_col[1, col] = lane_stats(jnp.sum(stat1[...], axis=0))
    finish_stats1 = col_direct(lambda c: stat_col.at[1, c])
    for finish in finish_k:
        finish()
    for copy in finish_stats1:
        copy.wait()
    columns1 = to_columns(stat_col[1])
    for c in range(n_col):
        for k in range(2):
            gathered1[k, :, c] = normalise(gathered1[k, :, c], columns1, c, gain1[k, 0:1])

    piece_long = 2 * patches
    piece_short = 3 * patches // 2
    third_rows = patches // 2

    def partial_product(g):
        return (
            jnp.dot(gathered1[0].reshape(n_tok, feats), w1_in[g, 0], preferred_element_type=F32)
            + jnp.dot(gathered1[1].reshape(n_tok, feats), w1_in[g, 1], preferred_element_type=F32)
        )

    @pl.when(in_first)
    def _():
        for g in range(3):
            value = partial_product(g).reshape(NZ, 4, third_rows, group)
            own1[:, :, g * third_rows:(g + 1) * third_rows] = value

    @pl.when(in_second)
    def _():
        for g in range(4):
            value = partial_product(g).reshape(2, 4, piece_long, group)
            own1[g] = value[0]
            own1[4 + g] = value[1]

    def by_section(action):
        either(in_first, lambda: action(piece_short), lambda: action(piece_long))

    up1, down1 = {}, {}

    def far(h, upward):
        return (h < 2) == upward

    def hop1(stage, h, upward):
        send_buf, recv_buf = (zs1_p, zr1_p) if upward else (zs1_m, zr1_m)
        table = up1 if upward else down1
        device = up_z if upward else down_z
        block = around(4 - stage) if upward else around(stage - 4)
        value = own1[block, h]
        if stage >= 2 or (stage == 1 and far(h, upward)):
            sem = table[(stage - 1, h)]
            by_section(lambda n: remote(
                recv_buf.at[stage - 1, h, 0:n], recv_buf.at[stage - 1, h, 0:n], sem, device).wait_recv())
            value = value + recv_buf[stage - 1, h].astype(F32)
        send_buf[stage, h] = value.astype(BF16)
        sem_out = next(sems)
        table[(stage, h)] = sem_out
        by_section(lambda n: remote(
            send_buf.at[stage, h, 0:n], recv_buf.at[stage, h, 0:n], sem_out, device).start())
        sent.append(lambda: by_section(lambda n: remote(
            send_buf.at[stage, h, 0:n], recv_buf.at[stage, h, 0:n], sem_out, device).wait_send()))

    for h in (0, 1):
        hop1(0, h, True)
        hop1(0, h + 2, False)
    for stage in (1, 2, 3):
        for h in (2, 3, 0, 1):
            hop1(stage, h, True)
            hop1(stage, (h + 2) % 4, False)
    for h in range(4):
        by_section(lambda n: remote(zr1_p.at[3, h, 0:n], zr1_p.at[3, h, 0:n], up1[(3, h)], up_z).wait_recv())
        by_section(lambda n: remote(zr1_m.at[3, h, 0:n], zr1_m.at[3, h, 0:n], down1[(3, h)], down_z).wait_recv())

    def summed(h):
        return own1[z, h] + zr1_p[3, h].astype(F32) + zr1_m[3, h].astype(F32)

    has_head = jnp.logical_and(in_second, jnp.logical_not(wide(z)))

    @pl.when(has_head)
    def _():
        value = jnp.concatenate([summed(h) for h in range(4)], axis=0).astype(BF16)
        result = attend(value[:, 0:HEAD], value[:, HEAD:2 * HEAD], value[:, 2 * HEAD:3 * HEAD])
        acts1[z, :, :, 0:HEAD] = result.reshape(4, piece_long, HEAD)

    @pl.when(jnp.logical_not(has_head))
    def _():
        for h in range(4):
            acts1[z, h] = gelu(summed(h))

    def by_kind(block, action):
        either(
            in_first,
            lambda: action(piece_short, group),
            lambda: by_width(block, HEAD, group, lambda w: action(piece_long, w)),
        )

    def act_copy1(block, piece, sem, device, what):
        def action(n, w):
            part = acts1.at[block, piece, 0:n, 0:w]
            getattr(remote(part, part, sem, device), what)()

        by_kind(block, action)

    pieces_of_ring(act_copy1)
    @pl.when(in_first)
    def _():
        for k in range(2):
            total = None
            for g in range(3):
                hidden = acts1[:, :, g * third_rows:(g + 1) * third_rows].reshape(n_tok, group)
                term = jnp.dot(hidden, w1_mix[k, g * group:(g + 1) * group], preferred_element_type=F32)
                total = term if total is None else total + term
            acc1[k] = total

    @pl.when(in_second)
    def _():
        for image in range(2):
            first = image * 4
            value = jnp.concatenate(
                [acts1[first + j, :, :, 0:HEAD].reshape(image_rows, HEAD) for j in range(3)]
                + [acts1[first + 3].reshape(image_rows, group)], axis=1)
            for k in range(2):
                acc1[k, image * image_rows:(image + 1) * image_rows] = jnp.dot(
                    value, w1_mix[k, 0:2 * group], preferred_element_type=F32)

    for k in range(2):
        mix1_s[k] = acc1[k].astype(BF16).reshape(2, n_x, 2, patches, feats)
    total = col_sum()
    ys1[...] = total.astype(BF16)
    to_pair, to_outer, to_diagonal = next(sems), next(sems), next(sems)

    @pl.when(in_first)
    def _():
        copies = [remote(ys1.at[other], yr1.at[1], to_outer, outer), remote(ys1.at[yb], yr1.at[2], to_diagonal, diagonal)]
        for copy in copies:
            copy.start()
        for copy in copies:
            copy.wait_send()

    @pl.when(in_second)
    def _():
        copy = remote(ys1.at[other], yr1.at[0], to_pair, pair)
        copy.start()
        copy.wait()
        remote(yr1.at[1], yr1.at[1], to_outer, outer).wait_recv()
        remote(yr1.at[2], yr1.at[2], to_diagonal, diagonal).wait_recv()
        result = xb1[yb].astype(F32) + ys1[yb].astype(F32)
        for k in range(3):
            result = result + yr1[k].astype(F32)
        y_ref[...] = result.astype(BF16)

    assert next(sems) < 304
    for wait in sent:
        wait()

    @pl.when(in_first)
    def _():
        for device, sem in ((pair, spread[0]), (outer, spread[1]), (diagonal, spread[2])):
            remote(terms.at[yb], terms.at[yb], sem, device).wait_send()


def layers(x, weights):
    gain, wq, wk, wv, wup, wout, wdown = weights
    n_col = lax.axis_size("col")
    images, patches, feats = x.shape
    wide_in = 6 * HEAD
    vmem = pl.BlockSpec(memory_space=pltpu.VMEM)
    anywhere = pl.BlockSpec(memory_space=pl.ANY)
    rows = n_col * patches
    late = rows // 2
    early = rows - late
    g_buf = pltpu.VMEM((4, 2, rows // 2, 2 * HEAD), BF16)
    z_buf = pltpu.VMEM((4, 2, late, 4 * HEAD), BF16)
    y_buf = pltpu.VMEM((4, 2, early // 2, 4 * HEAD), BF16)
    pair_buf = pltpu.VMEM((NZ, early, 4 * HEAD), BF16)
    z1_buf = pltpu.VMEM((4, 4, 2 * patches, feats), BF16)
    scratch = [
        pltpu.VMEM((NZ, feats, wide_in), BF16),
        pltpu.VMEM((NZ, wide_in, feats), BF16),
        pltpu.VMEM((NZ, feats, 4 * HEAD), BF16),
        pltpu.VMEM((4, 2, feats, 2 * HEAD), BF16),
        pltpu.VMEM((4, feats, 2 * HEAD), BF16),
        pltpu.VMEM((4, wide_in, feats), BF16),
        pltpu.VMEM((2, 2, n_col, patches, feats), BF16),
        pltpu.VMEM((2, 8, feats), F32),
        pltpu.VMEM((NZ, 2, rows, 4 * HEAD), F32),
        pltpu.VMEM((4, 2, 2, rows // 2, 2 * HEAD), F32),
        pltpu.VMEM((2 * NZ, 8, 128), F32),
        g_buf, g_buf, g_buf, g_buf, z_buf, z_buf, z_buf, z_buf, y_buf, y_buf, y_buf, y_buf, pair_buf, pair_buf,
        pltpu.VMEM((late, 4 * HEAD), BF16), pltpu.VMEM((late, 4 * HEAD), BF16),
        pltpu.VMEM((rows, 4 * HEAD), F32),
        pltpu.VMEM((NZ, 2, rows // 2, wide_in), BF16),
        pltpu.VMEM((2, 2, rows, feats), F32),
        pltpu.VMEM((2, n_col, 8, 128), F32),
        pltpu.VMEM((2, 2, patches, feats), BF16),
        pltpu.VMEM((2, 2, 2, patches, feats), BF16),
        pltpu.VMEM((2, 2, n_col // 2, patches, feats), BF16),
        pltpu.VMEM((2, 2, n_col // 2, patches, feats), BF16),
        pltpu.VMEM((n_col // 2 - 1, 2, 2, patches, feats), BF16),
        pltpu.VMEM((4, 2, feats, feats), BF16),
        pltpu.VMEM((2, 3 * feats, feats), BF16),
        pltpu.VMEM((2, 8, feats), F32),
        pltpu.VMEM((2, 2, patches, feats), BF16),
        pltpu.VMEM((2, 2, n_col, patches, feats), BF16),
        pltpu.VMEM((NZ, 4, 2 * patches, feats), F32),
        pltpu.VMEM((NZ, 8, 128), F32),
        z1_buf, z1_buf, z1_buf, z1_buf,
        pltpu.VMEM((NZ, 4, 2 * patches, feats), BF16),
        pltpu.VMEM((2, 2 * n_col * patches, feats), F32),
        pltpu.VMEM((2, 2, n_col // 2, 2, patches, feats), BF16),
        pltpu.VMEM((n_col - 1, 2, 2, patches, feats), BF16),
        pltpu.VMEM((2, 2, patches, feats), BF16),
        pltpu.VMEM((3, 2, patches, feats), BF16),
        pltpu.SemaphoreType.DMA((64,)),
        pltpu.SemaphoreType.DMA((304,)),
        pltpu.SemaphoreType.DMA((304,)),
    ]
    return pl.pallas_call(
        functools.partial(layers_kernel, n_col, patches, feats),
        out_shape=jax.ShapeDtypeStruct(x.shape, BF16),
        in_specs=[vmem, vmem] + [anywhere] * 6,
        out_specs=vmem,
        scratch_shapes=scratch,
        compiler_params=pltpu.CompilerParams(
            collective_id=0, has_side_effects=True, vmem_limit_bytes=67043328
        ),
    )(x, gain[None], wq, wk, wv, wup, wout, wdown)


def local(tokens, ln_gain, w_query, w_key, w_value, w_up, w_out, w_down):
    weights = (ln_gain[0], w_query[0], w_key[0], w_value[0], w_up[0], w_out[0], w_down[0])
    return layers(tokens, weights)[None]


def solution(mesh):
    return jax.shard_map(
        local,
        mesh=mesh,
        in_specs=(
            P(None, "col", "row"),
            P("section", "row"),
            P("section", "row", "col"),
            P("section", "row", "col"),
            P("section", "row", "col"),
            P("section", "row", "col"),
            P("section", "col", "row"),
            P("section", "col", "row"),
        ),
        out_specs=P("section", None, "col", "row"),
        check_vma=False,
    )
```

```python
import functools
import math

import jax
import jax.numpy as jnp
from jax import lax
from jax.experimental import pallas as pl
from jax.experimental.pallas import tpu as pltpu
from jax.sharding import PartitionSpec as P

D = 6144
HEAD = 128
EPS = 1e-06
NZ = 8
MESH = pl.DeviceIdType.MESH
BF16 = jnp.bfloat16
F32 = jnp.float32


def wide(block):
    return lax.rem(block, 4) == 3


def either(condition, yes, no):
    def run(action):
        def branch():
            action()

        return branch

    lax.cond(condition, run(yes), run(no))


def by_width(block, narrow_size, wide_size, action):
    either(wide(block), lambda: action(wide_size), lambda: action(narrow_size))


def layers_kernel(
    n_col, patches, feats,
    x_ref, gain_ref, wq_ref, wk_ref, wv_ref, wup_ref, wout_ref, wdn_ref,
    y_ref,
    w_in, w_mix, w_main, w_g, w_gs, w_ms, gathered, gain0, own, own_g, stat,
    gs_p, gs_m, gr_p, gr_m, zs_p, zs_m, zr_p, zr_m, ys_p, ys_m, yr_p, yr_m, pair_s, pair_r, last_s, last_r,
    full, acts, acc,
    stat_col, xraw, terms, mix_d, mix_t, mix_e,
    w1_in, w1_mix, gain1, xb1, gathered1, own1, stat1, zs1_p, zs1_m, zr1_p, zr1_m,
    acts1, acc1, mix1_s, mix_r, ys1, yr1,
    w_sem, ssem, rsem,
):
    section = lax.axis_index("section")
    row = lax.axis_index("row")
    col = lax.axis_index("col")
    n_row = 2 * NZ
    yb = lax.div(row, NZ)
    z = lax.rem(row, NZ)
    other = 1 - yb

    def around(step):
        return lax.rem(z + step + NZ, NZ)

    up_z = {"row": yb * NZ + around(1)}
    down_z = {"row": yb * NZ + around(-1)}
    pair = {"row": other * NZ + z}
    outer = {"section": 1 - section, "row": other * NZ + z}
    diagonal = {"section": 1 - section, "row": row}
    n_x = n_col // 2
    core = lax.rem(col, 2)
    chip_x = lax.div(col, 2)
    sibling = {"col": 2 * chip_x + 1 - core}

    def along_x(step):
        return lax.rem(chip_x + step, n_x)

    def same_core(step):
        return {"col": 2 * along_x(step) + core}
    in_first = section == 0
    in_second = section == 1

    narrow_mix, wide_mix = 3 * HEAD, 6 * HEAD

    barrier = pltpu.get_barrier_semaphore()
    for step in range(1, n_row):
        pl.semaphore_signal(barrier, inc=1, device_id={"row": lax.rem(row + step, n_row)}, device_id_type=MESH)
    for step in range(1, n_col):
        pl.semaphore_signal(barrier, inc=1, device_id={"col": lax.rem(col + step, n_col)}, device_id_type=MESH)
    for device in (outer, diagonal):
        pl.semaphore_signal(barrier, inc=1, device_id=device, device_id_type=MESH)

    sems = iter(range(1000))

    def remote(source, target, sem, device):
        return pltpu.make_async_remote_copy(
            src_ref=source, dst_ref=target, send_sem=ssem.at[sem], recv_sem=rsem.at[sem],
            device_id=device, device_id_type=MESH,
        )

    def ready():
        pl.semaphore_wait(barrier, n_row - 1 + n_col - 1 + 2)

    def column_stats(sums, squares):
        columns = jnp.concatenate(
            [jnp.broadcast_to(sums, (2 * patches, 128)), jnp.broadcast_to(squares, (2 * patches, 128))], axis=0
        )
        return columns.T[0:8]

    def lane_stats(total):
        mean = total * (1.0 / D)
        lane = lax.broadcasted_iota(jnp.int32, (8, 128), 1)
        shifted = pltpu.roll(mean, 2 * patches, axis=1)
        var = jnp.maximum(mean - shifted * shifted, 0.0)
        return jnp.where(lane < 2 * patches, mean, lax.rsqrt(var + EPS))

    def to_columns(table):
        rows = table[:, 0, :]
        return jnp.concatenate([rows] * (128 // n_col), axis=0).T

    def normalise(block, columns, c, gain):
        value = block.astype(F32).reshape(2 * patches, feats)
        mean, scale = columns[0:2 * patches, c:c + 1], columns[2 * patches:4 * patches, c:c + 1]
        return ((value - mean) * scale * gain).astype(BF16).reshape(2, patches, feats)

    def col_gather(view):
        arrive = []
        for step in (1, 3, 2):
            copy = remote(view(col), view(col), next(sems), same_core(step))
            copy.start()
            arrive.append((copy, step))
        first = remote(view(col), view(col), next(sems), sibling)
        first.start()

        def finish():
            handed = [first]
            for copy, step in arrive:
                copy.wait()
                block = view(2 * along_x(n_x - step) + core)
                onward = remote(block, block, next(sems), sibling)
                onward.start()
                handed.append(onward)
            for copy in handed:
                copy.wait()

        return finish

    def gelu(value):
        return (0.5 * value * (1.0 + lax.erf(value * math.sqrt(0.5)))).astype(BF16)

    def attend(query, keyed, valued):
        scores = lax.dot_general(query, keyed, (((1,), (1,)), ((), ())), preferred_element_type=F32)
        scores = scores * (1.0 / math.sqrt(HEAD))
        expo = jnp.exp(scores - jnp.max(scores, axis=-1, keepdims=True))
        probs = (expo / jnp.sum(expo, axis=-1, keepdims=True)).astype(BF16)
        return jnp.dot(probs, valued, preferred_element_type=F32).astype(BF16)

    def col_peers():
        for dx in (2, 1, 3, 0):
            for dc in range(2):
                if dx or dc:
                    target_core = lax.rem(core + dc, 2)
                    yield 2 * dx + dc - 1, along_x(dx), target_core, {"col": 2 * along_x(dx) + target_core}

    def col_direct(view):
        copies = []
        for _, _, _, device in col_peers():
            copy = remote(view(col), view(col), next(sems), device)
            copy.start()
            copies.append(copy)
        return copies

    def col_sum_by_core():
        swaps = []
        for step in (2, 1, 3, 0):
            target = along_x(step)
            swap = remote(mix1_s.at[:, :, target, 1 - core], mix_d.at[:, :, target], next(sems), sibling)
            swap.start()
            swaps.append(swap)
        copies = []
        for step, swap in zip((2, 1, 3), swaps):
            target = along_x(step)
            swap.wait()
            mix_t[:, :, target] = (
                mix1_s[:, :, target, core].astype(F32) + mix_d[:, :, target].astype(F32)).astype(BF16)
            copy = remote(mix_t.at[:, :, target], mix_e.at[step - 1], next(sems), same_core(step))
            copy.start()
            copies.append((copy, step - 1))
        swaps[3].wait()
        value = mix1_s[:, :, chip_x, core].astype(F32) + mix_d[:, :, chip_x].astype(F32)
        for copy, slot in copies:
            copy.wait()
            value = value + mix_e[slot].astype(F32)
        return value

    group = feats
    block_sems = {name: [next(sems) for _ in range(n)] for name, n in
                  (("pair", 5), ("outer", 5), ("via", 5), ("forward", 5), ("gain", 3))}
    mlp_first = 2 * group
    mlp_rest = 3 * group

    def head_cols(member, j):
        return pl.ds(pl.multiple_of((member * 3 + j) * HEAD, HEAD), HEAD)

    def third(at, g):
        return w_in.at[at + g // 2, :, (g % 2) * group:(g % 2 + 1) * group]

    @pl.when(in_second)
    def ship():
        copies = []

        def fetch(source, target):
            copy = pltpu.make_async_copy(source, target, w_sem.at[len(copies)])
            copy.start()
            copies.append(copy)

        start = pl.multiple_of(mlp_first + yb * mlp_rest, group)
        fetch(wup_ref.at[:, pl.ds(start, 2 * group)], w_in.at[4])
        fetch(wup_ref.at[:, pl.ds(pl.multiple_of(start + 2 * group, group), group)], w_in.at[5, :, 0:group])
        fetch(wdn_ref.at[pl.ds(start, 2 * group)], w_mix.at[3])
        fetch(wdn_ref.at[pl.ds(pl.multiple_of(start + 2 * group, group), group)], w_mix.at[4, 0:group])
        n_via = len(copies)
        start = pl.multiple_of(mlp_first + other * mlp_rest, group)
        fetch(wup_ref.at[:, pl.ds(start, 2 * group)], w_in.at[2])
        fetch(wup_ref.at[:, pl.ds(pl.multiple_of(start + 2 * group, group), group)], w_in.at[3, :, 0:group])
        fetch(wdn_ref.at[pl.ds(start, 2 * group)], w_mix.at[1])
        fetch(wdn_ref.at[pl.ds(pl.multiple_of(start + 2 * group, group), group)], w_mix.at[2, 0:group])
        n_outer = len(copies)
        for member, mine in ((other, False), (yb, True)):
            for j in range(3):
                for k, w_ref in enumerate((wq_ref, wk_ref, wv_ref)):
                    span = slice(k * HEAD, (k + 1) * HEAD)
                    at = (j % 2) * group + k * HEAD
                    target = w1_in.at[j, yb, :, span] if mine else w_in.at[j // 2, :, at:at + HEAD]
                    fetch(w_ref.at[:, head_cols(member, j)], target)
            rows = pl.ds(pl.multiple_of(member * group, group), group)
            fetch(wup_ref.at[:, rows], w1_in.at[3, yb] if mine else w_in.at[1, :, group:2 * group])
            fetch(wout_ref.at[rows], w1_mix.at[yb, 0:group] if mine else w_mix.at[0, 0:group])
            fetch(wdn_ref.at[rows], w1_mix.at[yb, group:2 * group] if mine else w_mix.at[0, group:2 * group])
            if not mine:
                n_pair = len(copies)
        gain1[yb] = jnp.broadcast_to(gain_ref[...], (8, feats))
        ready()
        out = []

        def send(source, target, sem, device):
            copy = remote(source, target, sem, device)
            copy.start()
            out.append(copy)

        for copy in copies[:n_via]:
            copy.wait()
        for g in range(3):
            send(third(4, g), third(6, g), block_sems["via"][g], pair)
        send(w_mix.at[3], w_mix.at[5], block_sems["via"][3], pair)
        send(w_mix.at[4, 0:group], w_mix.at[6, 0:group], block_sems["via"][4], pair)
        for copy in copies[n_via:n_outer]:
            copy.wait()
        for g in range(3):
            send(third(2, g), w1_in.at[g, yb], block_sems["outer"][g], outer)
        send(w_mix.at[1], w1_mix.at[yb, 0:2 * group], block_sems["outer"][3], outer)
        send(w_mix.at[2, 0:group], w1_mix.at[yb, 2 * group:3 * group], block_sems["outer"][4], outer)
        for copy in copies[n_outer:n_pair]:
            copy.wait()
        for g in range(4):
            send(third(0, g), w1_in.at[g, yb], block_sems["pair"][g], pair)
        send(w_mix.at[0], w1_mix.at[yb, 0:2 * group], block_sems["pair"][4], pair)
        for device, sem in zip((pair, outer, diagonal), block_sems["gain"]):
            send(gain1.at[yb], gain1.at[yb], sem, device)
        for g in range(3):
            remote(third(6, g), third(6, g), block_sems["via"][g], pair).wait_recv()
            send(third(6, g), w1_in.at[g, other], block_sems["forward"][g], outer)
        remote(w_mix.at[5], w_mix.at[5], block_sems["via"][3], pair).wait_recv()
        send(w_mix.at[5], w1_mix.at[other, 0:2 * group], block_sems["forward"][3], outer)
        remote(w_mix.at[6, 0:group], w_mix.at[6, 0:group], block_sems["via"][4], pair).wait_recv()
        send(w_mix.at[6, 0:group], w1_mix.at[other, 2 * group:3 * group], block_sems["forward"][4], outer)
        for copy in copies[n_pair:]:
            copy.wait()
        for g in range(4):
            remote(w1_in.at[g, other], w1_in.at[g, other], block_sems["pair"][g], pair).wait_recv()
        remote(w1_mix.at[other, 0:2 * group], w1_mix.at[other, 0:2 * group], block_sems["pair"][4], pair).wait_recv()
        remote(gain1.at[other], gain1.at[other], block_sems["gain"][0], pair).wait_recv()
        for copy in out:
            copy.wait_send()

    def pieces_of_ring(copy, after=None):
        ring_sem = {}

        def onward(stage, piece, upward):
            block = around(-stage) if upward else around(stage)
            sem = next(sems)
            ring_sem[(stage, piece, upward)] = sem
            copy(block, piece, sem, up_z if upward else down_z, "start")
            sent.append(lambda: copy(block, piece, sem, up_z if upward else down_z, "wait_send"))

        def last(piece, upward):
            return (piece < 2) == upward

        for piece in (2, 3, 0, 1):
            onward(0, piece, True)
            onward(0, (piece + 2) % 4, False)
        if after is not None:
            after(-1)
        for stage in range(4):
            for piece in (2, 3, 0, 1):
                for upward in (True, False):
                    p = piece if upward else (piece + 2) % 4
                    if stage == 3 and not last(p, upward):
                        continue
                    block = around(-1 - stage) if upward else around(1 + stage)
                    copy(block, p, ring_sem[(stage, p, upward)], up_z if upward else down_z, "wait_recv")
                    if stage < 2 or (stage == 2 and last(p, upward)):
                        onward(stage + 1, p, upward)
            if after is not None:
                after(stage)

    sent = []
    main_n, main_w, part_g = 3 * HEAD, 4 * HEAD, 2 * HEAD
    image_rows = n_col * patches
    late = image_rows // 2
    early = image_rows - late
    y_rows = early // 2

    def member_hidden(member, g):
        if g == 3:
            start = 6 * part_g + member * 3 * part_g
            return start, start + main_w
        start = (member * 3 + g) * part_g
        return start, start

    def first_layer():
        waits = {"stage": [], "own": [], "mix": [], "mix_stage": []}
        count = iter(range(1000))

        def fetch(source, target, kind):
            copy = pltpu.make_async_copy(source, target, w_sem.at[next(count)])
            copy.start()
            waits[kind].append(copy)

        def columns_at(start, size):
            return pl.ds(pl.multiple_of(start, HEAD), size)

        for g in range(4):
            fetch(wup_ref.at[:, columns_at(member_hidden(other, g)[1], part_g)], w_gs.at[g], "stage")
        xf = x_ref[...].astype(F32).reshape(2 * patches, feats)
        sums = jnp.sum(xf, axis=-1, keepdims=True)
        squares = jnp.sum(xf * xf, axis=-1, keepdims=True)
        stat[row] = column_stats(sums, squares)
        xraw[yb] = x_ref[...]
        gathered[yb, :, col] = x_ref[...]
        gain0[yb] = jnp.broadcast_to(gain_ref[...], (8, feats))
        ready()
        x_copy = remote(xraw.at[yb], xraw.at[yb], x_spread[0], pair)
        x_copy.start()
        stat_copies = []
        for step in range(1, n_row):
            copy = remote(stat.at[row], stat.at[row], next(sems), {"row": lax.rem(row + step, n_row)})
            copy.start()
            stat_copies.append(copy)
        finish_own = col_gather(lambda c: gathered.at[yb, :, c])
        gain_copy = remote(gain0.at[yb], gain0.at[yb], next(sems), pair)
        gain_copy.start()
        for device, sem in ((outer, x_spread[1]), (diagonal, x_spread[2])):
            copy = remote(xraw.at[yb], xraw.at[yb], sem, device)
            copy.start()
            sent.append(copy.wait_send)

        def group_at(i):
            return lax.rem(z + (0, 3, 1, 2)[i], 4)

        def traced_group_at(i):
            return lax.rem(z + jnp.where(i == 0, 0, jnp.where(i == 1, 3, i - 1)), 4)

        g_base = next(sems)
        for _ in range(3):
            next(sems)
        for g in range(4):
            fetch(wup_ref.at[:, columns_at(member_hidden(yb, g)[1], part_g)], w_g.at[g, yb], "own")
        for block in range(NZ):
            member, g = block // 4, block % 4
            if g == 3:
                start = member_hidden(member, g)[0]
                fetch(wup_ref.at[:, start:start + main_w], w_main.at[block], "own")
            else:
                cols = slice((member * 3 + g) * HEAD, (member * 3 + g + 1) * HEAD)
                for k, w_ref in enumerate((wq_ref, wk_ref, wv_ref)):
                    fetch(w_ref.at[:, cols], w_main.at[block, :, k * HEAD:(k + 1) * HEAD], "own")
        for member, kind in ((other, "mix_stage"), (yb, "mix")):
            for g in range(4):
                target = w_ms.at[g] if kind == "mix_stage" else w_mix.at[yb * 4 + g]
                rows = columns_at(member_hidden(member, g)[0], wide_mix if g == 3 else part_g)
                if g == 3:
                    fetch(wdn_ref.at[rows], target, kind)
                else:
                    fetch(wout_ref.at[columns_at((member * 3 + g) * HEAD, HEAD)], target.at[0:HEAD], kind)
                    fetch(wdn_ref.at[rows], target.at[HEAD:narrow_mix], kind)
        for copy in waits["stage"]:
            copy.wait()
        for i in range(4):
            g = group_at(i)
            copy = remote(w_gs.at[g], w_g.at[g, yb], g_base + i, pair)
            copy.start()
            sent.append(copy.wait_send)
        x_copy.wait()
        gathered[other, :, col] = xraw[other]
        finish_other = col_gather(lambda c: gathered.at[other, :, c])
        finish_own()
        for copy in stat_copies:
            copy.wait()
        stat_col[0, col] = lane_stats(jnp.sum(stat[...], axis=0))
        finish_stats = col_direct(lambda c: stat_col.at[0, c])
        for copy in waits["own"]:
            copy.wait()
        finish_other()
        for copy in finish_stats:
            copy.wait()
        gain_copy.wait()
        columns = to_columns(stat_col[0])
        for c in range(n_col):
            for k in range(2):
                gathered[k, :, c] = normalise(gathered[k, :, c], columns, c, gain0[k, 0:1])

        bufs = {
            "G": (gs_p, gs_m, gr_p, gr_m), "Z": (zs_p, zs_m, zr_p, zr_m), "Y": (ys_p, ys_m, yr_p, yr_m),
        }
        tables = {True: {}, False: {}}
        pair_base = next(sems)
        for _ in range(NZ - 1):
            next(sems)

        def by_part(kind, block, action):
            if kind == "G":
                action(part_g)
            else:
                by_width(block, main_n, main_w, action)

        def move(kind, source, target, sem, device, block, what):
            by_part(kind, block, lambda w: getattr(remote(source.at[:, 0:w], target.at[:, 0:w], sem, device), what)())

        def ring_block(stage, upward):
            return around(4 - stage) if upward else around(stage - 4)

        def term(kind, h, block):
            g, image = lax.rem(block, 4), lax.div(block, 4)
            if kind == "G":
                return own_g[g, image, h]
            if kind == "Z":
                return own[h * 4 + g, image, early:image_rows]
            return own[yb * 4 + g, image, h * y_rows:(h + 1) * y_rows]

        def reserve(kind, stage, h, upward):
            sem = next(sems)
            tables[upward][(kind, stage, h)] = sem
            send_buf = bufs[kind][0 if upward else 1].at[stage, h]
            device = up_z if upward else down_z
            block = ring_block(stage, upward)
            sent.append(lambda: move(kind, send_buf, send_buf, sem, device, block, "wait_send"))

        def hop(kind, stage, h, upward):
            send_buf = bufs[kind][0 if upward else 1]
            recv_buf = bufs[kind][2 if upward else 3]
            device = up_z if upward else down_z
            block = ring_block(stage, upward)
            value = term(kind, h, block)
            if stage >= 2 or (stage == 1 and h == (0 if upward else 1)):
                buf = recv_buf.at[stage - 1, h]
                move(kind, buf, buf, tables[upward][(kind, stage - 1, h)], device, block, "wait_recv")
                value = value + recv_buf[stage - 1, h].astype(F32)
            send_buf[stage, h] = value.astype(BF16)
            if (kind, stage, h) not in tables[upward]:
                reserve(kind, stage, h, upward)
            move(kind, send_buf.at[stage, h], recv_buf.at[stage, h], tables[upward][(kind, stage, h)], device, block, "start")

        for kind in ("G", "Z"):
            reserve(kind, 0, 0, True)
            reserve(kind, 0, 1, False)
            reserve(kind, 1, 1, True)
            reserve(kind, 1, 0, False)

        def order(i):
            away = 4 - lax.div(i + 1, 2)
            return around(jnp.where(lax.rem(i, 2) == 1, away, -away))

        def send_pair(i):
            block = order(i)
            pair_s[i] = own[other * 4 + lax.rem(block, 4), lax.div(block, 4), 0:early].astype(BF16)
            move("Y", pair_s.at[i], pair_r.at[i], pair_base + i, pair, block, "start")

        n_tok = 2 * image_rows

        def product(i, carry):
            g = traced_group_at(i)
            for member in range(2):
                own[member * 4 + g] = jnp.dot(
                    gathered[yb].reshape(n_tok, feats), w_main[member * 4 + g], preferred_element_type=F32
                ).reshape(2, image_rows, main_w)

            @pl.when(i == 0)
            def _():
                hop("Z", 0, 0, True)
                hop("Z", 0, 1, False)

            @pl.when(i == 1)
            def _():
                hop("Z", 1, 1, True)

            @pl.when(i == 2)
            def _():
                hop("Z", 1, 0, False)

            send_pair(i)
            return carry

        def product_g(i, carry):
            g = traced_group_at(i)
            remote(w_g.at[g, other], w_g.at[g, other], g_base + i, pair).wait_recv()
            own_g[g] = (
                jnp.dot(gathered[0].reshape(n_tok, feats), w_g[g, 0], preferred_element_type=F32)
                + jnp.dot(gathered[1].reshape(n_tok, feats), w_g[g, 1], preferred_element_type=F32)
            ).reshape(2, 2, image_rows // 2, part_g)

            @pl.when(i == 0)
            def _():
                hop("G", 0, 0, True)
                hop("G", 0, 1, False)

            @pl.when(i == 1)
            def _():
                hop("G", 1, 1, True)

            @pl.when(i == 2)
            def _():
                hop("G", 1, 0, False)

            return carry

        lax.fori_loop(0, 4, product, 0)

        def rest_of_pair(i, carry):
            send_pair(i)
            return carry

        lax.fori_loop(4, NZ, rest_of_pair, 0)
        for copy in waits["mix_stage"]:
            copy.wait()
        mix_sems = [next(sems) for _ in range(4)]

        def send_mix(g):
            n = wide_mix if g == 3 else narrow_mix
            copy = remote(w_ms.at[g, 0:n], w_mix.at[yb * 4 + g, 0:n], mix_sems[g], pair)
            copy.start()
            sent.append(copy.wait_send)

        for i in range(NZ):
            sent.append(lambda i=i: move(
                "Y", pair_s.at[i], pair_s.at[i], pair_base + i, pair, order(jnp.int32(i)), "wait_send"))

        def pair_sum(i):
            block = order(jnp.int32(i))
            move("Y", pair_r.at[i], pair_r.at[i], pair_base + i, pair, block, "wait_recv")
            at = own.at[yb * 4 + lax.rem(block, 4), lax.div(block, 4), 0:early]
            at[...] = at[...] + pair_r[i].astype(F32)

        def four(kind, stage, before=(None, None)):
            for sums, h, upward in ((before[0], 1, True), (before[1], 0, False), (None, 0, True), (None, 1, False)):
                if sums is not None:
                    pair_sum(sums)
                hop(kind, stage, h, upward)

        def all_in(kind):
            for h, upward in ((1, True), (0, False), (0, True), (1, False)):
                buf = bufs[kind][2 if upward else 3].at[3, h]
                move(kind, buf, buf, tables[upward][(kind, 3, h)], up_z if upward else down_z, z, "wait_recv")

        hop("Z", 1, 0, True)
        hop("Z", 1, 1, False)
        lax.fori_loop(0, 1, product_g, 0)
        four("Z", 2)
        lax.fori_loop(1, 3, product_g, 0)
        four("Z", 3)
        lax.fori_loop(3, 4, product_g, 0)
        hop("G", 1, 0, True)
        hop("G", 1, 1, False)
        pair_sum(0)
        hop("Y", 0, 0, True)
        hop("Y", 0, 1, False)
        four("G", 2)
        all_in("Z")
        last_s[...] = (term("Z", other, z) + zr_p[3, other].astype(F32) + zr_m[3, other].astype(F32)).astype(BF16)
        last_sem = next(sems)
        move("Z", last_s, last_r, last_sem, pair, z, "start")
        sent.append(lambda: move("Z", last_s, last_s, last_sem, pair, z, "wait_send"))
        for g in (3, 0, 1, 2):
            send_mix(g)
        four("Y", 1, (1, 2))
        four("G", 3)
        four("Y", 2, (3, 4))
        four("Y", 3, (5, 6))
        is_wide = wide(z)
        all_in("G")
        for h in range(2):
            hidden = gelu(term("G", h, z) + gr_p[3, h].astype(F32) + gr_m[3, h].astype(F32))

            @pl.when(is_wide)
            def _():
                acts[z, h, :, main_w:wide_mix] = hidden

            @pl.when(jnp.logical_not(is_wide))
            def _():
                acts[z, h, :, HEAD:narrow_mix] = hidden

        full[early:image_rows] = term("Z", yb, z) + zr_p[3, yb].astype(F32) + zr_m[3, yb].astype(F32)
        move("Z", last_r, last_r, last_sem, pair, z, "wait_recv")
        full[early:image_rows] = full[early:image_rows] + last_r[...].astype(F32)
        pair_sum(7)
        all_in("Y")
        for h in range(2):
            full[h * y_rows:(h + 1) * y_rows] = term("Y", h, z) + yr_p[3, h].astype(F32) + yr_m[3, h].astype(F32)

        @pl.when(is_wide)
        def _():
            acts[z, :, :, 0:main_w] = gelu(full[...]).reshape(2, image_rows // 2, main_w)

        @pl.when(jnp.logical_not(is_wide))
        def _():
            value = full[:, 0:main_n].astype(BF16)
            result = attend(value[:, 0:HEAD], value[:, HEAD:2 * HEAD], value[:, 2 * HEAD:3 * HEAD])
            acts[z, :, :, 0:HEAD] = result.reshape(2, image_rows // 2, HEAD)

        piece_rows = image_rows // 4

        def act_copy(block, piece, sem, device, what):
            rows = slice((piece % 2) * piece_rows, (piece % 2 + 1) * piece_rows)

            def action(w):
                part = acts.at[block, piece // 2, rows, 0:w]
                getattr(remote(part, part, sem, device), what)()

            by_width(block, narrow_mix, wide_mix, action)

        def add_product(k, block):
            g, image = lax.rem(block, 4), lax.div(block, 4)

            def add(w):
                acc[k, image] = acc[k, image] + jnp.dot(
                    acts[block, :, :, 0:w].reshape(image_rows, w), w_mix[k * 4 + g, 0:w], preferred_element_type=F32)

            by_width(block, narrow_mix, wide_mix, add)

        def add_known(k, block):
            g, image = block % 4, block // 4
            w = wide_mix if g == 3 else narrow_mix
            acc[k, image] = acc[k, image] + jnp.dot(
                acts[block, :, :, 0:w].reshape(image_rows, w), w_mix[k * 4 + g, 0:w], preferred_element_type=F32)

        acc[...] = jnp.zeros_like(acc)

        def after_stage(stage):
            if stage == -1:
                for copy in waits["mix"]:
                    copy.wait()
                add_product(yb, z)
            elif stage < 3:
                add_product(yb, around(-1 - stage))
                add_product(yb, around(1 + stage))
                if stage == 2:
                    for g in (3, 0, 1, 2):
                        n = wide_mix if g == 3 else narrow_mix
                        part = w_mix.at[other * 4 + g, 0:n]
                        remote(part, part, mix_sems[g], pair).wait_recv()
                        for block in (g, g + 4):
                            pl.when(around(4) != block)(lambda block=block: add_known(other, block))
            else:
                add_product(yb, around(4))
                add_product(other, around(4))

        pieces_of_ring(act_copy, after_stage)

        for k in range(2):
            mix1_s[k] = acc[k].astype(BF16).reshape(2, n_x, 2, patches, feats)
        total = col_sum_by_core()
        terms[yb] = total.astype(BF16)
        for device, sem in ((pair, spread[0]), (outer, spread[1]), (diagonal, spread[2])):
            copy = remote(terms.at[yb], terms.at[yb], sem, device)
            copy.start()
        for wait in sent:
            wait()
        sent.clear()
        for g in range(3):
            remote(w1_in.at[g, other], w1_in.at[g, other], block_sems["outer"][g], outer).wait_recv()
            remote(w1_in.at[g, yb], w1_in.at[g, yb], block_sems["forward"][g], outer).wait_recv()
        for half_k, name in ((other, "outer"), (yb, "forward")):
            for k, (lo, hi) in ((3, (0, 2 * group)), (4, (2 * group, 3 * group))):
                part = w1_mix.at[half_k, lo:hi]
                remote(part, part, block_sems[name][k], outer).wait_recv()
        remote(gain1.at[other], gain1.at[other], block_sems["gain"][1], outer).wait_recv()
        remote(gain1.at[yb], gain1.at[yb], block_sems["gain"][2], diagonal).wait_recv()
        remote(terms.at[other], terms.at[other], spread[0], pair).wait_recv()

    x_spread = [next(sems) for _ in range(3)]
    spread = [next(sems) for _ in range(3)]
    pl.when(in_first)(first_layer)

    @pl.when(in_second)
    def _():
        remote(terms.at[other], terms.at[other], spread[1], outer).wait_recv()
        remote(terms.at[yb], terms.at[yb], spread[2], diagonal).wait_recv()
        remote(xraw.at[other], xraw.at[other], x_spread[1], outer).wait_recv()
        remote(xraw.at[yb], xraw.at[yb], x_spread[2], diagonal).wait_recv()
    for k in range(2):
        xb1[k] = (xraw[k].astype(F32) + terms[0, k].astype(F32) + terms[1, k].astype(F32)).astype(BF16)

    @pl.when(in_first)
    def _():
        y_ref[...] = xb1[yb]

    n_tok = 2 * n_col * patches
    both = xb1[...].astype(F32).reshape(2, 2 * patches, feats)
    sums = jnp.sum(jnp.sum(both, axis=-1, keepdims=True), axis=0)
    squares = jnp.sum(jnp.sum(both * both, axis=-1, keepdims=True), axis=0)
    stat1[z] = column_stats(sums, squares)
    copies = []
    for step in range(1, NZ):
        copy = remote(stat1.at[z], stat1.at[z], next(sems), {"row": yb * NZ + around(step)})
        copy.start()
        copies.append(copy)
    finish_k = []
    for k in range(2):
        gathered1[k, :, col] = xb1[k]
        finish_k.append(col_gather(lambda c, k=k: gathered1.at[k, :, c]))
    for copy in copies:
        copy.wait()
    stat_col[1, col] = lane_stats(jnp.sum(stat1[...], axis=0))
    finish_stats1 = col_direct(lambda c: stat_col.at[1, c])
    for finish in finish_k:
        finish()
    for copy in finish_stats1:
        copy.wait()
    columns1 = to_columns(stat_col[1])
    for c in range(n_col):
        for k in range(2):
            gathered1[k, :, c] = normalise(gathered1[k, :, c], columns1, c, gain1[k, 0:1])

    piece_long = 2 * patches
    piece_short = 3 * patches // 2
    third_rows = patches // 2

    def partial_product(g):
        return (
            jnp.dot(gathered1[0].reshape(n_tok, feats), w1_in[g, 0], preferred_element_type=F32)
            + jnp.dot(gathered1[1].reshape(n_tok, feats), w1_in[g, 1], preferred_element_type=F32)
        )

    @pl.when(in_first)
    def _():
        for g in range(3):
            value = partial_product(g).reshape(NZ, 4, third_rows, group)
            own1[:, :, g * third_rows:(g + 1) * third_rows] = value

    @pl.when(in_second)
    def _():
        for g in range(4):
            value = partial_product(g).reshape(2, 4, piece_long, group)
            own1[g] = value[0]
            own1[4 + g] = value[1]

    def by_section(action):
        either(in_first, lambda: action(piece_short), lambda: action(piece_long))

    up1, down1 = {}, {}

    def far(h, upward):
        return (h < 2) == upward

    def hop1(stage, h, upward):
        send_buf, recv_buf = (zs1_p, zr1_p) if upward else (zs1_m, zr1_m)
        table = up1 if upward else down1
        device = up_z if upward else down_z
        block = around(4 - stage) if upward else around(stage - 4)
        value = own1[block, h]
        if stage >= 2 or (stage == 1 and far(h, upward)):
            sem = table[(stage - 1, h)]
            by_section(lambda n: remote(
                recv_buf.at[stage - 1, h, 0:n], recv_buf.at[stage - 1, h, 0:n], sem, device).wait_recv())
            value = value + recv_buf[stage - 1, h].astype(F32)
        send_buf[stage, h] = value.astype(BF16)
        sem_out = next(sems)
        table[(stage, h)] = sem_out
        by_section(lambda n: remote(
            send_buf.at[stage, h, 0:n], recv_buf.at[stage, h, 0:n], sem_out, device).start())
        sent.append(lambda: by_section(lambda n: remote(
            send_buf.at[stage, h, 0:n], recv_buf.at[stage, h, 0:n], sem_out, device).wait_send()))

    for h in (0, 1):
        hop1(0, h, True)
        hop1(0, h + 2, False)
    for stage in (1, 2, 3):
        for h in (2, 3, 0, 1):
            hop1(stage, h, True)
            hop1(stage, (h + 2) % 4, False)
    for h in range(4):
        by_section(lambda n: remote(zr1_p.at[3, h, 0:n], zr1_p.at[3, h, 0:n], up1[(3, h)], up_z).wait_recv())
        by_section(lambda n: remote(zr1_m.at[3, h, 0:n], zr1_m.at[3, h, 0:n], down1[(3, h)], down_z).wait_recv())

    def summed(h):
        return own1[z, h] + zr1_p[3, h].astype(F32) + zr1_m[3, h].astype(F32)

    has_head = jnp.logical_and(in_second, jnp.logical_not(wide(z)))

    @pl.when(has_head)
    def _():
        value = jnp.concatenate([summed(h) for h in range(4)], axis=0).astype(BF16)
        result = attend(value[:, 0:HEAD], value[:, HEAD:2 * HEAD], value[:, 2 * HEAD:3 * HEAD])
        acts1[z, :, :, 0:HEAD] = result.reshape(4, piece_long, HEAD)

    @pl.when(jnp.logical_not(has_head))
    def _():
        for h in range(4):
            acts1[z, h] = gelu(summed(h))

    def by_kind(block, action):
        either(
            in_first,
            lambda: action(piece_short, group),
            lambda: by_width(block, HEAD, group, lambda w: action(piece_long, w)),
        )

    def act_copy1(block, piece, sem, device, what):
        def action(n, w):
            part = acts1.at[block, piece, 0:n, 0:w]
            getattr(remote(part, part, sem, device), what)()

        by_kind(block, action)

    image_sums = []

    def send_image(image):
        first = image * 4
        span = pl.ds(pl.multiple_of(image * image_rows, image_rows), image_rows)

        @pl.when(in_first)
        def _():
            for k in range(2):
                total = None
                for g in range(3):
                    hidden = acts1[pl.ds(first, 4), :, g * third_rows:(g + 1) * third_rows].reshape(image_rows, group)
                    term = jnp.dot(hidden, w1_mix[k, g * group:(g + 1) * group], preferred_element_type=F32)
                    total = term if total is None else total + term
                acc1[k, span] = total

        @pl.when(in_second)
        def _():
            value = jnp.concatenate(
                [acts1[first + j, :, :, 0:HEAD].reshape(image_rows, HEAD) for j in range(3)]
                + [acts1[first + 3].reshape(image_rows, group)], axis=1)
            for k in range(2):
                acc1[k, span] = jnp.dot(value, w1_mix[k, 0:2 * group], preferred_element_type=F32)

        for k in range(2):
            mix1_s[k, image] = acc1[k, span].astype(BF16).reshape(n_x, 2, patches, feats)
        for slot, target_x, target_core, device in col_peers():
            copy = remote(
                mix1_s.at[:, image, target_x, target_core], mix_r.at[slot, :, image], next(sems), device)
            copy.start()
            image_sums.append(copy)

    near = lax.div(z, 4)

    def after_stage1(stage):
        if stage == 2:
            send_image(near)

    pieces_of_ring(act_copy1, after_stage1)
    send_image(1 - near)
    for copy in image_sums:
        copy.wait()
    total = mix1_s[:, :, chip_x, core].astype(F32)
    for slot in range(n_col - 1):
        total = total + mix_r[slot].astype(F32)
    ys1[...] = total.astype(BF16)
    to_pair, to_outer, to_diagonal = next(sems), next(sems), next(sems)

    @pl.when(in_first)
    def _():
        copies = [remote(ys1.at[other], yr1.at[1], to_outer, outer), remote(ys1.at[yb], yr1.at[2], to_diagonal, diagonal)]
        for copy in copies:
            copy.start()
        for copy in copies:
            copy.wait_send()

    @pl.when(in_second)
    def _():
        copy = remote(ys1.at[other], yr1.at[0], to_pair, pair)
        copy.start()
        copy.wait()
        remote(yr1.at[1], yr1.at[1], to_outer, outer).wait_recv()
        remote(yr1.at[2], yr1.at[2], to_diagonal, diagonal).wait_recv()
        result = xb1[yb].astype(F32) + ys1[yb].astype(F32)
        for k in range(3):
            result = result + yr1[k].astype(F32)
        y_ref[...] = result.astype(BF16)

    assert next(sems) < 320
    for wait in sent:
        wait()

    @pl.when(in_first)
    def _():
        for device, sem in ((pair, spread[0]), (outer, spread[1]), (diagonal, spread[2])):
            remote(terms.at[yb], terms.at[yb], sem, device).wait_send()


def layers(x, weights):
    gain, wq, wk, wv, wup, wout, wdown = weights
    n_col = lax.axis_size("col")
    images, patches, feats = x.shape
    wide_in = 6 * HEAD
    vmem = pl.BlockSpec(memory_space=pltpu.VMEM)
    anywhere = pl.BlockSpec(memory_space=pl.ANY)
    rows = n_col * patches
    late = rows // 2
    early = rows - late
    g_buf = pltpu.VMEM((4, 2, rows // 2, 2 * HEAD), BF16)
    z_buf = pltpu.VMEM((4, 2, late, 4 * HEAD), BF16)
    y_buf = pltpu.VMEM((4, 2, early // 2, 4 * HEAD), BF16)
    pair_buf = pltpu.VMEM((NZ, early, 4 * HEAD), BF16)
    z1_buf = pltpu.VMEM((4, 4, 2 * patches, feats), BF16)
    scratch = [
        pltpu.VMEM((NZ, feats, wide_in), BF16),
        pltpu.VMEM((NZ, wide_in, feats), BF16),
        pltpu.VMEM((NZ, feats, 4 * HEAD), BF16),
        pltpu.VMEM((4, 2, feats, 2 * HEAD), BF16),
        pltpu.VMEM((4, feats, 2 * HEAD), BF16),
        pltpu.VMEM((4, wide_in, feats), BF16),
        pltpu.VMEM((2, 2, n_col, patches, feats), BF16),
        pltpu.VMEM((2, 8, feats), F32),
        pltpu.VMEM((NZ, 2, rows, 4 * HEAD), F32),
        pltpu.VMEM((4, 2, 2, rows // 2, 2 * HEAD), F32),
        pltpu.VMEM((2 * NZ, 8, 128), F32),
        g_buf, g_buf, g_buf, g_buf, z_buf, z_buf, z_buf, z_buf, y_buf, y_buf, y_buf, y_buf, pair_buf, pair_buf,
        pltpu.VMEM((late, 4 * HEAD), BF16), pltpu.VMEM((late, 4 * HEAD), BF16),
        pltpu.VMEM((rows, 4 * HEAD), F32),
        pltpu.VMEM((NZ, 2, rows // 2, wide_in), BF16),
        pltpu.VMEM((2, 2, rows, feats), F32),
        pltpu.VMEM((2, n_col, 8, 128), F32),
        pltpu.VMEM((2, 2, patches, feats), BF16),
        pltpu.VMEM((2, 2, 2, patches, feats), BF16),
        pltpu.VMEM((2, 2, n_col // 2, patches, feats), BF16),
        pltpu.VMEM((2, 2, n_col // 2, patches, feats), BF16),
        pltpu.VMEM((n_col // 2 - 1, 2, 2, patches, feats), BF16),
        pltpu.VMEM((4, 2, feats, feats), BF16),
        pltpu.VMEM((2, 3 * feats, feats), BF16),
        pltpu.VMEM((2, 8, feats), F32),
        pltpu.VMEM((2, 2, patches, feats), BF16),
        pltpu.VMEM((2, 2, n_col, patches, feats), BF16),
        pltpu.VMEM((NZ, 4, 2 * patches, feats), F32),
        pltpu.VMEM((NZ, 8, 128), F32),
        z1_buf, z1_buf, z1_buf, z1_buf,
        pltpu.VMEM((NZ, 4, 2 * patches, feats), BF16),
        pltpu.VMEM((2, 2 * n_col * patches, feats), F32),
        pltpu.VMEM((2, 2, n_col // 2, 2, patches, feats), BF16),
        pltpu.VMEM((n_col - 1, 2, 2, patches, feats), BF16),
        pltpu.VMEM((2, 2, patches, feats), BF16),
        pltpu.VMEM((3, 2, patches, feats), BF16),
        pltpu.SemaphoreType.DMA((64,)),
        pltpu.SemaphoreType.DMA((320,)),
        pltpu.SemaphoreType.DMA((320,)),
    ]
    return pl.pallas_call(
        functools.partial(layers_kernel, n_col, patches, feats),
        out_shape=jax.ShapeDtypeStruct(x.shape, BF16),
        in_specs=[vmem, vmem] + [anywhere] * 6,
        out_specs=vmem,
        scratch_shapes=scratch,
        compiler_params=pltpu.CompilerParams(
            collective_id=0, has_side_effects=True, vmem_limit_bytes=67043328
        ),
    )(x, gain[None], wq, wk, wv, wup, wout, wdown)


def local(tokens, ln_gain, w_query, w_key, w_value, w_up, w_out, w_down):
    weights = (ln_gain[0], w_query[0], w_key[0], w_value[0], w_up[0], w_out[0], w_down[0])
    return layers(tokens, weights)[None]


def solution(mesh):
    return jax.shard_map(
        local,
        mesh=mesh,
        in_specs=(
            P(None, "col", "row"),
            P("section", "row"),
            P("section", "row", "col"),
            P("section", "row", "col"),
            P("section", "row", "col"),
            P("section", "row", "col"),
            P("section", "col", "row"),
            P("section", "col", "row"),
        ),
        out_specs=P("section", None, "col", "row"),
        check_vma=False,
    )
```

```python
import functools
import math

import jax
import jax.numpy as jnp
from jax import lax
from jax.experimental import pallas as pl
from jax.experimental.pallas import tpu as pltpu
from jax.sharding import PartitionSpec as P

D = 6144
HEAD = 128
EPS = 1e-06
NZ = 8
MESH = pl.DeviceIdType.MESH
BF16 = jnp.bfloat16
F32 = jnp.float32


def wide(block):
    return lax.rem(block, 4) == 3


def either(condition, yes, no):
    def run(action):
        def branch():
            action()

        return branch

    lax.cond(condition, run(yes), run(no))


def by_width(block, narrow_size, wide_size, action):
    either(wide(block), lambda: action(wide_size), lambda: action(narrow_size))


def layers_kernel(
    n_col, patches, feats,
    x_ref, gain_ref, wq_ref, wk_ref, wv_ref, wup_ref, wout_ref, wdn_ref,
    y_ref,
    w_in, w_mix, w_main, w_g, w_gs, w_ms, gathered, gain0, own, own_g, stat,
    gs_p, gs_m, gr_p, gr_m, zs_p, zs_m, zr_p, zr_m, ys_p, ys_m, yr_p, yr_m, pair_s, pair_r, last_s, last_r,
    full, acts, acc,
    stat_col, xraw, terms, mix_d, mix_t, mix_e,
    w1_in, w1_mix, gain1, xb1, gathered1, own1, stat1, zs1_p, zs1_m, zr1_p, zr1_m,
    acts1, acc1, mix1_s, mix_r, ys1, yr1,
    w_sem, ssem, rsem,
):
    section = lax.axis_index("section")
    row = lax.axis_index("row")
    col = lax.axis_index("col")
    n_row = 2 * NZ
    yb = lax.div(row, NZ)
    z = lax.rem(row, NZ)
    other = 1 - yb

    def around(step):
        return lax.rem(z + step + NZ, NZ)

    up_z = {"row": yb * NZ + around(1)}
    down_z = {"row": yb * NZ + around(-1)}
    pair = {"row": other * NZ + z}
    outer = {"section": 1 - section, "row": other * NZ + z}
    diagonal = {"section": 1 - section, "row": row}
    n_x = n_col // 2
    core = lax.rem(col, 2)
    chip_x = lax.div(col, 2)
    sibling = {"col": 2 * chip_x + 1 - core}

    def along_x(step):
        return lax.rem(chip_x + step, n_x)

    def same_core(step):
        return {"col": 2 * along_x(step) + core}
    in_first = section == 0
    in_second = section == 1

    narrow_mix, wide_mix = 3 * HEAD, 6 * HEAD

    barrier = pltpu.get_barrier_semaphore()
    for step in range(1, n_row):
        pl.semaphore_signal(barrier, inc=1, device_id={"row": lax.rem(row + step, n_row)}, device_id_type=MESH)
    for step in range(1, n_col):
        pl.semaphore_signal(barrier, inc=1, device_id={"col": lax.rem(col + step, n_col)}, device_id_type=MESH)
    for device in (outer, diagonal):
        pl.semaphore_signal(barrier, inc=1, device_id=device, device_id_type=MESH)

    sems = iter(range(1000))

    def remote(source, target, sem, device):
        return pltpu.make_async_remote_copy(
            src_ref=source, dst_ref=target, send_sem=ssem.at[sem], recv_sem=rsem.at[sem],
            device_id=device, device_id_type=MESH,
        )

    def ready():
        pl.semaphore_wait(barrier, n_row - 1 + n_col - 1 + 2)

    def column_stats(sums, squares):
        columns = jnp.concatenate(
            [jnp.broadcast_to(sums, (2 * patches, 128)), jnp.broadcast_to(squares, (2 * patches, 128))], axis=0
        )
        return columns.T[0:8]

    def lane_stats(total):
        mean = total * (1.0 / D)
        lane = lax.broadcasted_iota(jnp.int32, (8, 128), 1)
        shifted = pltpu.roll(mean, 2 * patches, axis=1)
        var = jnp.maximum(mean - shifted * shifted, 0.0)
        return jnp.where(lane < 2 * patches, mean, lax.rsqrt(var + EPS))

    def to_columns(table):
        rows = table[:, 0, :]
        return jnp.concatenate([rows] * (128 // n_col), axis=0).T

    def normalise(block, columns, c, gain):
        value = block.astype(F32).reshape(2 * patches, feats)
        mean, scale = columns[0:2 * patches, c:c + 1], columns[2 * patches:4 * patches, c:c + 1]
        return ((value - mean) * scale * gain).astype(BF16).reshape(2, patches, feats)

    def col_gather(view):
        arrive = []
        for step in (1, 3, 2):
            copy = remote(view(col), view(col), next(sems), same_core(step))
            copy.start()
            arrive.append((copy, step))
        first = remote(view(col), view(col), next(sems), sibling)
        first.start()

        def finish():
            handed = [first]
            for copy, step in arrive:
                copy.wait()
                block = view(2 * along_x(n_x - step) + core)
                onward = remote(block, block, next(sems), sibling)
                onward.start()
                handed.append(onward)
            for copy in handed:
                copy.wait()

        return finish

    def gelu(value):
        return (0.5 * value * (1.0 + lax.erf(value * math.sqrt(0.5)))).astype(BF16)

    def attend(query, keyed, valued):
        scores = lax.dot_general(query, keyed, (((1,), (1,)), ((), ())), preferred_element_type=F32)
        scores = scores * (1.0 / math.sqrt(HEAD))
        expo = jnp.exp(scores - jnp.max(scores, axis=-1, keepdims=True))
        probs = (expo / jnp.sum(expo, axis=-1, keepdims=True)).astype(BF16)
        return jnp.dot(probs, valued, preferred_element_type=F32).astype(BF16)

    def col_peers():
        for dx in (2, 1, 3, 0):
            for dc in range(2):
                if dx or dc:
                    target_core = lax.rem(core + dc, 2)
                    yield 2 * dx + dc - 1, along_x(dx), target_core, {"col": 2 * along_x(dx) + target_core}

    def col_direct(view):
        copies = []
        for _, _, _, device in col_peers():
            copy = remote(view(col), view(col), next(sems), device)
            copy.start()
            copies.append(copy)
        return copies

    def col_sum_by_core():
        swaps = []
        for step in (2, 1, 3, 0):
            target = along_x(step)
            swap = remote(mix1_s.at[:, :, target, 1 - core], mix_d.at[:, :, target], next(sems), sibling)
            swap.start()
            swaps.append(swap)
        copies = []
        for step, swap in zip((2, 1, 3), swaps):
            target = along_x(step)
            swap.wait()
            mix_t[:, :, target] = (
                mix1_s[:, :, target, core].astype(F32) + mix_d[:, :, target].astype(F32)).astype(BF16)
            copy = remote(mix_t.at[:, :, target], mix_e.at[step - 1], next(sems), same_core(step))
            copy.start()
            copies.append((copy, step - 1))
        swaps[3].wait()
        value = mix1_s[:, :, chip_x, core].astype(F32) + mix_d[:, :, chip_x].astype(F32)
        for copy, slot in copies:
            copy.wait()
            value = value + mix_e[slot].astype(F32)
        return value

    group = feats
    block_sems = {name: [next(sems) for _ in range(n)] for name, n in
                  (("pair", 5), ("outer", 5), ("via", 5), ("forward", 5), ("gain", 3))}
    mlp_first = 2 * group
    mlp_rest = 3 * group

    def head_cols(member, j):
        return pl.ds(pl.multiple_of((member * 3 + j) * HEAD, HEAD), HEAD)

    def third(at, g):
        return w_in.at[at + g // 2, :, (g % 2) * group:(g % 2 + 1) * group]

    @pl.when(in_second)
    def ship():
        copies = []

        def fetch(source, target):
            copy = pltpu.make_async_copy(source, target, w_sem.at[len(copies)])
            copy.start()
            copies.append(copy)

        start = pl.multiple_of(mlp_first + yb * mlp_rest, group)
        fetch(wup_ref.at[:, pl.ds(start, 2 * group)], w_in.at[4])
        fetch(wup_ref.at[:, pl.ds(pl.multiple_of(start + 2 * group, group), group)], w_in.at[5, :, 0:group])
        fetch(wdn_ref.at[pl.ds(start, 2 * group)], w_mix.at[3])
        fetch(wdn_ref.at[pl.ds(pl.multiple_of(start + 2 * group, group), group)], w_mix.at[4, 0:group])
        n_via = len(copies)
        start = pl.multiple_of(mlp_first + other * mlp_rest, group)
        fetch(wup_ref.at[:, pl.ds(start, 2 * group)], w_in.at[2])
        fetch(wup_ref.at[:, pl.ds(pl.multiple_of(start + 2 * group, group), group)], w_in.at[3, :, 0:group])
        fetch(wdn_ref.at[pl.ds(start, 2 * group)], w_mix.at[1])
        fetch(wdn_ref.at[pl.ds(pl.multiple_of(start + 2 * group, group), group)], w_mix.at[2, 0:group])
        n_outer = len(copies)
        for member, mine in ((other, False), (yb, True)):
            for j in range(3):
                for k, w_ref in enumerate((wq_ref, wk_ref, wv_ref)):
                    span = slice(k * HEAD, (k + 1) * HEAD)
                    at = (j % 2) * group + k * HEAD
                    target = w1_in.at[j, yb, :, span] if mine else w_in.at[j // 2, :, at:at + HEAD]
                    fetch(w_ref.at[:, head_cols(member, j)], target)
            rows = pl.ds(pl.multiple_of(member * group, group), group)
            fetch(wup_ref.at[:, rows], w1_in.at[3, yb] if mine else w_in.at[1, :, group:2 * group])
            fetch(wout_ref.at[rows], w1_mix.at[yb, 0:group] if mine else w_mix.at[0, 0:group])
            fetch(wdn_ref.at[rows], w1_mix.at[yb, group:2 * group] if mine else w_mix.at[0, group:2 * group])
            if not mine:
                n_pair = len(copies)
        gain1[yb] = jnp.broadcast_to(gain_ref[...], (8, feats))
        ready()
        out = []

        def send(source, target, sem, device):
            copy = remote(source, target, sem, device)
            copy.start()
            out.append(copy)

        for copy in copies[:n_via]:
            copy.wait()
        for g in range(3):
            send(third(4, g), third(6, g), block_sems["via"][g], pair)
        send(w_mix.at[3], w_mix.at[5], block_sems["via"][3], pair)
        send(w_mix.at[4, 0:group], w_mix.at[6, 0:group], block_sems["via"][4], pair)
        for copy in copies[n_via:n_outer]:
            copy.wait()
        for g in range(3):
            send(third(2, g), w1_in.at[g, yb], block_sems["outer"][g], outer)
        send(w_mix.at[1], w1_mix.at[yb, 0:2 * group], block_sems["outer"][3], outer)
        send(w_mix.at[2, 0:group], w1_mix.at[yb, 2 * group:3 * group], block_sems["outer"][4], outer)
        for copy in copies[n_outer:n_pair]:
            copy.wait()
        for g in range(4):
            send(third(0, g), w1_in.at[g, yb], block_sems["pair"][g], pair)
        send(w_mix.at[0], w1_mix.at[yb, 0:2 * group], block_sems["pair"][4], pair)
        for device, sem in zip((pair, outer, diagonal), block_sems["gain"]):
            send(gain1.at[yb], gain1.at[yb], sem, device)
        for g in range(3):
            remote(third(6, g), third(6, g), block_sems["via"][g], pair).wait_recv()
            send(third(6, g), w1_in.at[g, other], block_sems["forward"][g], outer)
        remote(w_mix.at[5], w_mix.at[5], block_sems["via"][3], pair).wait_recv()
        send(w_mix.at[5], w1_mix.at[other, 0:2 * group], block_sems["forward"][3], outer)
        remote(w_mix.at[6, 0:group], w_mix.at[6, 0:group], block_sems["via"][4], pair).wait_recv()
        send(w_mix.at[6, 0:group], w1_mix.at[other, 2 * group:3 * group], block_sems["forward"][4], outer)
        for copy in copies[n_pair:]:
            copy.wait()
        for g in range(4):
            remote(w1_in.at[g, other], w1_in.at[g, other], block_sems["pair"][g], pair).wait_recv()
        remote(w1_mix.at[other, 0:2 * group], w1_mix.at[other, 0:2 * group], block_sems["pair"][4], pair).wait_recv()
        remote(gain1.at[other], gain1.at[other], block_sems["gain"][0], pair).wait_recv()
        for copy in out:
            copy.wait_send()

    def pieces_of_ring(copy, after=None):
        ring_sem = {}

        def onward(stage, piece, upward):
            block = around(-stage) if upward else around(stage)
            sem = next(sems)
            ring_sem[(stage, piece, upward)] = sem
            copy(block, piece, sem, up_z if upward else down_z, "start")
            sent.append(lambda: copy(block, piece, sem, up_z if upward else down_z, "wait_send"))

        def last(piece, upward):
            return (piece < 2) == upward

        for piece in (2, 3, 0, 1):
            onward(0, piece, True)
            onward(0, (piece + 2) % 4, False)
        if after is not None:
            after(-1)
        for stage in range(4):
            for piece in (2, 3, 0, 1):
                for upward in (True, False):
                    p = piece if upward else (piece + 2) % 4
                    if stage == 3 and not last(p, upward):
                        continue
                    block = around(-1 - stage) if upward else around(1 + stage)
                    copy(block, p, ring_sem[(stage, p, upward)], up_z if upward else down_z, "wait_recv")
                    if stage < 2 or (stage == 2 and last(p, upward)):
                        onward(stage + 1, p, upward)
            if after is not None:
                after(stage)

    sent = []
    main_n, main_w, part_g = 3 * HEAD, 4 * HEAD, 2 * HEAD
    image_rows = n_col * patches
    late = image_rows // 2
    early = image_rows - late
    y_rows = early // 2

    def member_hidden(member, g):
        if g == 3:
            start = 6 * part_g + member * 3 * part_g
            return start, start + main_w
        start = (member * 3 + g) * part_g
        return start, start

    def first_layer():
        waits = {"stage": [], "own": [], "mix": [], "mix_stage": []}
        count = iter(range(1000))

        def fetch(source, target, kind):
            copy = pltpu.make_async_copy(source, target, w_sem.at[next(count)])
            copy.start()
            waits[kind].append(copy)

        def columns_at(start, size):
            return pl.ds(pl.multiple_of(start, HEAD), size)

        for g in range(4):
            fetch(wup_ref.at[:, columns_at(member_hidden(other, g)[1], part_g)], w_gs.at[g], "stage")
        xf = x_ref[...].astype(F32).reshape(2 * patches, feats)
        sums = jnp.sum(xf, axis=-1, keepdims=True)
        squares = jnp.sum(xf * xf, axis=-1, keepdims=True)
        stat[row] = column_stats(sums, squares)
        xraw[yb] = x_ref[...]
        gathered[yb, :, col] = x_ref[...]
        gain0[yb] = jnp.broadcast_to(gain_ref[...], (8, feats))
        ready()
        x_copy = remote(xraw.at[yb], xraw.at[yb], x_spread[0], pair)
        x_copy.start()
        stat_copies = []
        for step in range(1, n_row):
            copy = remote(stat.at[row], stat.at[row], next(sems), {"row": lax.rem(row + step, n_row)})
            copy.start()
            stat_copies.append(copy)
        finish_own = col_gather(lambda c: gathered.at[yb, :, c])
        gain_copy = remote(gain0.at[yb], gain0.at[yb], next(sems), pair)
        gain_copy.start()

        def group_at(i):
            return lax.rem(z + (0, 3, 1, 2)[i], 4)

        def traced_group_at(i):
            return lax.rem(z + jnp.where(i == 0, 0, jnp.where(i == 1, 3, i - 1)), 4)

        g_base = next(sems)
        for _ in range(3):
            next(sems)
        for g in range(4):
            fetch(wup_ref.at[:, columns_at(member_hidden(yb, g)[1], part_g)], w_g.at[g, yb], "own")
        for block in range(NZ):
            member, g = block // 4, block % 4
            if g == 3:
                start = member_hidden(member, g)[0]
                fetch(wup_ref.at[:, start:start + main_w], w_main.at[block], "own")
            else:
                cols = slice((member * 3 + g) * HEAD, (member * 3 + g + 1) * HEAD)
                for k, w_ref in enumerate((wq_ref, wk_ref, wv_ref)):
                    fetch(w_ref.at[:, cols], w_main.at[block, :, k * HEAD:(k + 1) * HEAD], "own")
        for member, kind in ((other, "mix_stage"), (yb, "mix")):
            for g in range(4):
                target = w_ms.at[g] if kind == "mix_stage" else w_mix.at[yb * 4 + g]
                rows = columns_at(member_hidden(member, g)[0], wide_mix if g == 3 else part_g)
                if g == 3:
                    fetch(wdn_ref.at[rows], target, kind)
                else:
                    fetch(wout_ref.at[columns_at((member * 3 + g) * HEAD, HEAD)], target.at[0:HEAD], kind)
                    fetch(wdn_ref.at[rows], target.at[HEAD:narrow_mix], kind)
        for copy in waits["stage"]:
            copy.wait()
        for i in range(4):
            g = group_at(i)
            copy = remote(w_gs.at[g], w_g.at[g, yb], g_base + i, pair)
            copy.start()
            sent.append(copy.wait_send)
        x_copy.wait()
        gathered[other, :, col] = xraw[other]
        finish_other = col_gather(lambda c: gathered.at[other, :, c])
        finish_own()
        for copy in stat_copies:
            copy.wait()
        stat_col[0, col] = lane_stats(jnp.sum(stat[...], axis=0))
        finish_stats = col_direct(lambda c: stat_col.at[0, c])
        for copy in waits["own"]:
            copy.wait()
        finish_other()
        for copy in finish_stats:
            copy.wait()
        gain_copy.wait()
        columns = to_columns(stat_col[0])
        for c in range(n_col):
            for k in range(2):
                gathered[k, :, c] = normalise(gathered[k, :, c], columns, c, gain0[k, 0:1])

        bufs = {
            "G": (gs_p, gs_m, gr_p, gr_m), "Z": (zs_p, zs_m, zr_p, zr_m), "Y": (ys_p, ys_m, yr_p, yr_m),
        }
        tables = {True: {}, False: {}}
        pair_base = next(sems)
        for _ in range(NZ - 1):
            next(sems)

        def by_part(kind, block, action):
            if kind == "G":
                action(part_g)
            else:
                by_width(block, main_n, main_w, action)

        def move(kind, source, target, sem, device, block, what):
            by_part(kind, block, lambda w: getattr(remote(source.at[:, 0:w], target.at[:, 0:w], sem, device), what)())

        def ring_block(stage, upward):
            return around(4 - stage) if upward else around(stage - 4)

        def term(kind, h, block):
            g, image = lax.rem(block, 4), lax.div(block, 4)
            if kind == "G":
                return own_g[g, image, h]
            if kind == "Z":
                return own[h * 4 + g, image, early:image_rows]
            return own[yb * 4 + g, image, h * y_rows:(h + 1) * y_rows]

        def reserve(kind, stage, h, upward):
            sem = next(sems)
            tables[upward][(kind, stage, h)] = sem
            send_buf = bufs[kind][0 if upward else 1].at[stage, h]
            device = up_z if upward else down_z
            block = ring_block(stage, upward)
            sent.append(lambda: move(kind, send_buf, send_buf, sem, device, block, "wait_send"))

        def hop(kind, stage, h, upward):
            send_buf = bufs[kind][0 if upward else 1]
            recv_buf = bufs[kind][2 if upward else 3]
            device = up_z if upward else down_z
            block = ring_block(stage, upward)
            value = term(kind, h, block)
            if stage >= 2 or (stage == 1 and h == (0 if upward else 1)):
                buf = recv_buf.at[stage - 1, h]
                move(kind, buf, buf, tables[upward][(kind, stage - 1, h)], device, block, "wait_recv")
                value = value + recv_buf[stage - 1, h].astype(F32)
            send_buf[stage, h] = value.astype(BF16)
            if (kind, stage, h) not in tables[upward]:
                reserve(kind, stage, h, upward)
            move(kind, send_buf.at[stage, h], recv_buf.at[stage, h], tables[upward][(kind, stage, h)], device, block, "start")

        for kind in ("G", "Z"):
            reserve(kind, 0, 0, True)
            reserve(kind, 0, 1, False)
            reserve(kind, 1, 1, True)
            reserve(kind, 1, 0, False)

        def order(i):
            away = 4 - lax.div(i + 1, 2)
            return around(jnp.where(lax.rem(i, 2) == 1, away, -away))

        def send_pair(i):
            block = order(i)
            pair_s[i] = own[other * 4 + lax.rem(block, 4), lax.div(block, 4), 0:early].astype(BF16)
            move("Y", pair_s.at[i], pair_r.at[i], pair_base + i, pair, block, "start")

        n_tok = 2 * image_rows

        def product(i, carry):
            g = traced_group_at(i)
            for member in range(2):
                own[member * 4 + g] = jnp.dot(
                    gathered[yb].reshape(n_tok, feats), w_main[member * 4 + g], preferred_element_type=F32
                ).reshape(2, image_rows, main_w)

            @pl.when(i == 0)
            def _():
                hop("Z", 0, 0, True)
                hop("Z", 0, 1, False)

            @pl.when(i == 1)
            def _():
                hop("Z", 1, 1, True)

            @pl.when(i == 2)
            def _():
                hop("Z", 1, 0, False)

            send_pair(i)
            return carry

        def product_g(i, carry):
            g = traced_group_at(i)
            remote(w_g.at[g, other], w_g.at[g, other], g_base + i, pair).wait_recv()
            own_g[g] = (
                jnp.dot(gathered[0].reshape(n_tok, feats), w_g[g, 0], preferred_element_type=F32)
                + jnp.dot(gathered[1].reshape(n_tok, feats), w_g[g, 1], preferred_element_type=F32)
            ).reshape(2, 2, image_rows // 2, part_g)

            @pl.when(i == 0)
            def _():
                hop("G", 0, 0, True)
                hop("G", 0, 1, False)

            @pl.when(i == 1)
            def _():
                hop("G", 1, 1, True)

            @pl.when(i == 2)
            def _():
                hop("G", 1, 0, False)

            return carry

        lax.fori_loop(0, 4, product, 0)

        def rest_of_pair(i, carry):
            send_pair(i)
            return carry

        lax.fori_loop(4, NZ, rest_of_pair, 0)
        for copy in waits["mix_stage"]:
            copy.wait()
        mix_sems = [next(sems) for _ in range(4)]

        def send_mix(g):
            n = wide_mix if g == 3 else narrow_mix
            copy = remote(w_ms.at[g, 0:n], w_mix.at[yb * 4 + g, 0:n], mix_sems[g], pair)
            copy.start()
            sent.append(copy.wait_send)

        for i in range(NZ):
            sent.append(lambda i=i: move(
                "Y", pair_s.at[i], pair_s.at[i], pair_base + i, pair, order(jnp.int32(i)), "wait_send"))

        def pair_sum(i):
            block = order(jnp.int32(i))
            move("Y", pair_r.at[i], pair_r.at[i], pair_base + i, pair, block, "wait_recv")
            at = own.at[yb * 4 + lax.rem(block, 4), lax.div(block, 4), 0:early]
            at[...] = at[...] + pair_r[i].astype(F32)

        def four(kind, stage, before=(None, None)):
            for sums, h, upward in ((before[0], 1, True), (before[1], 0, False), (None, 0, True), (None, 1, False)):
                if sums is not None:
                    pair_sum(sums)
                hop(kind, stage, h, upward)

        def all_in(kind):
            for h, upward in ((1, True), (0, False), (0, True), (1, False)):
                buf = bufs[kind][2 if upward else 3].at[3, h]
                move(kind, buf, buf, tables[upward][(kind, 3, h)], up_z if upward else down_z, z, "wait_recv")

        hop("Z", 1, 0, True)
        hop("Z", 1, 1, False)
        lax.fori_loop(0, 1, product_g, 0)
        four("Z", 2)
        lax.fori_loop(1, 3, product_g, 0)
        four("Z", 3)
        lax.fori_loop(3, 4, product_g, 0)
        hop("G", 1, 0, True)
        hop("G", 1, 1, False)
        pair_sum(0)
        hop("Y", 0, 0, True)
        hop("Y", 0, 1, False)
        four("G", 2)
        all_in("Z")
        last_s[...] = (term("Z", other, z) + zr_p[3, other].astype(F32) + zr_m[3, other].astype(F32)).astype(BF16)
        last_sem = next(sems)
        move("Z", last_s, last_r, last_sem, pair, z, "start")
        sent.append(lambda: move("Z", last_s, last_s, last_sem, pair, z, "wait_send"))
        for g in (3, 0, 1, 2):
            send_mix(g)
        for device, sem in ((outer, x_spread[1]), (diagonal, x_spread[2])):
            copy = remote(xraw.at[yb], xraw.at[yb], sem, device)
            copy.start()
            sent.append(copy.wait_send)
        four("Y", 1, (1, 2))
        four("G", 3)
        four("Y", 2, (3, 4))
        four("Y", 3, (5, 6))
        is_wide = wide(z)
        all_in("G")
        for h in range(2):
            hidden = gelu(term("G", h, z) + gr_p[3, h].astype(F32) + gr_m[3, h].astype(F32))

            @pl.when(is_wide)
            def _():
                acts[z, h, :, main_w:wide_mix] = hidden

            @pl.when(jnp.logical_not(is_wide))
            def _():
                acts[z, h, :, HEAD:narrow_mix] = hidden

        full[early:image_rows] = term("Z", yb, z) + zr_p[3, yb].astype(F32) + zr_m[3, yb].astype(F32)
        move("Z", last_r, last_r, last_sem, pair, z, "wait_recv")
        full[early:image_rows] = full[early:image_rows] + last_r[...].astype(F32)
        pair_sum(7)
        all_in("Y")
        for h in range(2):
            full[h * y_rows:(h + 1) * y_rows] = term("Y", h, z) + yr_p[3, h].astype(F32) + yr_m[3, h].astype(F32)

        @pl.when(is_wide)
        def _():
            acts[z, :, :, 0:main_w] = gelu(full[...]).reshape(2, image_rows // 2, main_w)

        @pl.when(jnp.logical_not(is_wide))
        def _():
            value = full[:, 0:main_n].astype(BF16)
            result = attend(value[:, 0:HEAD], value[:, HEAD:2 * HEAD], value[:, 2 * HEAD:3 * HEAD])
            acts[z, :, :, 0:HEAD] = result.reshape(2, image_rows // 2, HEAD)

        piece_rows = image_rows // 4

        def act_copy(block, piece, sem, device, what):
            rows = slice((piece % 2) * piece_rows, (piece % 2 + 1) * piece_rows)

            def action(w):
                part = acts.at[block, piece // 2, rows, 0:w]
                getattr(remote(part, part, sem, device), what)()

            by_width(block, narrow_mix, wide_mix, action)

        def add_product(k, block):
            g, image = lax.rem(block, 4), lax.div(block, 4)

            def add(w):
                acc[k, image] = acc[k, image] + jnp.dot(
                    acts[block, :, :, 0:w].reshape(image_rows, w), w_mix[k * 4 + g, 0:w], preferred_element_type=F32)

            by_width(block, narrow_mix, wide_mix, add)

        def add_known(k, block):
            g, image = block % 4, block // 4
            w = wide_mix if g == 3 else narrow_mix
            acc[k, image] = acc[k, image] + jnp.dot(
                acts[block, :, :, 0:w].reshape(image_rows, w), w_mix[k * 4 + g, 0:w], preferred_element_type=F32)

        acc[...] = jnp.zeros_like(acc)

        def after_stage(stage):
            if stage == -1:
                for copy in waits["mix"]:
                    copy.wait()
                add_product(yb, z)
            elif stage < 3:
                add_product(yb, around(-1 - stage))
                add_product(yb, around(1 + stage))
                if stage == 2:
                    for g in (3, 0, 1, 2):
                        n = wide_mix if g == 3 else narrow_mix
                        part = w_mix.at[other * 4 + g, 0:n]
                        remote(part, part, mix_sems[g], pair).wait_recv()
                        for block in (g, g + 4):
                            pl.when(around(4) != block)(lambda block=block: add_known(other, block))
            else:
                add_product(yb, around(4))
                add_product(other, around(4))

        pieces_of_ring(act_copy, after_stage)

        for k in range(2):
            mix1_s[k] = acc[k].astype(BF16).reshape(2, n_x, 2, patches, feats)
        total = col_sum_by_core()
        terms[yb] = total.astype(BF16)
        for device, sem in ((pair, spread[0]), (outer, spread[1]), (diagonal, spread[2])):
            copy = remote(terms.at[yb], terms.at[yb], sem, device)
            copy.start()
        for wait in sent:
            wait()
        sent.clear()
        for g in range(3):
            remote(w1_in.at[g, other], w1_in.at[g, other], block_sems["outer"][g], outer).wait_recv()
            remote(w1_in.at[g, yb], w1_in.at[g, yb], block_sems["forward"][g], outer).wait_recv()
        for half_k, name in ((other, "outer"), (yb, "forward")):
            for k, (lo, hi) in ((3, (0, 2 * group)), (4, (2 * group, 3 * group))):
                part = w1_mix.at[half_k, lo:hi]
                remote(part, part, block_sems[name][k], outer).wait_recv()
        remote(gain1.at[other], gain1.at[other], block_sems["gain"][1], outer).wait_recv()
        remote(gain1.at[yb], gain1.at[yb], block_sems["gain"][2], diagonal).wait_recv()
        remote(terms.at[other], terms.at[other], spread[0], pair).wait_recv()

    x_spread = [next(sems) for _ in range(3)]
    spread = [next(sems) for _ in range(3)]
    pl.when(in_first)(first_layer)

    @pl.when(in_second)
    def _():
        remote(terms.at[other], terms.at[other], spread[1], outer).wait_recv()
        remote(terms.at[yb], terms.at[yb], spread[2], diagonal).wait_recv()
        remote(xraw.at[other], xraw.at[other], x_spread[1], outer).wait_recv()
        remote(xraw.at[yb], xraw.at[yb], x_spread[2], diagonal).wait_recv()
    for k in range(2):
        xb1[k] = (xraw[k].astype(F32) + terms[0, k].astype(F32) + terms[1, k].astype(F32)).astype(BF16)

    @pl.when(in_first)
    def _():
        y_ref[...] = xb1[yb]

    n_tok = 2 * n_col * patches
    both = xb1[...].astype(F32).reshape(2, 2 * patches, feats)
    sums = jnp.sum(jnp.sum(both, axis=-1, keepdims=True), axis=0)
    squares = jnp.sum(jnp.sum(both * both, axis=-1, keepdims=True), axis=0)
    stat1[z] = column_stats(sums, squares)
    copies = []
    for step in range(1, NZ):
        copy = remote(stat1.at[z], stat1.at[z], next(sems), {"row": yb * NZ + around(step)})
        copy.start()
        copies.append(copy)
    finish_k = []
    for k in range(2):
        gathered1[k, :, col] = xb1[k]
        finish_k.append(col_gather(lambda c, k=k: gathered1.at[k, :, c]))
    for copy in copies:
        copy.wait()
    stat_col[1, col] = lane_stats(jnp.sum(stat1[...], axis=0))
    finish_stats1 = col_direct(lambda c: stat_col.at[1, c])
    for finish in finish_k:
        finish()
    for copy in finish_stats1:
        copy.wait()
    columns1 = to_columns(stat_col[1])
    for c in range(n_col):
        for k in range(2):
            gathered1[k, :, c] = normalise(gathered1[k, :, c], columns1, c, gain1[k, 0:1])

    piece_long = 2 * patches
    piece_short = 3 * patches // 2
    third_rows = patches // 2

    def partial_product(g):
        return (
            jnp.dot(gathered1[0].reshape(n_tok, feats), w1_in[g, 0], preferred_element_type=F32)
            + jnp.dot(gathered1[1].reshape(n_tok, feats), w1_in[g, 1], preferred_element_type=F32)
        )

    @pl.when(in_first)
    def _():
        for g in range(3):
            value = partial_product(g).reshape(NZ, 4, third_rows, group)
            own1[:, :, g * third_rows:(g + 1) * third_rows] = value

    @pl.when(in_second)
    def _():
        for g in range(4):
            value = partial_product(g).reshape(2, 4, piece_long, group)
            own1[g] = value[0]
            own1[4 + g] = value[1]

    def by_section(action):
        either(in_first, lambda: action(piece_short), lambda: action(piece_long))

    up1, down1 = {}, {}

    def far(h, upward):
        return (h < 2) == upward

    def hop1(stage, h, upward):
        send_buf, recv_buf = (zs1_p, zr1_p) if upward else (zs1_m, zr1_m)
        table = up1 if upward else down1
        device = up_z if upward else down_z
        block = around(4 - stage) if upward else around(stage - 4)
        value = own1[block, h]
        if stage >= 2 or (stage == 1 and far(h, upward)):
            sem = table[(stage - 1, h)]
            by_section(lambda n: remote(
                recv_buf.at[stage - 1, h, 0:n], recv_buf.at[stage - 1, h, 0:n], sem, device).wait_recv())
            value = value + recv_buf[stage - 1, h].astype(F32)
        send_buf[stage, h] = value.astype(BF16)
        sem_out = next(sems)
        table[(stage, h)] = sem_out
        by_section(lambda n: remote(
            send_buf.at[stage, h, 0:n], recv_buf.at[stage, h, 0:n], sem_out, device).start())
        sent.append(lambda: by_section(lambda n: remote(
            send_buf.at[stage, h, 0:n], recv_buf.at[stage, h, 0:n], sem_out, device).wait_send()))

    for h in (0, 1):
        hop1(0, h, True)
        hop1(0, h + 2, False)
    for stage in (1, 2, 3):
        for h in (2, 3, 0, 1):
            hop1(stage, h, True)
            hop1(stage, (h + 2) % 4, False)
    for h in range(4):
        by_section(lambda n: remote(zr1_p.at[3, h, 0:n], zr1_p.at[3, h, 0:n], up1[(3, h)], up_z).wait_recv())
        by_section(lambda n: remote(zr1_m.at[3, h, 0:n], zr1_m.at[3, h, 0:n], down1[(3, h)], down_z).wait_recv())

    def summed(h):
        return own1[z, h] + zr1_p[3, h].astype(F32) + zr1_m[3, h].astype(F32)

    has_head = jnp.logical_and(in_second, jnp.logical_not(wide(z)))

    @pl.when(has_head)
    def _():
        value = jnp.concatenate([summed(h) for h in range(4)], axis=0).astype(BF16)
        result = attend(value[:, 0:HEAD], value[:, HEAD:2 * HEAD], value[:, 2 * HEAD:3 * HEAD])
        acts1[z, :, :, 0:HEAD] = result.reshape(4, piece_long, HEAD)

    @pl.when(jnp.logical_not(has_head))
    def _():
        for h in range(4):
            acts1[z, h] = gelu(summed(h))

    def by_kind(block, action):
        either(
            in_first,
            lambda: action(piece_short, group),
            lambda: by_width(block, HEAD, group, lambda w: action(piece_long, w)),
        )

    def act_copy1(block, piece, sem, device, what):
        def action(n, w):
            part = acts1.at[block, piece, 0:n, 0:w]
            getattr(remote(part, part, sem, device), what)()

        by_kind(block, action)

    image_sums = []

    def send_image(image):
        first = image * 4
        span = pl.ds(pl.multiple_of(image * image_rows, image_rows), image_rows)

        @pl.when(in_first)
        def _():
            for k in range(2):
                total = None
                for g in range(3):
                    hidden = acts1[pl.ds(first, 4), :, g * third_rows:(g + 1) * third_rows].reshape(image_rows, group)
                    term = jnp.dot(hidden, w1_mix[k, g * group:(g + 1) * group], preferred_element_type=F32)
                    total = term if total is None else total + term
                acc1[k, span] = total

        @pl.when(in_second)
        def _():
            value = jnp.concatenate(
                [acts1[first + j, :, :, 0:HEAD].reshape(image_rows, HEAD) for j in range(3)]
                + [acts1[first + 3].reshape(image_rows, group)], axis=1)
            for k in range(2):
                acc1[k, span] = jnp.dot(value, w1_mix[k, 0:2 * group], preferred_element_type=F32)

        for k in range(2):
            mix1_s[k, image] = acc1[k, span].astype(BF16).reshape(n_x, 2, patches, feats)
        for slot, target_x, target_core, device in col_peers():
            copy = remote(
                mix1_s.at[:, image, target_x, target_core], mix_r.at[slot, :, image], next(sems), device)
            copy.start()
            image_sums.append(copy)

    near = lax.div(z, 4)

    def after_stage1(stage):
        if stage == 2:
            send_image(near)

    pieces_of_ring(act_copy1, after_stage1)
    send_image(1 - near)
    for copy in image_sums:
        copy.wait()
    total = mix1_s[:, :, chip_x, core].astype(F32)
    for slot in range(n_col - 1):
        total = total + mix_r[slot].astype(F32)
    ys1[...] = total.astype(BF16)
    to_pair, to_outer, to_diagonal = next(sems), next(sems), next(sems)

    @pl.when(in_first)
    def _():
        copies = [remote(ys1.at[other], yr1.at[1], to_outer, outer), remote(ys1.at[yb], yr1.at[2], to_diagonal, diagonal)]
        for copy in copies:
            copy.start()
        for copy in copies:
            copy.wait_send()

    @pl.when(in_second)
    def _():
        copy = remote(ys1.at[other], yr1.at[0], to_pair, pair)
        copy.start()
        copy.wait()
        remote(yr1.at[1], yr1.at[1], to_outer, outer).wait_recv()
        remote(yr1.at[2], yr1.at[2], to_diagonal, diagonal).wait_recv()
        result = xb1[yb].astype(F32) + ys1[yb].astype(F32)
        for k in range(3):
            result = result + yr1[k].astype(F32)
        y_ref[...] = result.astype(BF16)

    assert next(sems) < 320
    for wait in sent:
        wait()

    @pl.when(in_first)
    def _():
        for device, sem in ((pair, spread[0]), (outer, spread[1]), (diagonal, spread[2])):
            remote(terms.at[yb], terms.at[yb], sem, device).wait_send()


def layers(x, weights):
    gain, wq, wk, wv, wup, wout, wdown = weights
    n_col = lax.axis_size("col")
    images, patches, feats = x.shape
    wide_in = 6 * HEAD
    vmem = pl.BlockSpec(memory_space=pltpu.VMEM)
    anywhere = pl.BlockSpec(memory_space=pl.ANY)
    rows = n_col * patches
    late = rows // 2
    early = rows - late
    g_buf = pltpu.VMEM((4, 2, rows // 2, 2 * HEAD), BF16)
    z_buf = pltpu.VMEM((4, 2, late, 4 * HEAD), BF16)
    y_buf = pltpu.VMEM((4, 2, early // 2, 4 * HEAD), BF16)
    pair_buf = pltpu.VMEM((NZ, early, 4 * HEAD), BF16)
    z1_buf = pltpu.VMEM((4, 4, 2 * patches, feats), BF16)
    scratch = [
        pltpu.VMEM((NZ, feats, wide_in), BF16),
        pltpu.VMEM((NZ, wide_in, feats), BF16),
        pltpu.VMEM((NZ, feats, 4 * HEAD), BF16),
        pltpu.VMEM((4, 2, feats, 2 * HEAD), BF16),
        pltpu.VMEM((4, feats, 2 * HEAD), BF16),
        pltpu.VMEM((4, wide_in, feats), BF16),
        pltpu.VMEM((2, 2, n_col, patches, feats), BF16),
        pltpu.VMEM((2, 8, feats), F32),
        pltpu.VMEM((NZ, 2, rows, 4 * HEAD), F32),
        pltpu.VMEM((4, 2, 2, rows // 2, 2 * HEAD), F32),
        pltpu.VMEM((2 * NZ, 8, 128), F32),
        g_buf, g_buf, g_buf, g_buf, z_buf, z_buf, z_buf, z_buf, y_buf, y_buf, y_buf, y_buf, pair_buf, pair_buf,
        pltpu.VMEM((late, 4 * HEAD), BF16), pltpu.VMEM((late, 4 * HEAD), BF16),
        pltpu.VMEM((rows, 4 * HEAD), F32),
        pltpu.VMEM((NZ, 2, rows // 2, wide_in), BF16),
        pltpu.VMEM((2, 2, rows, feats), F32),
        pltpu.VMEM((2, n_col, 8, 128), F32),
        pltpu.VMEM((2, 2, patches, feats), BF16),
        pltpu.VMEM((2, 2, 2, patches, feats), BF16),
        pltpu.VMEM((2, 2, n_col // 2, patches, feats), BF16),
        pltpu.VMEM((2, 2, n_col // 2, patches, feats), BF16),
        pltpu.VMEM((n_col // 2 - 1, 2, 2, patches, feats), BF16),
        pltpu.VMEM((4, 2, feats, feats), BF16),
        pltpu.VMEM((2, 3 * feats, feats), BF16),
        pltpu.VMEM((2, 8, feats), F32),
        pltpu.VMEM((2, 2, patches, feats), BF16),
        pltpu.VMEM((2, 2, n_col, patches, feats), BF16),
        pltpu.VMEM((NZ, 4, 2 * patches, feats), F32),
        pltpu.VMEM((NZ, 8, 128), F32),
        z1_buf, z1_buf, z1_buf, z1_buf,
        pltpu.VMEM((NZ, 4, 2 * patches, feats), BF16),
        pltpu.VMEM((2, 2 * n_col * patches, feats), F32),
        pltpu.VMEM((2, 2, n_col // 2, 2, patches, feats), BF16),
        pltpu.VMEM((n_col - 1, 2, 2, patches, feats), BF16),
        pltpu.VMEM((2, 2, patches, feats), BF16),
        pltpu.VMEM((3, 2, patches, feats), BF16),
        pltpu.SemaphoreType.DMA((64,)),
        pltpu.SemaphoreType.DMA((320,)),
        pltpu.SemaphoreType.DMA((320,)),
    ]
    return pl.pallas_call(
        functools.partial(layers_kernel, n_col, patches, feats),
        out_shape=jax.ShapeDtypeStruct(x.shape, BF16),
        in_specs=[vmem, vmem] + [anywhere] * 6,
        out_specs=vmem,
        scratch_shapes=scratch,
        compiler_params=pltpu.CompilerParams(
            collective_id=0, has_side_effects=True, vmem_limit_bytes=67043328
        ),
    )(x, gain[None], wq, wk, wv, wup, wout, wdown)


def local(tokens, ln_gain, w_query, w_key, w_value, w_up, w_out, w_down):
    weights = (ln_gain[0], w_query[0], w_key[0], w_value[0], w_up[0], w_out[0], w_down[0])
    return layers(tokens, weights)[None]


def solution(mesh):
    return jax.shard_map(
        local,
        mesh=mesh,
        in_specs=(
            P(None, "col", "row"),
            P("section", "row"),
            P("section", "row", "col"),
            P("section", "row", "col"),
            P("section", "row", "col"),
            P("section", "row", "col"),
            P("section", "col", "row"),
            P("section", "col", "row"),
        ),
        out_specs=P("section", None, "col", "row"),
        check_vma=False,
    )
```
